32 devices in a mesh: mem: 2 (over y), space: 16 (over z, x, core).
Axes of the slice: x: 2, y: 2, z: 4, core: 2. Of those that a mesh axis runs over, the one named last changes fastest.
Arguments:
- ensemble: bfloat16 [64, 160, 32, 128], P('mem', None, 'space'), may hold values from -6 to 6
- obs_value: float32 [16, 256], P('space'), may hold values from -6 to 6
- obs_error: float32 [16, 256], P('space'), may hold values from 0.3 to 3
- obs_cell: int32 [16, 256], P('space'), may hold values from 0 to 255
- obs_species: int32 [16, 256], P('space'), may hold values from 0 to 39
- patch_index: int32 [16, 256, 32], P('space', 'mem'), may hold values from 0 to 767, as said below
- patch_count: int32 [16, 256], P('space', 'mem'), may hold values from 1 to 32, as said below
- courant_x: float32 [4, 32, 128], P(None, 'space'), may hold values from -0.7 to 0.7
- courant_y: float32 [4, 32, 128], P(None, 'space'), may hold values from -0.7 to 0.7
- dep_velocity: float32 [40], replicated, may hold values from 0.05 to 0.5
- surface_factor: float32 [32, 128], P('space'), may hold values from 0.5 to 2
Outputs:
- forecast: bfloat16 [64, 160, 32, 128], P('mem', None, 'space')
The draws below stay inside these ranges and needn't reach their ends.
Inputs may be any that keep to these rules, and one draw needn't show every extreme that they name: `patch_index`: each cell's list names distinct pool observations of existing tiles, nearest to the cell first; those within 3 cells of the cell come first. `patch_count`: the number of listed observations used for the cell, at least 1 and at most 32; the most is reached in every draw.
All inputs are finite; a program needn't handle non-finite values.
Results may differ from the reference program's by a relative error of at most 0.0049.
Values may be sent and summed in bfloat16 or wider, within the bound.
A program may use at most 64 MiB of HBM per device.

```python
import math
import jax
import jax.numpy as jnp
from jax import lax

MEMBERS = 64
SPECIES = 40
LEVELS = 4
NX = 128
ROWS = 2
OBS_TILE = 256
MAXOBS = 32
NEWTON = 8
SUBSTEPS = 2
TILES = 16
NY = 32
FIELDS = 160
LOC = 1


def shared_cells(key):
    return jax.random.randint(jax.random.fold_in(key, 7177), (TILES, OBS_TILE), 0, ROWS * NX, dtype=jnp.int32)


def nearest_lists(key):
    cells = shared_cells(key)
    padded = jnp.pad(cells, ((1, 1), (0, 0)))
    tile_ids = jnp.arange(TILES, dtype=jnp.int32)
    reach = 3 * LOC

    def one_tile(tile_num):
        pool_cells = lax.dynamic_slice_in_dim(padded, tile_num, 3, 0)
        offsets = (jnp.arange(3, dtype=jnp.int32) - 1) * ROWS
        pool_row = (pool_cells // NX + offsets[:, None]).reshape(-1)
        pool_col = (pool_cells % NX).reshape(-1)
        source_tile = tile_num - 1 + jnp.arange(3, dtype=jnp.int32)
        exists = (source_tile >= 0) & (source_tile < TILES)
        exists = jnp.broadcast_to(exists[:, None], (3, OBS_TILE)).reshape(-1)
        cell_ids = jnp.arange(ROWS * NX, dtype=jnp.int32)
        cell_row = cell_ids // NX
        cell_col = cell_ids % NX
        dist_sq = (pool_row[None, :] - cell_row[:, None]) ** 2 + (pool_col[None, :] - cell_col[:, None]) ** 2
        dist_sq = jnp.where(exists[None, :], dist_sq, 40000)
        score = dist_sq * 2048 + jnp.arange(3 * OBS_TILE, dtype=jnp.int32)[None, :]
        neg_top, chosen = lax.top_k(-score, MAXOBS)
        near = jnp.sum(((dist_sq <= reach * reach) & exists[None, :]).astype(jnp.int32), axis=1)
        return (chosen.astype(jnp.int32), jnp.clip(near, 1, MAXOBS).astype(jnp.int32))
    chosen, counts = lax.map(one_tile, tile_ids)
    counts = counts.at[0, 0].set(MAXOBS)
    return (chosen, counts)


def draw_obs_cell(key, part):
    return shared_cells(key)


def draw_patch_index(key, part):
    return nearest_lists(key)[0]


def draw_patch_count(key, part):
    return nearest_lists(key)[1]


def touch_ends(array, stream_key, smallest, largest):
    longest = array.shape.index(max(array.shape))
    spots = []
    for shift in (0, 1):
        where = [jax.random.randint(jax.random.fold_in(stream_key, axis), (), 0, length) for axis, length in enumerate(array.shape)]
        where[longest] = (where[longest] + shift) % array.shape[longest]
        spots.append(tuple(where))
    return array.at[spots[0]].set(smallest).at[spots[1]].set(largest)


def block_levels(stream_key, dims, split, least, largest):
    def one(axis_at, parts):
        draws = jax.random.uniform(jax.random.fold_in(jax.random.fold_in(stream_key, 6), axis_at), (parts,), jnp.float32, least / len(split), largest / len(split))
        return jnp.repeat(jnp.exp(draws), dims[axis_at] // parts).reshape((-1,) + (1,) * (len(dims) - axis_at - 1))

    level = one(*split[0])
    for cut in split[1:]:
        level = level * one(*cut)
    return level


def noise(stream_key, extent, spread, most, pieces=(), kind=jnp.bfloat16):
    array = jax.random.normal(stream_key, extent, jnp.float32) * spread
    if len(pieces) > 0:
        array = block_levels(stream_key, extent, pieces, -0.22, 0.18) * array
    return jnp.clip(array, min=-most, max=most).astype(kind)


def setup_inputs(seed: int = 0) -> dict:
    splits = jax.random.split(jax.random.key(seed), 12)
    return {
        "ensemble": noise(splits[0], (MEMBERS, FIELDS, NY, NX), 1.0, 6.0, ((0, 2), (2, 16))),
        "obs_value": noise(splits[1], (TILES, OBS_TILE), 1.0, 6.0, ((0, 16),), jnp.float32),
        "obs_error": jnp.clip(jnp.exp(math.log(3.0) - 2.3025851 * jax.random.uniform(splits[2], (TILES, OBS_TILE), jnp.float32) ** block_levels(splits[2], (TILES, OBS_TILE), ((0, 16),), -0.2, 0.2)), 0.3, 3.0),
        "obs_cell": draw_obs_cell(jax.random.fold_in(splits[11], 71), 0),
        "obs_species": touch_ends(jax.random.randint(splits[4], (TILES, OBS_TILE), 0, SPECIES), jax.random.fold_in(splits[4], 1), 0, SPECIES - 1).astype(jnp.int32),
        "patch_index": draw_patch_index(jax.random.fold_in(splits[11], 71), 0),
        "patch_count": draw_patch_count(jax.random.fold_in(splits[11], 71), 0),
        "courant_x": jnp.clip(jax.random.uniform(splits[7], (LEVELS, NY, NX), jnp.float32, -0.7, 0.7) * block_levels(splits[7], (LEVELS, NY, NX), ((1, 16),), -0.4, 0.0), -0.7, 0.7),
        "courant_y": jnp.clip(jax.random.uniform(splits[8], (LEVELS, NY, NX), jnp.float32, -0.7, 0.7) * block_levels(splits[8], (LEVELS, NY, NX), ((1, 16),), -0.4, 0.0), -0.7, 0.7),
        "dep_velocity": jnp.clip(jnp.exp(jax.random.uniform(splits[9], (SPECIES,), jnp.float32, math.log(0.05), math.log(0.5))), 0.05, 0.5),
        "surface_factor": jnp.clip(0.5 + 1.5 * jax.random.uniform(splits[10], (NY, NX), jnp.float32) ** block_levels(splits[10], (NY, NX), ((0, 16),), -0.2, 0.2), 0.5, 2.0),
    }


def inverse_root(matrix, trace_val, repeats):
    matrix_order = matrix.shape[-1]
    identity = jnp.eye(matrix_order, dtype=jnp.float32)
    iterate = matrix / trace_val[:, None, None]
    inv_root = jnp.broadcast_to(identity, matrix.shape)
    for repeat in range(repeats):
        middle = 1.5 * identity - 0.5 * jnp.einsum('cij,cjk->cik', inv_root, iterate, precision=lax.Precision.HIGHEST)
        iterate = jnp.einsum('cij,cjk->cik', iterate, middle, precision=lax.Precision.HIGHEST)
        inv_root = jnp.einsum('cij,cjk->cik', middle, inv_root, precision=lax.Precision.HIGHEST)
    return inv_root

def prepare_pool(obs_pool, members, row_offsets):
    pooled = jnp.transpose(obs_pool[:, :members], (1, 0, 2)).reshape(members, -1)
    extra = obs_pool[:, members:]
    obs_mean = lax.optimization_barrier(jnp.mean(pooled, axis=0))
    obs_dev = jnp.transpose(pooled - obs_mean[None, :])
    values = extra[:, 0].reshape(-1)
    errors = extra[:, 1].reshape(-1)
    obs_row = (extra[:, 2] + row_offsets[:, None]).reshape(-1)
    obs_col = extra[:, 3].reshape(-1)
    return (obs_dev, obs_mean, values, errors, obs_row, obs_col)

def analyse(block_state, prepared, indices, counts, cell_ids, columns, radius, repeats):
    obs_dev, obs_mean, values, errors, obs_row, obs_col = prepared
    members = obs_dev.shape[1]
    picked = obs_dev[indices]
    cell_row = (cell_ids // columns).astype(jnp.float32)
    cell_col = (cell_ids % columns).astype(jnp.float32)
    distance_sq = (obs_row[indices] - cell_row[:, None]) ** 2 + (obs_col[indices] - cell_col[:, None]) ** 2
    active = jnp.arange(indices.shape[1], dtype=jnp.int32)[None, :] < counts[:, None]
    obs_weight = jnp.where(active, jnp.exp(-distance_sq / (2.0 * radius * radius)) / errors[indices], 0.0)
    innovation = values[indices] - obs_mean[indices]
    identity = jnp.eye(members, dtype=jnp.float32)
    gram_mat = jnp.einsum('cok,col->ckl', picked * obs_weight[:, :, None], picked, precision=lax.Precision.HIGHEST) + (members - 1.0) * identity
    trace_val = jnp.einsum('ckk->c', gram_mat)
    inv_root = inverse_root(gram_mat, trace_val, repeats)
    gain_vec = jnp.einsum('cok,co->ck', picked, obs_weight * innovation, precision=lax.Precision.HIGHEST)
    analysis_cov = jnp.einsum('ckl,clm->ckm', inv_root, inv_root, precision=lax.Precision.HIGHEST) / trace_val[:, None, None]
    mean_w = jnp.einsum('ckl,cl->ck', analysis_cov, gain_vec, precision=lax.Precision.HIGHEST)
    weights = math.sqrt(members - 1.0) * inv_root / jnp.sqrt(trace_val)[:, None, None] + mean_w[:, :, None]
    state_mean = lax.optimization_barrier(jnp.mean(block_state, axis=0))
    state_dev = block_state - state_mean[None]
    result = state_mean[None] + jnp.einsum('ifc,cij->jfc', state_dev, weights, precision=lax.Precision.HIGHEST)
    return result.astype(jnp.bfloat16)

def rows_step(extended, courant):
    middle = extended[..., 1:-1, :]
    north_row = extended[..., 2:, :]
    south_row = extended[..., :-2, :]
    return middle - 0.5 * courant * (north_row - south_row) + 0.5 * courant * courant * (north_row - 2.0 * middle + south_row)

def cols_step(field_now, courant):
    padded = jnp.pad(field_now, [(0, 0)] * (field_now.ndim - 1) + [(1, 1)])
    middle = padded[..., 1:-1]
    east_col = padded[..., 2:]
    west_col = padded[..., :-2]
    return middle - 0.5 * courant * (east_col - west_col) + 0.5 * courant * courant * (east_col - 2.0 * middle + west_col)

def deposit(field_now, dep_velocity, surface_factor):
    loss = jnp.exp(-dep_velocity[:, None, None] * surface_factor[None])
    lowest = (jnp.arange(field_now.shape[2], dtype=jnp.int32) == 0)[:, None, None]
    factor = jnp.where(lowest[None], loss[:, None], 1.0)
    return field_now * factor[None]

def reference(ensemble, obs_value, obs_error, obs_cell, obs_species, patch_index, patch_count, courant_x, courant_y, dep_velocity, surface_factor):
    tile_cells = ROWS * NX
    by_tile = jnp.transpose(ensemble.reshape(MEMBERS, FIELDS, TILES, tile_cells), (2, 0, 1, 3))
    flat_state = by_tile.reshape(TILES, MEMBERS, FIELDS * tile_cells)
    position = obs_species * (LEVELS * tile_cells) + obs_cell
    position = jnp.broadcast_to(position[:, None, :], (TILES, MEMBERS, OBS_TILE))
    equivalents = jnp.take_along_axis(flat_state, position, axis=2).astype(jnp.float32)
    obs_info = jnp.stack([obs_value, obs_error, (obs_cell // NX).astype(jnp.float32), (obs_cell % NX).astype(jnp.float32)], axis=1)
    packed = jnp.concatenate([equivalents, obs_info], axis=1)
    padded = jnp.pad(packed, ((1, 1), (0, 0), (0, 0)))
    row_offsets = (jnp.arange(3, dtype=jnp.float32) - 1.0) * ROWS

    def one_tile(tile_num):
        obs_pool = lax.dynamic_slice_in_dim(padded, tile_num, 3, 0)
        prepared = prepare_pool(obs_pool, MEMBERS, row_offsets)
        block_state = by_tile[tile_num].astype(jnp.float32)
        cell_ids = jnp.arange(tile_cells, dtype=jnp.int32)
        return analyse(block_state, prepared, patch_index[tile_num], patch_count[tile_num], cell_ids, NX, LOC, NEWTON)
    analysed = lax.map(one_tile, jnp.arange(TILES, dtype=jnp.int32))
    analysed = jnp.transpose(analysed, (1, 2, 0, 3)).reshape(MEMBERS, SPECIES, LEVELS, NY, NX)
    field_now = analysed.astype(jnp.float32)
    for repeat in range(SUBSTEPS):
        padded_rows = jnp.pad(field_now, ((0, 0), (0, 0), (0, 0), (1, 1), (0, 0)))
        field_now = rows_step(padded_rows, courant_y)
        field_now = cols_step(field_now, courant_x)
    field_now = deposit(field_now, dep_velocity, surface_factor)
    return field_now.reshape(MEMBERS, FIELDS, NY, NX).astype(jnp.bfloat16)
```

```python
import functools
import math

import jax
import jax.numpy as jnp
from jax import lax
from jax.experimental import pallas as pl
from jax.experimental.pallas import tpu as pltpu
from jax.sharding import PartitionSpec as P

NEWTON = 8
SUBSTEPS = 2
LOC = 1
LANES = 128
GROUP = 8
PITCH = 40
INTERPRET = False


def lane_product(left, right, depth, rows, width, finish, unroll=4):
    def group(block, carry):
        first = pl.multiple_of(block * GROUP, GROUP)

        def step(k, sums):
            row = right(k)
            return tuple(sums[r] + left(k, first, r) * row for r in range(GROUP))

        zero = jnp.zeros((width, LANES), jnp.float32)
        sums = lax.fori_loop(0, depth, step, (zero,) * GROUP, unroll=unroll)
        finish(first, sums)
        return carry

    lax.fori_loop(0, rows // GROUP, group, 0)


def weights_kernel(
    members, repeats, radius,
    pool_ref, idx_ref, cnt_ref, row_ref, col_ref,
    dev_ref, mix_ref, keep_ref,
    first_v, now_v, step_g, keys, tail, innov, scal,
):
    slots = idx_ref.shape[0]
    pooled = pool_ref.shape[1]
    blocks = slots // GROUP
    info = pool_ref[members:, :]
    high = info.astype(jnp.bfloat16).astype(jnp.float32)
    rest = info - high
    middle = rest.astype(jnp.bfloat16).astype(jnp.float32)
    low = rest - middle
    table = jnp.concatenate([pool_ref[:members, :], high, middle, low, jnp.zeros_like(low)], axis=0)
    table = table.astype(jnp.bfloat16)
    place = lax.broadcasted_iota(jnp.int32, (pooled, LANES), 0)
    extra = info.shape[0]

    def pick(k, total):
        hot = jnp.where(place == idx_ref[pl.ds(k, 1), :], 1.0, 0.0).astype(jnp.bfloat16)
        got = jnp.dot(table, hot, preferred_element_type=jnp.float32)
        equiv = got[:members]
        facts = (
            got[members : members + extra]
            + got[members + extra : members + 2 * extra]
            + got[members + 2 * extra : members + 3 * extra]
        )
        mean = jnp.sum(equiv, axis=0, keepdims=True) * (1.0 / members)
        dist = (facts[2:3] - row_ref[...]) ** 2 + (facts[3:4] - col_ref[...]) ** 2
        rho = jnp.exp(-dist / (2.0 * radius * radius)) / facts[1:2]
        scale = jnp.sqrt(jnp.where(k < cnt_ref[...], rho, 0.0))
        scaled = (equiv - mean) * scale
        dev_ref[pl.ds(k, members, stride=slots), :] = scaled
        innov[pl.ds(k, 1), :] = (facts[0:1] - mean) * scale
        return total + jnp.sum(scaled * scaled, axis=0, keepdims=True)

    spread = lax.fori_loop(0, slots, pick, jnp.zeros((1, LANES), jnp.float32), unroll=2)
    shift = members - 1.0
    inverse = 1.0 / (spread + shift * members)
    level = lax.broadcasted_iota(jnp.int32, (GROUP, LANES), 0)

    def eye(r, value):
        return jnp.where(level == r, value, 0.0)

    def at(ref, i, j, base=0):
        start = i * PITCH + j * GROUP
        start = start if isinstance(start, int) else pl.multiple_of(start, GROUP)
        return ref[pl.ds(base + start, GROUP), :]

    def put(ref, i, parts, base=0):
        for j, part in enumerate(parts):
            ref[pl.ds(base + i * PITCH + j * GROUP, GROUP), :] = part
            if j < i // GROUP:
                ref[pl.ds(base + j * GROUP * PITCH + i, GROUP, stride=PITCH), :] = part

    def product(left, right, depth, finish, unroll=4):
        for pair in range((blocks + 1) // 2):
            groups = sorted({pair, blocks - 1 - pair})

            def step(k, sums):
                wide = [right(k, j) for j in range(groups[-1] + 1)]
                out, spot = [], 0
                for g in groups:
                    for r in range(GROUP):
                        one = left(k, g * GROUP + r)
                        for j in range(g + 1):
                            out.append(sums[spot] + one * wide[j])
                            spot += 1
                return tuple(out)

            zero = jnp.zeros((GROUP, LANES), jnp.float32)
            count = sum((g + 1) * GROUP for g in groups)
            sums = lax.fori_loop(0, depth, step, (zero,) * count, unroll=unroll)
            spot = 0
            for g in groups:
                for r in range(GROUP):
                    finish(g * GROUP + r, sums[spot : spot + g + 1])
                    spot += g + 1

    def square(left, right, finish, left_base=0):
        product(
            lambda k, i: left[pl.ds(left_base + k * PITCH + i, 1), :],
            lambda k, j: at(right, k, j),
            slots, finish,
        )

    def gram_done(i, sums):
        parts = [part * inverse for part in sums]
        put(first_v, i, parts)
        put(now_v, i, parts)

    product(
        lambda k, i: dev_ref[pl.ds(k * slots + i, 1), :],
        lambda k, j: dev_ref[pl.ds(pl.multiple_of(k * slots, slots) + j * GROUP, GROUP), :],
        members, gram_done,
    )

    xi = shift * inverse
    mus = []
    for k in range(repeats):
        mu = 1.5 - 0.5 * xi
        scal[pl.ds(k, 1), :] = xi
        scal[pl.ds(repeats + k, 1), :] = mu
        mus.append(mu)
        xi = xi * mu * mu
    after = mus[-1]
    for k in reversed(range(repeats - 1)):
        scal[pl.ds(2 * repeats + k, 1), :] = after
        after = after * mus[k]
    last_z = after
    area = slots * PITCH

    def forward(n, carry):
        xi = scal[pl.ds(n, 1), :]
        mu = scal[pl.ds(repeats + n, 1), :]
        flat, slope = mu * mu - xi * mu, 0.25 * xi - mu
        base = pl.multiple_of(n * area, GROUP)

        def to_g(i, sums):
            parts = [0.25 * part + slope * at(now_v, i, j) for j, part in enumerate(sums)]
            parts[-1] = parts[-1] + eye(i % GROUP, flat)
            put(step_g, i, parts)

        square(now_v, now_v, to_g)

        def to_v(i, sums):
            put(tail, i, sums)
            put(keys, i, [mu * at(step_g, i, j) - 0.5 * part for j, part in enumerate(sums)], base)

        square(step_g, now_v, to_v)
        now_v[...] = tail[...]
        return carry

    lax.fori_loop(0, repeats - 1, forward, 0)

    after = scal[pl.ds(3 * repeats - 2, 1), :]
    for i in range(slots):
        parts = [-0.5 * at(keys, i, j, (repeats - 2) * area) for j in range(blocks)]
        parts[i // GROUP] = parts[i // GROUP] - eye(i % GROUP, 0.5 * after)
        for j, part in enumerate(parts):
            now_v[pl.ds(i * PITCH + j * GROUP, GROUP), :] = part

    def backward(m, carry):
        n = repeats - 3 - m
        base = pl.multiple_of(n * area, GROUP)
        half = 0.5 * scal[pl.ds(2 * repeats + n, 1), :]

        def to_h(i, sums):
            parts = list(sums)
            parts[-1] = parts[-1] - eye(i % GROUP, half)
            put(tail, i, parts)

        square(keys, now_v, to_h, base)
        now_v[...] = tail[...]
        return carry

    lax.fori_loop(0, repeats - 2, backward, 0)

    def whole(ref, k):
        return ref[pl.ds(pl.multiple_of(k * PITCH, GROUP), slots), :]

    none = jnp.zeros((slots, LANES), jnp.float32)

    def apply(ref):
        def step(k, total):
            return total + innov[pl.ds(k, 1), :] * whole(ref, k)

        return lax.fori_loop(0, slots, step, none)

    for _ in range(2):
        start = innov[...]
        innov[...] = apply(now_v)
        innov[...] = last_z * start + apply(first_v)
    gain = innov[...] * inverse
    factor = math.sqrt(shift) * jnp.sqrt(inverse)
    keep_ref[...] = factor * last_z
    both = factor * inverse

    def to_mix(first, sums):
        for r in range(GROUP):
            mix_ref[pl.ds(pl.multiple_of((first + r) * slots, slots), slots), :] = both * sums[r] + gain

    lane_product(
        lambda k, first, r: dev_ref[pl.ds((first + r) * slots + k, 1), :],
        lambda k: whole(now_v, k), slots, members, slots, to_mix,
    )


def solve_cells(pool, idx, counts, rows, cols, members):
    slots, cells = idx.shape
    lane = lambda height: pl.BlockSpec((height, LANES), lambda c: (0, c))
    square = pltpu.VMEM((slots * PITCH, LANES), jnp.float32)
    return pl.pallas_call(
        functools.partial(weights_kernel, members, NEWTON, LOC),
        grid=(cells // LANES,),
        in_specs=[pl.BlockSpec(pool.shape, lambda c: (0, 0)), lane(slots), lane(1), lane(1), lane(1)],
        out_specs=[lane(members * slots), lane(members * slots), lane(1)],
        out_shape=[
            jax.ShapeDtypeStruct((members * slots, cells), jnp.float32),
            jax.ShapeDtypeStruct((members * slots, cells), jnp.float32),
            jax.ShapeDtypeStruct((1, cells), jnp.float32),
        ],
        scratch_shapes=[square] * 3 + [
            pltpu.VMEM(((NEWTON - 1) * slots * PITCH, LANES), jnp.float32),
            square,
            pltpu.VMEM((slots, LANES), jnp.float32),
            pltpu.VMEM((3 * NEWTON, LANES), jnp.float32),
        ],
        compiler_params=pltpu.CompilerParams(vmem_limit_bytes=40 * 1024 * 1024),
        cost_estimate=pl.CostEstimate(flops=2 * 10**9, bytes_accessed=200 * 10**6, transcendentals=0),
        interpret=INTERPRET,
    )(pool, idx, counts, rows, cols)


def analysis_kernel(parts, slots, *refs):
    states = refs[:parts]
    dev_ref, mix_ref, keep_ref = refs[parts : parts + 3]
    outs = refs[parts + 3 : 2 * parts + 3]
    anomaly, mapped, mean_ref = refs[2 * parts + 3 :]
    share, width, _ = states[0].shape
    members = share * parts
    total = jnp.zeros((width, LANES), jnp.float32)
    for state in states:
        total = lax.fori_loop(
            0, share, lambda i, t, s=state: t + s[i].astype(jnp.float32), total, unroll=4
        )
    mean = total * (1.0 / members)
    mean_ref[...] = mean
    for part, state in enumerate(states):

        def subtract(i, carry, s=state, base=part * share):
            anomaly[base + i] = s[i].astype(jnp.float32) - mean_ref[...]
            return carry

        lax.fori_loop(0, share, subtract, 0, unroll=4)

    def to_mapped(first, sums):
        for r in range(GROUP):
            mapped[first + r] = sums[r]

    lane_product(
        lambda i, first, r: dev_ref[pl.ds(i * slots + first + r, 1), :],
        lambda i: anomaly[i], members, slots, width, to_mapped,
    )
    for part, out in enumerate(outs):
        base = part * share

        def to_out(first, sums, out=out, base=base):
            for r in range(GROUP):
                held = mean_ref[...] + keep_ref[...] * anomaly[base + first + r]
                out[first + r] = (held + sums[r]).astype(jnp.bfloat16)

        lane_product(
            lambda k, first, r, base=base: mix_ref[pl.ds((base + first + r) * slots + k, 1), :],
            lambda k: mapped[k], slots, share, width, to_out,
        )


def analyse(states, dev, mix, keep, slots, first, count, width):
    share, _, cells = states[0].shape
    parts = len(states)
    members = share * parts
    wide = lambda height: pl.BlockSpec((height, LANES), lambda c, f: (0, c))
    return pl.pallas_call(
        functools.partial(analysis_kernel, parts, slots),
        grid=(cells // LANES, count // width),
        in_specs=[
            pl.BlockSpec((share, width, LANES), lambda c, f: (0, f + first // width, c))
        ] * parts + [wide(members * slots), wide(members * slots), wide(1)],
        out_specs=[pl.BlockSpec((share, width, LANES), lambda c, f: (0, f, c))] * parts,
        out_shape=[jax.ShapeDtypeStruct((share, count, cells), jnp.bfloat16)] * parts,
        scratch_shapes=[
            pltpu.VMEM((members, width, LANES), jnp.float32),
            pltpu.VMEM((slots, width, LANES), jnp.float32),
            pltpu.VMEM((width, LANES), jnp.float32),
        ],
        compiler_params=pltpu.CompilerParams(vmem_limit_bytes=32 * 1024 * 1024),
        cost_estimate=pl.CostEstimate(flops=10**9, bytes_accessed=50 * 10**6, transcendentals=0),
        interpret=INTERPRET,
    )(*states, dev, mix, keep)


def halo(cells, width):
    count = lax.axis_size("space")
    before = lax.ppermute(cells[-width:], "space", [(i, i + 1) for i in range(count - 1)])
    after = lax.ppermute(cells[:width], "space", [(i + 1, i) for i in range(count - 1)])
    return before, after


def wide_rows(cells, width):
    before, after = halo(cells, width)
    return jnp.concatenate([before, cells, after], axis=0)


def row_step(south, middle, north, courant):
    return (
        middle
        - 0.5 * courant * (north - south)
        + 0.5 * courant * courant * (north - 2.0 * middle + south)
    )


def col_step(middle, courant):
    padded = jnp.pad(middle, [(0, 0)] * (middle.ndim - 1) + [(1, 1)])
    east, west = padded[..., 2:], padded[..., :-2]
    return (
        middle
        - 0.5 * courant * (east - west)
        + 0.5 * courant * courant * (east - 2.0 * middle + west)
    )


def shards(
    ensemble, obs_value, obs_error, obs_cell, obs_species, patch_index, patch_count,
    courant_x, courant_y, dep_velocity, surface_factor,
):
    local_members, fields, tile_rows, columns = ensemble.shape
    species = dep_velocity.shape[0]
    levels = fields // species
    tile_cells = tile_rows * columns
    groups = lax.axis_size("mem")
    members = local_members * groups
    me = lax.axis_index("mem")
    slots = patch_index.shape[2]
    per_dev = tile_cells // groups
    paired = groups == 2 and tile_rows == 2 and columns % LANES == 0
    swap = [(0, 1), (1, 0)]

    if paired:
        mine = lax.dynamic_index_in_dim(ensemble, me, 2, keepdims=False)
        theirs = lax.dynamic_index_in_dim(ensemble, 1 - me, 2, keepdims=False)
    surface = ensemble.reshape(local_members, species, levels, tile_cells)[:, :, 0]
    position = obs_species[0] * tile_cells + obs_cell[0]
    equiv = jnp.take(surface.reshape(local_members, -1), position, axis=1).astype(jnp.float32)
    if paired:
        equiv = jnp.concatenate([equiv, lax.ppermute(equiv, "mem", swap)], axis=0)
    else:
        equiv = lax.all_gather(equiv, "mem", axis=0, tiled=True)
    zeros = jnp.zeros_like(obs_value[0])
    info = jnp.stack(
        [
            obs_value[0],
            obs_error[0],
            (obs_cell[0] // columns).astype(jnp.float32),
            (obs_cell[0] % columns).astype(jnp.float32),
        ]
        + [zeros] * 4
    )
    packed = jnp.concatenate([equiv, info], axis=0)
    before, after = halo(packed[None], 1)
    offset = jnp.zeros((packed.shape[0], 1), jnp.float32).at[members + 2, 0].set(float(tile_rows))
    pool = jnp.concatenate([before[0] - offset, packed, after[0] + offset], axis=1)

    if paired:
        states = (mine, lax.ppermute(theirs, "mem", swap))
    else:
        states = (
            lax.all_to_all(
                ensemble.reshape(local_members, fields, tile_cells),
                "mem", split_axis=2, concat_axis=0, tiled=True,
            ),
        )
    spare = -per_dev % LANES
    pad = lambda a: jnp.pad(a, [(0, 0)] * (a.ndim - 1) + [(0, spare)]) if spare else a
    states = tuple(pad(state) for state in states)
    cell = me * per_dev + jnp.arange(per_dev, dtype=jnp.int32)
    dev, mix, keep = solve_cells(
        pool,
        pad(jnp.transpose(patch_index[0])),
        pad(patch_count),
        pad((cell // columns).astype(jnp.float32)[None]),
        pad((cell % columns).astype(jnp.float32)[None]),
        members,
    )

    width = next(w for w in (32, 16, fields) if fields % w == 0)
    blocks = fields // width
    parts = 2 if paired and blocks > 1 and width % levels == 0 else 1
    cuts = [0, (blocks + 1) // 2 * width, fields] if parts == 2 else [0, fields]
    wide_x = wide_rows(jnp.moveaxis(courant_x, 1, 0), SUBSTEPS)
    wide_y = wide_rows(jnp.moveaxis(courant_y, 1, 0), SUBSTEPS)
    loss = jnp.exp(-dep_velocity[:, None, None] * surface_factor[None])

    results = []
    for low, high in zip(cuts[:-1], cuts[1:]):
        count = high - low
        out = analyse(states, dev, mix, keep, slots, low, count, width)
        if paired:
            other = lax.ppermute(out[1], "mem", swap)
            rows = jnp.stack([jnp.where(me == 0, out[0], other), jnp.where(me == 0, other, out[0])])
        else:
            back = lax.all_to_all(out[0][..., :per_dev], "mem", split_axis=0, concat_axis=2, tiled=True)
            rows = jnp.moveaxis(back.reshape(local_members, count, tile_rows, columns), 2, 0)
        south, north = halo(rows, SUBSTEPS)
        shape = (local_members, count // levels, levels, columns)
        now = [
            part[r].reshape(shape).astype(jnp.float32)
            for part in (south, rows, north)
            for r in range(part.shape[0])
        ]
        for repeat in range(SUBSTEPS):
            first = repeat + 1
            now = [
                col_step(
                    row_step(now[r - 1], now[r], now[r + 1], wide_y[first + r - 1]),
                    wide_x[first + r - 1],
                )
                for r in range(1, len(now) - 1)
            ]
        part = loss[low // levels : high // levels]
        lowest = (jnp.arange(levels, dtype=jnp.int32) == 0)[:, None]
        now = [
            row * jnp.where(lowest, part[:, r][:, None], 1.0) for r, row in enumerate(now)
        ]
        joined = jnp.stack([row.astype(jnp.bfloat16) for row in now], axis=3)
        results.append(joined.reshape(local_members, count, tile_rows, columns))
    return jnp.concatenate(results, axis=1) if len(results) > 1 else results[0]


def solution(mesh):
    in_specs = (
        P("mem", None, "space", None),
        P("space", None),
        P("space", None),
        P("space", None),
        P("space", None),
        P("space", "mem", None),
        P("space", "mem"),
        P(None, "space", None),
        P(None, "space", None),
        P(),
        P("space", None),
    )
    out_specs = P("mem", None, "space", None)
    return jax.shard_map(shards, mesh=mesh, in_specs=in_specs, out_specs=out_specs, check_vma=False)
```

```python
import functools
import math

import jax
import jax.numpy as jnp
from jax import lax
from jax.experimental import pallas as pl
from jax.experimental.pallas import tpu as pltpu
from jax.sharding import PartitionSpec as P

NEWTON = 8
SUBSTEPS = 2
LOC = 1
LANES = 128
GROUP = 8
PITCH = 40
INTERPRET = False


def lane_product(left, right, depth, rows, width, finish, unroll=4):
    def group(block, carry):
        first = pl.multiple_of(block * GROUP, GROUP)

        def step(k, sums):
            row = right(k)
            return tuple(sums[r] + left(k, first, r) * row for r in range(GROUP))

        zero = jnp.zeros((width, LANES), jnp.float32)
        sums = lax.fori_loop(0, depth, step, (zero,) * GROUP, unroll=unroll)
        finish(first, sums)
        return carry

    lax.fori_loop(0, rows // GROUP, group, 0)


def weights_kernel(
    members, repeats, radius,
    pool_ref, idx_ref, cnt_ref, row_ref, col_ref,
    dev_ref, mix_ref, keep_ref,
    first_v, now_v, step_g, keys, tail, innov, scal,
):
    slots = idx_ref.shape[0]
    pooled = pool_ref.shape[1]
    blocks = slots // GROUP
    info = pool_ref[members:, :]
    high = info.astype(jnp.bfloat16).astype(jnp.float32)
    rest = info - high
    middle = rest.astype(jnp.bfloat16).astype(jnp.float32)
    low = rest - middle
    table = jnp.concatenate([pool_ref[:members, :], high, middle, low, jnp.zeros_like(low)], axis=0)
    table = table.astype(jnp.bfloat16)
    place = lax.broadcasted_iota(jnp.int32, (pooled, LANES), 0)
    extra = info.shape[0]

    def pick(k, total):
        hot = jnp.where(place == idx_ref[pl.ds(k, 1), :], 1.0, 0.0).astype(jnp.bfloat16)
        got = jnp.dot(table, hot, preferred_element_type=jnp.float32)
        equiv = got[:members]
        facts = (
            got[members : members + extra]
            + got[members + extra : members + 2 * extra]
            + got[members + 2 * extra : members + 3 * extra]
        )
        mean = jnp.sum(equiv, axis=0, keepdims=True) * (1.0 / members)
        dist = (facts[2:3] - row_ref[...]) ** 2 + (facts[3:4] - col_ref[...]) ** 2
        rho = jnp.exp(-dist / (2.0 * radius * radius)) / facts[1:2]
        scale = jnp.sqrt(jnp.where(k < cnt_ref[...], rho, 0.0))
        scaled = (equiv - mean) * scale
        dev_ref[pl.ds(k, members, stride=slots), :] = scaled
        innov[pl.ds(k, 1), :] = (facts[0:1] - mean) * scale
        return total + jnp.sum(scaled * scaled, axis=0, keepdims=True)

    spread = lax.fori_loop(0, slots, pick, jnp.zeros((1, LANES), jnp.float32), unroll=2)
    shift = members - 1.0
    inverse = 1.0 / (spread + shift * members)
    level = lax.broadcasted_iota(jnp.int32, (GROUP, LANES), 0)

    def eye(r, value):
        return jnp.where(level == r, value, 0.0)

    def at(ref, i, j, base=0):
        start = i * PITCH + j * GROUP
        start = start if isinstance(start, int) else pl.multiple_of(start, GROUP)
        return ref[pl.ds(base + start, GROUP), :]

    def put(ref, i, parts, base=0):
        for j, part in enumerate(parts):
            ref[pl.ds(base + i * PITCH + j * GROUP, GROUP), :] = part
            if j < i // GROUP:
                ref[pl.ds(base + j * GROUP * PITCH + i, GROUP, stride=PITCH), :] = part

    def product(left, right, depth, finish, unroll=4):
        for pair in range((blocks + 1) // 2):
            groups = sorted({pair, blocks - 1 - pair})

            def step(k, sums):
                wide = [right(k, j) for j in range(groups[-1] + 1)]
                out, spot = [], 0
                for g in groups:
                    for r in range(GROUP):
                        one = left(k, g * GROUP + r)
                        for j in range(g + 1):
                            out.append(sums[spot] + one * wide[j])
                            spot += 1
                return tuple(out)

            zero = jnp.zeros((GROUP, LANES), jnp.float32)
            count = sum((g + 1) * GROUP for g in groups)
            sums = lax.fori_loop(0, depth, step, (zero,) * count, unroll=unroll)
            spot = 0
            for g in groups:
                for r in range(GROUP):
                    finish(g * GROUP + r, sums[spot : spot + g + 1])
                    spot += g + 1

    def square(left, right, finish, left_base=0):
        product(
            lambda k, i: left[pl.ds(left_base + k * PITCH + i, 1), :],
            lambda k, j: at(right, k, j),
            slots, finish,
        )

    def gram_done(i, sums):
        parts = [part * inverse for part in sums]
        put(first_v, i, parts)
        put(now_v, i, parts)

    product(
        lambda k, i: dev_ref[pl.ds(k * slots + i, 1), :],
        lambda k, j: dev_ref[pl.ds(pl.multiple_of(k * slots, slots) + j * GROUP, GROUP), :],
        members, gram_done,
    )

    xi = shift * inverse
    mus = []
    for k in range(repeats):
        mu = 1.5 - 0.5 * xi
        scal[pl.ds(k, 1), :] = xi
        scal[pl.ds(repeats + k, 1), :] = mu
        mus.append(mu)
        xi = xi * mu * mu
    after = mus[-1]
    for k in reversed(range(repeats - 1)):
        scal[pl.ds(2 * repeats + k, 1), :] = after
        after = after * mus[k]
    last_z = after
    area = slots * PITCH

    def forward(n, carry):
        xi = scal[pl.ds(n, 1), :]
        mu = scal[pl.ds(repeats + n, 1), :]
        flat, slope = mu * mu - xi * mu, 0.25 * xi - mu
        base = pl.multiple_of(n * area, GROUP)

        def to_g(i, sums):
            parts = [0.25 * part + slope * at(now_v, i, j) for j, part in enumerate(sums)]
            parts[-1] = parts[-1] + eye(i % GROUP, flat)
            put(step_g, i, parts)

        square(now_v, now_v, to_g)

        def to_v(i, sums):
            put(tail, i, sums)
            put(keys, i, [mu * at(step_g, i, j) - 0.5 * part for j, part in enumerate(sums)], base)

        square(step_g, now_v, to_v)
        now_v[...] = tail[...]
        return carry

    lax.fori_loop(0, repeats - 1, forward, 0)

    after = scal[pl.ds(3 * repeats - 2, 1), :]
    for i in range(slots):
        parts = [-0.5 * at(keys, i, j, (repeats - 2) * area) for j in range(blocks)]
        parts[i // GROUP] = parts[i // GROUP] - eye(i % GROUP, 0.5 * after)
        for j, part in enumerate(parts):
            now_v[pl.ds(i * PITCH + j * GROUP, GROUP), :] = part

    def backward(m, carry):
        n = repeats - 3 - m
        base = pl.multiple_of(n * area, GROUP)
        half = 0.5 * scal[pl.ds(2 * repeats + n, 1), :]

        def to_h(i, sums):
            parts = list(sums)
            parts[-1] = parts[-1] - eye(i % GROUP, half)
            put(tail, i, parts)

        square(keys, now_v, to_h, base)
        now_v[...] = tail[...]
        return carry

    lax.fori_loop(0, repeats - 2, backward, 0)

    def whole(ref, k):
        return ref[pl.ds(pl.multiple_of(k * PITCH, GROUP), slots), :]

    none = jnp.zeros((slots, LANES), jnp.float32)

    def apply(ref):
        def step(k, total):
            return total + innov[pl.ds(k, 1), :] * whole(ref, k)

        return lax.fori_loop(0, slots, step, none)

    for _ in range(2):
        start = innov[...]
        innov[...] = apply(now_v)
        innov[...] = last_z * start + apply(first_v)
    gain = innov[...] * inverse
    factor = math.sqrt(shift) * jnp.sqrt(inverse)
    keep_ref[...] = factor * last_z
    both = factor * inverse

    def to_mix(first, sums):
        for r in range(GROUP):
            mix_ref[pl.ds(pl.multiple_of((first + r) * slots, slots), slots), :] = both * sums[r] + gain

    lane_product(
        lambda k, first, r: dev_ref[pl.ds((first + r) * slots + k, 1), :],
        lambda k: whole(now_v, k), slots, members, slots, to_mix,
    )


def solve_cells(pool, idx, counts, rows, cols, members):
    slots, cells = idx.shape
    lane = lambda height: pl.BlockSpec((height, LANES), lambda c: (0, c))
    square = pltpu.VMEM((slots * PITCH, LANES), jnp.float32)
    return pl.pallas_call(
        functools.partial(weights_kernel, members, NEWTON, LOC),
        grid=(cells // LANES,),
        in_specs=[pl.BlockSpec(pool.shape, lambda c: (0, 0)), lane(slots), lane(1), lane(1), lane(1)],
        out_specs=[lane(members * slots), lane(members * slots), lane(1)],
        out_shape=[
            jax.ShapeDtypeStruct((members * slots, cells), jnp.float32),
            jax.ShapeDtypeStruct((members * slots, cells), jnp.float32),
            jax.ShapeDtypeStruct((1, cells), jnp.float32),
        ],
        scratch_shapes=[square] * 3 + [
            pltpu.VMEM(((NEWTON - 1) * slots * PITCH, LANES), jnp.float32),
            square,
            pltpu.VMEM((slots, LANES), jnp.float32),
            pltpu.VMEM((3 * NEWTON, LANES), jnp.float32),
        ],
        compiler_params=pltpu.CompilerParams(vmem_limit_bytes=40 * 1024 * 1024),
        cost_estimate=pl.CostEstimate(flops=2 * 10**9, bytes_accessed=200 * 10**6, transcendentals=0),
        interpret=INTERPRET,
    )(pool, idx, counts, rows, cols)


def prep_kernel(rows, ens_ref, small_ref, pool_ref, edge_ref, mine_ref, theirs_ref, block, land, spread, send_sems, recv_sems):
    share, fields, _ = mine_ref.shape
    observed = small_ref.shape[1]
    span = fields * rows
    facts = small_ref.shape[0]
    me, place, count = lax.axis_index("mem"), lax.axis_index("space"), lax.axis_size("space")

    def exists(step):
        return (place + step >= 0) & (place + step < count)

    def guard(step, act):
        if step == 0:
            act()
        else:
            pl.when(exists(step))(act)

    ways = [(1, 0), (0, -1), (0, 1), (1, -1), (1, 1)]
    barrier = pltpu.get_barrier_semaphore()

    def target(flip, step):
        return (1 - me if flip else me, place + step)

    for flip, step in ways:
        def greet(flip=flip, step=step):
            pl.semaphore_signal(barrier, inc=1, device_id=target(flip, step), device_id_type=pl.DeviceIdType.MESH)

        guard(step, greet)

    block[pl.ds(share, facts), :] = small_ref[...]
    hot = jnp.where(
        lax.broadcasted_iota(jnp.int32, (LANES, observed), 0).astype(jnp.float32) == small_ref[3:4, :], 1.0, 0.0
    ).astype(jnp.bfloat16)
    wanted = lax.broadcasted_iota(jnp.int32, (span, observed), 0).astype(jnp.float32) == small_ref[4:5, :]

    def look(i, carry):
        got = jnp.dot(
            ens_ref[pl.ds(pl.multiple_of(i * span, span), span), :], hot, preferred_element_type=jnp.float32
        )
        block[pl.ds(i, 1), :] = jnp.sum(jnp.where(wanted, got, 0.0), axis=0, keepdims=True)
        return carry

    lax.fori_loop(0, share, look, 0)

    greeted = 1 + 2 * exists(-1).astype(jnp.int32) + 2 * exists(1).astype(jnp.int32)
    pl.semaphore_wait(barrier, greeted)

    def copy(n):
        flip, step = ways[n]
        return pltpu.make_async_remote_copy(
            src_ref=block, dst_ref=land.at[1 - step, flip],
            send_sem=send_sems.at[n], recv_sem=recv_sems.at[1 - step, flip],
            device_id=target(flip, step), device_id_type=pl.DeviceIdType.MESH,
        )

    for n, (flip, step) in enumerate(ways):
        guard(step, lambda n=n: copy(n).start())

    def split(pair, carry):
        for slot in range(2):
            i = 2 * pair + slot
            spread[slot] = ens_ref[pl.ds(pl.multiple_of(i * span, span), span), :].astype(jnp.float32)
            mine_ref[i] = spread[slot, pl.ds(me, fields, stride=rows), :].astype(jnp.bfloat16)
            theirs_ref[i] = spread[slot, pl.ds(1 - me, fields, stride=rows), :].astype(jnp.bfloat16)
        return carry

    lax.fori_loop(0, share // 2, split, 0)

    for n, (flip, step) in enumerate(ways):
        def arrive(n=n):
            copy(n).wait_send()

        guard(step, arrive)
    for n, (flip, step) in enumerate(ways):
        def landed(n=n):
            copy(n).wait_recv()

        guard(-step, landed)
    for step in (-1, 1):
        def blank(step=step):
            land[1 + step] = jnp.zeros_like(land[1 + step])

        pl.when(jnp.logical_not(exists(step)))(blank)
    line = lax.broadcasted_iota(jnp.int32, (GROUP, observed), 0)
    for part in range(3):
        own = block[...] if part == 1 else land[part, 0]
        lanes = pl.ds(part * observed, observed)
        pool_ref[pl.ds(0, share), lanes] = own[:share]
        pool_ref[pl.ds(share, share), lanes] = land[part, 1, pl.ds(0, share), :]
        pool_ref[pl.ds(2 * share, GROUP), lanes] = own[share : share + GROUP] + jnp.where(
            line == 2, float(rows * (part - 1)), 0.0
        )
        edge_ref[part] = own[share + GROUP :]


def prepare(flat, small, members, fields, rows):
    share = members // 2
    observed = small.shape[1]
    high = share + small.shape[0]
    vmem = pl.BlockSpec(memory_space=pltpu.VMEM)
    return pl.pallas_call(
        functools.partial(prep_kernel, rows),
        in_specs=[vmem] * 2,
        out_specs=[vmem] * 4,
        out_shape=[
            jax.ShapeDtypeStruct((members + GROUP, 3 * observed), jnp.float32),
            jax.ShapeDtypeStruct((3, small.shape[0] - GROUP, observed), jnp.float32),
            jax.ShapeDtypeStruct((share, fields, LANES), jnp.bfloat16),
            jax.ShapeDtypeStruct((share, fields, LANES), jnp.bfloat16),
        ],
        scratch_shapes=[
            pltpu.VMEM((high, observed), jnp.float32),
            pltpu.VMEM((3, 2, high, observed), jnp.float32),
            pltpu.VMEM((2, fields * rows, LANES), jnp.float32),
            pltpu.SemaphoreType.DMA((5,)),
            pltpu.SemaphoreType.DMA((3, 2)),
        ],
        compiler_params=pltpu.CompilerParams(
            vmem_limit_bytes=32 * 1024 * 1024, collective_id=0, has_side_effects=True
        ),
        cost_estimate=pl.CostEstimate(flops=10**8, bytes_accessed=8 * 10**6, transcendentals=0),
        interpret=INTERPRET,
    )(flat, small)


def analysis_kernel(parts, slots, *refs):
    states = refs[:parts]
    dev_ref, mix_ref, keep_ref = refs[parts : parts + 3]
    outs = refs[parts + 3 : 2 * parts + 3]
    anomaly, mapped, mean_ref = refs[2 * parts + 3 :]
    share, width, _ = states[0].shape
    members = share * parts
    total = jnp.zeros((width, LANES), jnp.float32)
    for state in states:
        total = lax.fori_loop(
            0, share, lambda i, t, s=state: t + s[i].astype(jnp.float32), total, unroll=4
        )
    mean = total * (1.0 / members)
    mean_ref[...] = mean
    for part, state in enumerate(states):

        def subtract(i, carry, s=state, base=part * share):
            anomaly[base + i] = s[i].astype(jnp.float32) - mean_ref[...]
            return carry

        lax.fori_loop(0, share, subtract, 0, unroll=4)

    def to_mapped(first, sums):
        for r in range(GROUP):
            mapped[first + r] = sums[r]

    lane_product(
        lambda i, first, r: dev_ref[pl.ds(i * slots + first + r, 1), :],
        lambda i: anomaly[i], members, slots, width, to_mapped,
    )
    for part, out in enumerate(outs):
        base = part * share

        def to_out(first, sums, out=out, base=base):
            for r in range(GROUP):
                held = mean_ref[...] + keep_ref[...] * anomaly[base + first + r]
                out[first + r] = (held + sums[r]).astype(jnp.bfloat16)

        lane_product(
            lambda k, first, r, base=base: mix_ref[pl.ds((base + first + r) * slots + k, 1), :],
            lambda k: mapped[k], slots, share, width, to_out,
        )


def analyse(states, dev, mix, keep, slots, first, count, width):
    share, _, cells = states[0].shape
    parts = len(states)
    members = share * parts
    wide = lambda height: pl.BlockSpec((height, LANES), lambda c, f: (0, c))
    return pl.pallas_call(
        functools.partial(analysis_kernel, parts, slots),
        grid=(cells // LANES, count // width),
        in_specs=[
            pl.BlockSpec((share, width, LANES), lambda c, f: (0, f + first // width, c))
        ] * parts + [wide(members * slots), wide(members * slots), wide(1)],
        out_specs=[pl.BlockSpec((share, width, LANES), lambda c, f: (0, f, c))] * parts,
        out_shape=[jax.ShapeDtypeStruct((share, count, cells), jnp.bfloat16)] * parts,
        scratch_shapes=[
            pltpu.VMEM((members, width, LANES), jnp.float32),
            pltpu.VMEM((slots, width, LANES), jnp.float32),
            pltpu.VMEM((width, LANES), jnp.float32),
        ],
        compiler_params=pltpu.CompilerParams(vmem_limit_bytes=32 * 1024 * 1024),
        cost_estimate=pl.CostEstimate(flops=10**9, bytes_accessed=50 * 10**6, transcendentals=0),
        interpret=INTERPRET,
    )(*states, dev, mix, keep)


def halo(cells, width):
    count = lax.axis_size("space")
    before = lax.ppermute(cells[-width:], "space", [(i, i + 1) for i in range(count - 1)])
    after = lax.ppermute(cells[:width], "space", [(i + 1, i) for i in range(count - 1)])
    return before, after


def wide_rows(cells, width):
    before, after = halo(cells, width)
    return jnp.concatenate([before, cells, after], axis=0)


def row_step(south, middle, north, courant):
    return (
        middle
        - 0.5 * courant * (north - south)
        + 0.5 * courant * courant * (north - 2.0 * middle + south)
    )


def col_step(middle, courant):
    padded = jnp.pad(middle, [(0, 0)] * (middle.ndim - 1) + [(1, 1)])
    east, west = padded[..., 2:], padded[..., :-2]
    return (
        middle
        - 0.5 * courant * (east - west)
        + 0.5 * courant * courant * (east - 2.0 * middle + west)
    )


def shards(
    ensemble, obs_value, obs_error, obs_cell, obs_species, patch_index, patch_count,
    courant_x, courant_y, dep_velocity, surface_factor,
):
    local_members, fields, tile_rows, columns = ensemble.shape
    species = dep_velocity.shape[0]
    levels = fields // species
    tile_cells = tile_rows * columns
    groups = lax.axis_size("mem")
    members = local_members * groups
    me = lax.axis_index("mem")
    slots = patch_index.shape[2]
    per_dev = tile_cells // groups
    paired = groups == 2 and tile_rows == 2 and columns == LANES and GROUP % levels == 0
    swap = [(0, 1), (1, 0)]

    if paired:
        tall = GROUP // levels
        small = jnp.concatenate(
            [
                obs_value,
                obs_error,
                (obs_cell // columns).astype(jnp.float32),
                (obs_cell % columns).astype(jnp.float32),
                (obs_species * (levels * tile_rows) + obs_cell // columns).astype(jnp.float32),
                jnp.zeros((GROUP - 5, obs_value.shape[1]), jnp.float32),
            ]
            + [courant_x.reshape(levels, tile_cells)] * tall
            + [courant_y.reshape(levels, tile_cells)] * tall,
            axis=0,
        )
        pool, edge, mine, theirs = prepare(
            ensemble.reshape(-1, columns), small, members, fields, tile_rows
        )
    else:
        surface = ensemble.reshape(local_members, species, levels, tile_cells)[:, :, 0]
        position = obs_species[0] * tile_cells + obs_cell[0]
        equiv = jnp.take(surface.reshape(local_members, -1), position, axis=1).astype(jnp.float32)
        equiv = lax.all_gather(equiv, "mem", axis=0, tiled=True)
        zeros = jnp.zeros_like(obs_value[0])
        info = jnp.stack(
            [
                obs_value[0],
                obs_error[0],
                (obs_cell[0] // columns).astype(jnp.float32),
                (obs_cell[0] % columns).astype(jnp.float32),
            ]
            + [zeros] * 4
        )
        packed = jnp.concatenate([equiv, info], axis=0)
        before, after = halo(packed[None], 1)
        offset = jnp.zeros((packed.shape[0], 1), jnp.float32).at[members + 2, 0].set(float(tile_rows))
        pool = jnp.concatenate([before[0] - offset, packed, after[0] + offset], axis=1)

    if paired:
        states = (mine, lax.ppermute(theirs, "mem", swap))
    else:
        states = (
            lax.all_to_all(
                ensemble.reshape(local_members, fields, tile_cells),
                "mem", split_axis=2, concat_axis=0, tiled=True,
            ),
        )
    spare = -per_dev % LANES
    pad = lambda a: jnp.pad(a, [(0, 0)] * (a.ndim - 1) + [(0, spare)]) if spare else a
    states = tuple(pad(state) for state in states)
    cell = me * per_dev + jnp.arange(per_dev, dtype=jnp.int32)
    dev, mix, keep = solve_cells(
        pool,
        pad(jnp.transpose(patch_index[0])),
        pad(patch_count),
        pad((cell // columns).astype(jnp.float32)[None]),
        pad((cell % columns).astype(jnp.float32)[None]),
        members,
    )

    width = next(w for w in (32, 16, fields) if fields % w == 0)
    blocks = fields // width
    parts = 2 if paired and blocks > 1 and width % levels == 0 else 1
    cuts = [0, (blocks + 1) // 2 * width, fields] if parts == 2 else [0, fields]
    if paired:
        tiled = edge.reshape(3, 2, GROUP, tile_rows, columns)[:, :, :levels]
        wide_x, wide_y = jnp.moveaxis(tiled, (1, 3), (0, 2)).reshape(2, 3 * tile_rows, levels, columns)
    else:
        wide_x = wide_rows(jnp.moveaxis(courant_x, 1, 0), SUBSTEPS)
        wide_y = wide_rows(jnp.moveaxis(courant_y, 1, 0), SUBSTEPS)
    loss = jnp.exp(-dep_velocity[:, None, None] * surface_factor[None])

    results = []
    for low, high in zip(cuts[:-1], cuts[1:]):
        count = high - low
        out = analyse(states, dev, mix, keep, slots, low, count, width)
        if paired:
            other = lax.ppermute(out[1], "mem", swap)
            rows = jnp.stack([jnp.where(me == 0, out[0], other), jnp.where(me == 0, other, out[0])])
        else:
            back = lax.all_to_all(out[0][..., :per_dev], "mem", split_axis=0, concat_axis=2, tiled=True)
            rows = jnp.moveaxis(back.reshape(local_members, count, tile_rows, columns), 2, 0)
        south, north = halo(rows, SUBSTEPS)
        shape = (local_members, count // levels, levels, columns)
        now = [
            part[r].reshape(shape).astype(jnp.float32)
            for part in (south, rows, north)
            for r in range(part.shape[0])
        ]
        for repeat in range(SUBSTEPS):
            first = repeat + 1
            now = [
                col_step(
                    row_step(now[r - 1], now[r], now[r + 1], wide_y[first + r - 1]),
                    wide_x[first + r - 1],
                )
                for r in range(1, len(now) - 1)
            ]
        part = loss[low // levels : high // levels]
        lowest = (jnp.arange(levels, dtype=jnp.int32) == 0)[:, None]
        now = [
            row * jnp.where(lowest, part[:, r][:, None], 1.0) for r, row in enumerate(now)
        ]
        joined = jnp.stack([row.astype(jnp.bfloat16) for row in now], axis=3)
        results.append(joined.reshape(local_members, count, tile_rows, columns))
    return jnp.concatenate(results, axis=1) if len(results) > 1 else results[0]


def solution(mesh):
    in_specs = (
        P("mem", None, "space", None),
        P("space", None),
        P("space", None),
        P("space", None),
        P("space", None),
        P("space", "mem", None),
        P("space", "mem"),
        P(None, "space", None),
        P(None, "space", None),
        P(),
        P("space", None),
    )
    out_specs = P("mem", None, "space", None)
    return jax.shard_map(shards, mesh=mesh, in_specs=in_specs, out_specs=out_specs, check_vma=False)
```

```python
import functools
import math

import jax
import jax.numpy as jnp
from jax import lax
from jax.experimental import pallas as pl
from jax.experimental.pallas import tpu as pltpu
from jax.sharding import PartitionSpec as P

NEWTON = 8
SUBSTEPS = 2
LOC = 1
LANES = 128
GROUP = 8
PITCH = 40
WIDTH = 16
LAG = 3
INTERPRET = False


def lane_product(left, right, depth, rows, width, finish, unroll=4, group=GROUP):
    def several(block, carry):
        first = pl.multiple_of(block * group, group)

        def step(k, sums):
            row = right(k)
            return tuple(sums[r] + left(k, first, r) * row for r in range(group))

        zero = jnp.zeros((width, LANES), jnp.float32)
        sums = lax.fori_loop(0, depth, step, (zero,) * group, unroll=unroll)
        finish(first, sums)
        return carry

    lax.fori_loop(0, rows // group, several, 0)


def weights_kernel(
    members, repeats, radius,
    pool_ref, idx_ref, cnt_ref, row_ref, col_ref,
    dev_ref, mix_ref, keep_ref,
    first_v, now_v, step_g, keys, tail, innov, scal,
):
    slots = idx_ref.shape[0]
    pooled = pool_ref.shape[1]
    blocks = slots // GROUP
    info = pool_ref[members:, :]
    high = info.astype(jnp.bfloat16).astype(jnp.float32)
    rest = info - high
    middle = rest.astype(jnp.bfloat16).astype(jnp.float32)
    low = rest - middle
    table = jnp.concatenate([pool_ref[:members, :], high, middle, low, jnp.zeros_like(low)], axis=0)
    table = table.astype(jnp.bfloat16)
    place = lax.broadcasted_iota(jnp.int32, (pooled, LANES), 0)
    extra = info.shape[0]

    def pick(k, total):
        hot = jnp.where(place == idx_ref[pl.ds(k, 1), :], 1.0, 0.0).astype(jnp.bfloat16)
        got = jnp.dot(table, hot, preferred_element_type=jnp.float32)
        equiv = got[:members]
        facts = (
            got[members : members + extra]
            + got[members + extra : members + 2 * extra]
            + got[members + 2 * extra : members + 3 * extra]
        )
        mean = jnp.sum(equiv, axis=0, keepdims=True) * (1.0 / members)
        dist = (facts[2:3] - row_ref[...]) ** 2 + (facts[3:4] - col_ref[...]) ** 2
        rho = jnp.exp(-dist / (2.0 * radius * radius)) / facts[1:2]
        scale = jnp.sqrt(jnp.where(k < cnt_ref[...], rho, 0.0))
        scaled = (equiv - mean) * scale
        dev_ref[pl.ds(k, members, stride=slots), :] = scaled
        innov[pl.ds(k, 1), :] = (facts[0:1] - mean) * scale
        return total + jnp.sum(scaled * scaled, axis=0, keepdims=True)

    spread = lax.fori_loop(0, slots, pick, jnp.zeros((1, LANES), jnp.float32), unroll=2)
    shift = members - 1.0
    inverse = 1.0 / (spread + shift * members)
    level = lax.broadcasted_iota(jnp.int32, (GROUP, LANES), 0)

    def eye(r, value):
        return jnp.where(level == r, value, 0.0)

    def at(ref, i, j, base=0):
        start = i * PITCH + j * GROUP
        start = start if isinstance(start, int) else pl.multiple_of(start, GROUP)
        return ref[pl.ds(base + start, GROUP), :]

    def put(ref, i, parts, base=0):
        for j, part in enumerate(parts):
            ref[pl.ds(base + i * PITCH + j * GROUP, GROUP), :] = part
            if j < i // GROUP:
                ref[pl.ds(base + j * GROUP * PITCH + i, GROUP, stride=PITCH), :] = part

    def product(left, right, depth, finish, unroll=4):
        for pair in range((blocks + 1) // 2):
            groups = sorted({pair, blocks - 1 - pair})

            def step(k, sums):
                wide = [right(k, j) for j in range(groups[-1] + 1)]
                out, spot = [], 0
                for g in groups:
                    for r in range(GROUP):
                        one = left(k, g * GROUP + r)
                        for j in range(g + 1):
                            out.append(sums[spot] + one * wide[j])
                            spot += 1
                return tuple(out)

            zero = jnp.zeros((GROUP, LANES), jnp.float32)
            count = sum((g + 1) * GROUP for g in groups)
            sums = lax.fori_loop(0, depth, step, (zero,) * count, unroll=unroll)
            spot = 0
            for g in groups:
                for r in range(GROUP):
                    finish(g * GROUP + r, sums[spot : spot + g + 1])
                    spot += g + 1

    def square(left, right, finish, left_base=0):
        product(
            lambda k, i: left[pl.ds(left_base + k * PITCH + i, 1), :],
            lambda k, j: at(right, k, j),
            slots, finish,
        )

    def gram_done(i, sums):
        parts = [part * inverse for part in sums]
        put(first_v, i, parts)
        put(now_v, i, parts)

    product(
        lambda k, i: dev_ref[pl.ds(k * slots + i, 1), :],
        lambda k, j: dev_ref[pl.ds(pl.multiple_of(k * slots, slots) + j * GROUP, GROUP), :],
        members, gram_done,
    )

    xi = shift * inverse
    mus = []
    for k in range(repeats):
        mu = 1.5 - 0.5 * xi
        scal[pl.ds(k, 1), :] = xi
        scal[pl.ds(repeats + k, 1), :] = mu
        mus.append(mu)
        xi = xi * mu * mu
    after = mus[-1]
    for k in reversed(range(repeats - 1)):
        scal[pl.ds(2 * repeats + k, 1), :] = after
        after = after * mus[k]
    last_z = after
    area = slots * PITCH

    def forward(n, carry):
        xi = scal[pl.ds(n, 1), :]
        mu = scal[pl.ds(repeats + n, 1), :]
        flat, slope = mu * mu - xi * mu, 0.25 * xi - mu
        base = pl.multiple_of(n * area, GROUP)

        def to_g(i, sums):
            parts = [0.25 * part + slope * at(now_v, i, j) for j, part in enumerate(sums)]
            parts[-1] = parts[-1] + eye(i % GROUP, flat)
            put(step_g, i, parts)

        square(now_v, now_v, to_g)

        def to_v(i, sums):
            put(tail, i, sums)
            put(keys, i, [mu * at(step_g, i, j) - 0.5 * part for j, part in enumerate(sums)], base)

        square(step_g, now_v, to_v)
        now_v[...] = tail[...]
        return carry

    lax.fori_loop(0, repeats - 1, forward, 0)

    after = scal[pl.ds(3 * repeats - 2, 1), :]
    for i in range(slots):
        parts = [-0.5 * at(keys, i, j, (repeats - 2) * area) for j in range(blocks)]
        parts[i // GROUP] = parts[i // GROUP] - eye(i % GROUP, 0.5 * after)
        for j, part in enumerate(parts):
            now_v[pl.ds(i * PITCH + j * GROUP, GROUP), :] = part

    def backward(m, carry):
        n = repeats - 3 - m
        base = pl.multiple_of(n * area, GROUP)
        half = 0.5 * scal[pl.ds(2 * repeats + n, 1), :]

        def to_h(i, sums):
            parts = list(sums)
            parts[-1] = parts[-1] - eye(i % GROUP, half)
            put(tail, i, parts)

        square(keys, now_v, to_h, base)
        now_v[...] = tail[...]
        return carry

    lax.fori_loop(0, repeats - 2, backward, 0)

    def whole(ref, k):
        return ref[pl.ds(pl.multiple_of(k * PITCH, GROUP), slots), :]

    none = jnp.zeros((slots, LANES), jnp.float32)

    def apply(ref):
        def step(k, total):
            return total + innov[pl.ds(k, 1), :] * whole(ref, k)

        return lax.fori_loop(0, slots, step, none)

    for _ in range(2):
        start = innov[...]
        innov[...] = apply(now_v)
        innov[...] = last_z * start + apply(first_v)
    gain = innov[...] * inverse
    factor = math.sqrt(shift) * jnp.sqrt(inverse)
    keep_ref[...] = factor * last_z
    both = factor * inverse

    def to_mix(first, sums):
        for r in range(GROUP):
            mix_ref[pl.ds(pl.multiple_of((first + r) * slots, slots), slots), :] = both * sums[r] + gain

    lane_product(
        lambda k, first, r: dev_ref[pl.ds((first + r) * slots + k, 1), :],
        lambda k: whole(now_v, k), slots, members, slots, to_mix,
    )


def solve_cells(pool, idx, counts, rows, cols, members):
    slots, cells = idx.shape
    lane = lambda height: pl.BlockSpec((height, LANES), lambda c: (0, c))
    square = pltpu.VMEM((slots * PITCH, LANES), jnp.float32)
    return pl.pallas_call(
        functools.partial(weights_kernel, members, NEWTON, LOC),
        grid=(cells // LANES,),
        in_specs=[pl.BlockSpec(pool.shape, lambda c: (0, 0)), lane(slots), lane(1), lane(1), lane(1)],
        out_specs=[lane(members * slots), lane(members * slots), lane(1)],
        out_shape=[
            jax.ShapeDtypeStruct((members * slots, cells), jnp.float32),
            jax.ShapeDtypeStruct((members * slots, cells), jnp.float32),
            jax.ShapeDtypeStruct((1, cells), jnp.float32),
        ],
        scratch_shapes=[square] * 3 + [
            pltpu.VMEM(((NEWTON - 1) * slots * PITCH, LANES), jnp.float32),
            square,
            pltpu.VMEM((slots, LANES), jnp.float32),
            pltpu.VMEM((3 * NEWTON, LANES), jnp.float32),
        ],
        compiler_params=pltpu.CompilerParams(vmem_limit_bytes=40 * 1024 * 1024),
        cost_estimate=pl.CostEstimate(flops=2 * 10**9, bytes_accessed=200 * 10**6, transcendentals=0),
        interpret=INTERPRET,
    )(pool, idx, counts, rows, cols)


def prep_kernel(rows, ens_ref, small_ref, pool_ref, edge_ref, mine_ref, theirs_ref, block, land, spread, send_sems, recv_sems):
    share, fields, _ = mine_ref.shape
    observed = small_ref.shape[1]
    span = fields * rows
    facts = small_ref.shape[0]
    me, place, count = lax.axis_index("mem"), lax.axis_index("space"), lax.axis_size("space")

    def exists(step):
        return (place + step >= 0) & (place + step < count)

    def guard(step, act):
        if step == 0:
            act()
        else:
            pl.when(exists(step))(act)

    ways = [(1, 0), (0, -1), (0, 1), (1, -1), (1, 1)]
    barrier = pltpu.get_barrier_semaphore()

    def target(flip, step):
        return (1 - me if flip else me, place + step)

    for flip, step in ways:
        def greet(flip=flip, step=step):
            pl.semaphore_signal(barrier, inc=1, device_id=target(flip, step), device_id_type=pl.DeviceIdType.MESH)

        guard(step, greet)

    block[pl.ds(share, facts), :] = small_ref[...]
    hot = jnp.where(
        lax.broadcasted_iota(jnp.int32, (LANES, observed), 0).astype(jnp.float32) == small_ref[3:4, :], 1.0, 0.0
    ).astype(jnp.bfloat16)
    wanted = lax.broadcasted_iota(jnp.int32, (span, observed), 0).astype(jnp.float32) == small_ref[4:5, :]

    def look(i, carry):
        got = jnp.dot(
            ens_ref[pl.ds(pl.multiple_of(i * span, span), span), :], hot, preferred_element_type=jnp.float32
        )
        block[pl.ds(i, 1), :] = jnp.sum(jnp.where(wanted, got, 0.0), axis=0, keepdims=True)
        return carry

    lax.fori_loop(0, share, look, 0)

    greeted = 1 + 2 * exists(-1).astype(jnp.int32) + 2 * exists(1).astype(jnp.int32)
    pl.semaphore_wait(barrier, greeted)

    def copy(n):
        flip, step = ways[n]
        return pltpu.make_async_remote_copy(
            src_ref=block, dst_ref=land.at[1 - step, flip],
            send_sem=send_sems.at[n], recv_sem=recv_sems.at[1 - step, flip],
            device_id=target(flip, step), device_id_type=pl.DeviceIdType.MESH,
        )

    for n, (flip, step) in enumerate(ways):
        guard(step, lambda n=n: copy(n).start())

    def split(pair, carry):
        for slot in range(2):
            i = 2 * pair + slot
            spread[slot] = ens_ref[pl.ds(pl.multiple_of(i * span, span), span), :].astype(jnp.float32)
            mine_ref[i] = spread[slot, pl.ds(me, fields, stride=rows), :].astype(jnp.bfloat16)
            theirs_ref[i] = spread[slot, pl.ds(1 - me, fields, stride=rows), :].astype(jnp.bfloat16)
        return carry

    lax.fori_loop(0, share // 2, split, 0)

    for n, (flip, step) in enumerate(ways):
        def arrive(n=n):
            copy(n).wait_send()

        guard(step, arrive)
    for n, (flip, step) in enumerate(ways):
        def landed(n=n):
            copy(n).wait_recv()

        guard(-step, landed)
    for step in (-1, 1):
        def blank(step=step):
            land[1 + step] = jnp.zeros_like(land[1 + step])

        pl.when(jnp.logical_not(exists(step)))(blank)
    line = lax.broadcasted_iota(jnp.int32, (GROUP, observed), 0)
    for part in range(3):
        own = block[...] if part == 1 else land[part, 0]
        lanes = pl.ds(part * observed, observed)
        pool_ref[pl.ds(0, share), lanes] = own[:share]
        pool_ref[pl.ds(share, share), lanes] = land[part, 1, pl.ds(0, share), :]
        pool_ref[pl.ds(2 * share, GROUP), lanes] = own[share : share + GROUP] + jnp.where(
            line == 2, float(rows * (part - 1)), 0.0
        )
        edge_ref[part] = own[share + GROUP :]


def prepare(flat, small, members, fields, rows):
    share = members // 2
    observed = small.shape[1]
    high = share + small.shape[0]
    vmem = pl.BlockSpec(memory_space=pltpu.VMEM)
    return pl.pallas_call(
        functools.partial(prep_kernel, rows),
        in_specs=[vmem] * 2,
        out_specs=[vmem] * 4,
        out_shape=[
            jax.ShapeDtypeStruct((members + GROUP, 3 * observed), jnp.float32),
            jax.ShapeDtypeStruct((3, small.shape[0] - GROUP, observed), jnp.float32),
            jax.ShapeDtypeStruct((share, fields, LANES), jnp.bfloat16),
            jax.ShapeDtypeStruct((share, fields, LANES), jnp.bfloat16),
        ],
        scratch_shapes=[
            pltpu.VMEM((high, observed), jnp.float32),
            pltpu.VMEM((3, 2, high, observed), jnp.float32),
            pltpu.VMEM((2, fields * rows, LANES), jnp.float32),
            pltpu.SemaphoreType.DMA((5,)),
            pltpu.SemaphoreType.DMA((3, 2)),
        ],
        compiler_params=pltpu.CompilerParams(
            vmem_limit_bytes=32 * 1024 * 1024, collective_id=0, has_side_effects=True
        ),
        cost_estimate=pl.CostEstimate(flops=10**8, bytes_accessed=8 * 10**6, transcendentals=0),
        interpret=INTERPRET,
    )(flat, small)


def analysis_kernel(parts, slots, *refs):
    states = refs[:parts]
    dev_ref, mix_ref, keep_ref = refs[parts : parts + 3]
    outs = refs[parts + 3 : 2 * parts + 3]
    anomaly, mapped, mean_ref = refs[2 * parts + 3 :]
    share, width, _ = states[0].shape
    members = share * parts
    total = jnp.zeros((width, LANES), jnp.float32)
    for state in states:
        total = lax.fori_loop(
            0, share, lambda i, t, s=state: t + s[i].astype(jnp.float32), total, unroll=4
        )
    mean = total * (1.0 / members)
    mean_ref[...] = mean
    for part, state in enumerate(states):

        def subtract(i, carry, s=state, base=part * share):
            anomaly[base + i] = s[i].astype(jnp.float32) - mean_ref[...]
            return carry

        lax.fori_loop(0, share, subtract, 0, unroll=4)

    def to_mapped(first, sums):
        for r in range(GROUP):
            mapped[first + r] = sums[r]

    lane_product(
        lambda i, first, r: dev_ref[pl.ds(i * slots + first + r, 1), :],
        lambda i: anomaly[i], members, slots, width, to_mapped,
    )
    for part, out in enumerate(outs):
        base = part * share

        def to_out(first, sums, out=out, base=base):
            for r in range(GROUP):
                held = mean_ref[...] + keep_ref[...] * anomaly[base + first + r]
                out[first + r] = (held + sums[r]).astype(jnp.bfloat16)

        lane_product(
            lambda k, first, r, base=base: mix_ref[pl.ds((base + first + r) * slots + k, 1), :],
            lambda k: mapped[k], slots, share, width, to_out,
        )


def finish_kernel(
    slots, width,
    mine_ref, other_ref, dev_ref, mix_ref, keep_ref, edge_ref, loss_ref, out_ref,
    rows, away, south, north, anomaly, mapped, mean_ref, coef, weave,
    away_sent, away_come, edge_sent, edge_come,
):
    share, fields, _ = mine_ref.shape
    members = 2 * share
    chunks = fields // width
    group = 2 * LANES // width
    me, place, count = lax.axis_index("mem"), lax.axis_index("space"), lax.axis_size("space")
    mesh_id = pl.DeviceIdType.MESH
    exists = (place > 0, place + 1 < count)
    sides = ((1 - me, place), (me, place - 1), (me, place + 1))
    barrier = pltpu.get_barrier_semaphore()
    pl.semaphore_signal(barrier, inc=1, device_id=sides[0], device_id_type=mesh_id)
    for side in range(2):
        @pl.when(exists[side])
        def _():
            pl.semaphore_signal(barrier, inc=1, device_id=sides[1 + side], device_id_type=mesh_id)

    for side, buffer in enumerate((south, north)):
        @pl.when(jnp.logical_not(exists[side]))
        def _():
            def clear(n, carry):
                for r in range(2):
                    buffer[r, n // share, n % share] = jnp.zeros((width, LANES), jnp.bfloat16)
                return carry

            lax.fori_loop(0, chunks * share, clear, 0)

    lane = lax.broadcasted_iota(jnp.int32, (GROUP, LANES), 1)
    for at, (part, r) in enumerate(((0, 1), (1, 0), (1, 1), (2, 0))):
        cut = pl.ds(r * LANES, LANES)
        cx = edge_ref[part, pl.ds(0, GROUP), cut]
        cy = edge_ref[part, pl.ds(GROUP, GROUP), cut]
        six = (
            1.0 - cy * cy,
            0.5 * cy * cy - 0.5 * cy,
            0.5 * cy * cy + 0.5 * cy,
            1.0 - cx * cx,
            jnp.where(lane == LANES - 1, 0.0, 0.5 * cx * cx - 0.5 * cx),
            jnp.where(lane == 0, 0.0, 0.5 * cx * cx + 0.5 * cx),
        )
        for n, value in enumerate(six):
            for piece in range(width // GROUP):
                coef[6 * at + n, pl.ds(piece * GROUP, GROUP), :] = value

    greeted = 1 + exists[0].astype(jnp.int32) + exists[1].astype(jnp.int32)
    pl.semaphore_wait(barrier, greeted)

    def swap(q):
        return pltpu.make_async_remote_copy(
            src_ref=away.at[q], dst_ref=rows.at[me, q],
            send_sem=away_sent.at[q], recv_sem=away_come.at[q],
            device_id=sides[0], device_id_type=mesh_id,
        )

    def pass_on(side, r, q):
        return pltpu.make_async_remote_copy(
            src_ref=rows.at[r, q], dst_ref=(north, south)[side].at[r, q],
            send_sem=edge_sent.at[side, r, q], recv_sem=edge_come.at[side, r, q],
            device_id=sides[1 + side], device_id_type=mesh_id,
        )

    def pass_both(r, q):
        for side in range(2):
            @pl.when(exists[side])
            def _():
                pass_on(side, r, q).start()

    def analyse_chunk(q):
        cut = pl.ds(pl.multiple_of(q * width, width), width)
        total = jnp.zeros((width, LANES), jnp.float32)
        for state in (mine_ref, other_ref):
            total = lax.fori_loop(
                0, share, lambda i, t, s=state: t + s[i, cut, :].astype(jnp.float32), total, unroll=4
            )
        mean_ref[...] = total * (1.0 / members)
        for part, state in enumerate((mine_ref, other_ref)):
            def subtract(i, carry, s=state, base=part * share):
                anomaly[base + i] = s[i, cut, :].astype(jnp.float32) - mean_ref[...]
                return carry

            lax.fori_loop(0, share, subtract, 0, unroll=4)

        def to_mapped(first, sums):
            for r in range(group):
                mapped[first + r] = sums[r]

        lane_product(
            lambda i, first, r: dev_ref[pl.ds(i * slots + first + r, 1), :],
            lambda i: anomaly[i], members, slots, width, to_mapped, group=group,
        )
        for part in (1, 0):
            base = part * share

            def to_out(first, sums, base=base, part=part):
                for r in range(group):
                    held = mean_ref[...] + keep_ref[...] * anomaly[base + first + r]
                    value = (held + sums[r]).astype(jnp.bfloat16)
                    if part:
                        away[q, first + r] = value
                    else:
                        rows[me, q, first + r] = value

            lane_product(
                lambda k, first, r, base=base: mix_ref[pl.ds((base + first + r) * slots + k, 1), :],
                lambda k: mapped[k], slots, share, width, to_out, group=group,
            )
            if part:
                swap(q).start()
            else:
                pass_both(me, q)

    def advect_chunk(q):
        cut = pl.ds(pl.multiple_of(q * width, width), width)

        def along(at, low, middle, high):
            now = coef[6 * at] * middle + coef[6 * at + 1] * high + coef[6 * at + 2] * low
            east = pltpu.roll(now, LANES - 1, 1)
            west = pltpu.roll(now, 1, 1)
            return coef[6 * at + 3] * now + coef[6 * at + 4] * east + coef[6 * at + 5] * west

        def pair(n, carry):
            for slot in range(2):
                i = 2 * n + slot
                now = [
                    part[r, q, i].astype(jnp.float32) for part in (south, rows, north) for r in range(2)
                ]
                now = [along(at, *now[at : at + 3]) for at in range(4)]
                now = [along(1 + at, *now[at : at + 3]) for at in range(2)]
                for r in range(2):
                    weave[slot, pl.ds(r, width, stride=2), :] = now[r] * loss_ref[r, cut, :]
                start = pl.multiple_of((i * fields + q * width) * 2, 2 * width)
                out_ref[pl.ds(start, 2 * width), :] = weave[slot].astype(jnp.bfloat16)
            return carry

        lax.fori_loop(0, share // 2, pair, 0)

    def step(q, carry):
        @pl.when(q < chunks)
        def _():
            analyse_chunk(q)

        @pl.when((q >= 1) & (q - 1 < chunks))
        def _():
            swap(q - 1).wait_recv()
            pass_both(1 - me, q - 1)

        @pl.when((q >= LAG) & (q - LAG < chunks))
        def _():
            for side in range(2):
                @pl.when(exists[1 - side])
                def _():
                    for r in range(2):
                        pass_on(side, r, q - LAG).wait_recv()

            advect_chunk(q - LAG)

        return carry

    lax.fori_loop(0, chunks + LAG, step, 0)

    def drain(q, carry):
        swap(q).wait_send()
        for side in range(2):
            @pl.when(exists[side])
            def _():
                for r in range(2):
                    pass_on(side, r, q).wait_send()

        return carry

    lax.fori_loop(0, chunks, drain, 0)


def finish(mine, other, dev, mix, keep, edge, loss, slots, rows):
    share, fields, _ = mine.shape
    width = WIDTH
    chunks = fields // width
    vmem = pl.BlockSpec(memory_space=pltpu.VMEM)
    piece = (chunks, share, width, LANES)
    return pl.pallas_call(
        functools.partial(finish_kernel, slots, width),
        in_specs=[vmem] * 7,
        out_specs=vmem,
        out_shape=jax.ShapeDtypeStruct((share * fields * rows, LANES), jnp.bfloat16),
        scratch_shapes=[
            pltpu.VMEM((2,) + piece, jnp.bfloat16),
            pltpu.VMEM(piece, jnp.bfloat16),
            pltpu.VMEM((2,) + piece, jnp.bfloat16),
            pltpu.VMEM((2,) + piece, jnp.bfloat16),
            pltpu.VMEM((2 * share, width, LANES), jnp.float32),
            pltpu.VMEM((slots, width, LANES), jnp.float32),
            pltpu.VMEM((width, LANES), jnp.float32),
            pltpu.VMEM((24, width, LANES), jnp.float32),
            pltpu.VMEM((2, 2 * width, LANES), jnp.float32),
            pltpu.SemaphoreType.DMA((chunks,)),
            pltpu.SemaphoreType.DMA((chunks,)),
            pltpu.SemaphoreType.DMA((2, 2, chunks)),
            pltpu.SemaphoreType.DMA((2, 2, chunks)),
        ],
        compiler_params=pltpu.CompilerParams(
            vmem_limit_bytes=40 * 1024 * 1024, collective_id=1, has_side_effects=True
        ),
        cost_estimate=pl.CostEstimate(flops=10**9, bytes_accessed=10**7, transcendentals=0),
        interpret=INTERPRET,
    )(mine, other, dev, mix, keep, edge, loss)


def analyse(states, dev, mix, keep, slots, first, count, width):
    share, _, cells = states[0].shape
    parts = len(states)
    members = share * parts
    wide = lambda height: pl.BlockSpec((height, LANES), lambda c, f: (0, c))
    return pl.pallas_call(
        functools.partial(analysis_kernel, parts, slots),
        grid=(cells // LANES, count // width),
        in_specs=[
            pl.BlockSpec((share, width, LANES), lambda c, f: (0, f + first // width, c))
        ] * parts + [wide(members * slots), wide(members * slots), wide(1)],
        out_specs=[pl.BlockSpec((share, width, LANES), lambda c, f: (0, f, c))] * parts,
        out_shape=[jax.ShapeDtypeStruct((share, count, cells), jnp.bfloat16)] * parts,
        scratch_shapes=[
            pltpu.VMEM((members, width, LANES), jnp.float32),
            pltpu.VMEM((slots, width, LANES), jnp.float32),
            pltpu.VMEM((width, LANES), jnp.float32),
        ],
        compiler_params=pltpu.CompilerParams(vmem_limit_bytes=32 * 1024 * 1024),
        cost_estimate=pl.CostEstimate(flops=10**9, bytes_accessed=50 * 10**6, transcendentals=0),
        interpret=INTERPRET,
    )(*states, dev, mix, keep)


def halo(cells, width):
    count = lax.axis_size("space")
    before = lax.ppermute(cells[-width:], "space", [(i, i + 1) for i in range(count - 1)])
    after = lax.ppermute(cells[:width], "space", [(i + 1, i) for i in range(count - 1)])
    return before, after


def wide_rows(cells, width):
    before, after = halo(cells, width)
    return jnp.concatenate([before, cells, after], axis=0)


def row_step(south, middle, north, courant):
    return (
        middle
        - 0.5 * courant * (north - south)
        + 0.5 * courant * courant * (north - 2.0 * middle + south)
    )


def col_step(middle, courant):
    padded = jnp.pad(middle, [(0, 0)] * (middle.ndim - 1) + [(1, 1)])
    east, west = padded[..., 2:], padded[..., :-2]
    return (
        middle
        - 0.5 * courant * (east - west)
        + 0.5 * courant * courant * (east - 2.0 * middle + west)
    )


def shards(
    ensemble, obs_value, obs_error, obs_cell, obs_species, patch_index, patch_count,
    courant_x, courant_y, dep_velocity, surface_factor,
):
    local_members, fields, tile_rows, columns = ensemble.shape
    species = dep_velocity.shape[0]
    levels = fields // species
    tile_cells = tile_rows * columns
    groups = lax.axis_size("mem")
    members = local_members * groups
    me = lax.axis_index("mem")
    slots = patch_index.shape[2]
    per_dev = tile_cells // groups
    paired = groups == 2 and tile_rows == 2 and columns == LANES
    paired = paired and GROUP % levels == 0 and fields % WIDTH == 0
    swap = [(0, 1), (1, 0)]

    if paired:
        tall = GROUP // levels
        small = jnp.concatenate(
            [
                obs_value,
                obs_error,
                (obs_cell // columns).astype(jnp.float32),
                (obs_cell % columns).astype(jnp.float32),
                (obs_species * (levels * tile_rows) + obs_cell // columns).astype(jnp.float32),
                jnp.zeros((GROUP - 5, obs_value.shape[1]), jnp.float32),
            ]
            + [courant_x.reshape(levels, tile_cells)] * tall
            + [courant_y.reshape(levels, tile_cells)] * tall,
            axis=0,
        )
        pool, edge, mine, theirs = prepare(
            ensemble.reshape(-1, columns), small, members, fields, tile_rows
        )
    else:
        surface = ensemble.reshape(local_members, species, levels, tile_cells)[:, :, 0]
        position = obs_species[0] * tile_cells + obs_cell[0]
        equiv = jnp.take(surface.reshape(local_members, -1), position, axis=1).astype(jnp.float32)
        equiv = lax.all_gather(equiv, "mem", axis=0, tiled=True)
        zeros = jnp.zeros_like(obs_value[0])
        info = jnp.stack(
            [
                obs_value[0],
                obs_error[0],
                (obs_cell[0] // columns).astype(jnp.float32),
                (obs_cell[0] % columns).astype(jnp.float32),
            ]
            + [zeros] * 4
        )
        packed = jnp.concatenate([equiv, info], axis=0)
        before, after = halo(packed[None], 1)
        offset = jnp.zeros((packed.shape[0], 1), jnp.float32).at[members + 2, 0].set(float(tile_rows))
        pool = jnp.concatenate([before[0] - offset, packed, after[0] + offset], axis=1)

    if paired:
        states = (mine, lax.ppermute(theirs, "mem", swap))
    else:
        states = (
            lax.all_to_all(
                ensemble.reshape(local_members, fields, tile_cells),
                "mem", split_axis=2, concat_axis=0, tiled=True,
            ),
        )
    spare = -per_dev % LANES
    pad = lambda a: jnp.pad(a, [(0, 0)] * (a.ndim - 1) + [(0, spare)]) if spare else a
    states = tuple(pad(state) for state in states)
    cell = me * per_dev + jnp.arange(per_dev, dtype=jnp.int32)
    dev, mix, keep = solve_cells(
        pool,
        pad(jnp.transpose(patch_index[0])),
        pad(patch_count),
        pad((cell // columns).astype(jnp.float32)[None]),
        pad((cell % columns).astype(jnp.float32)[None]),
        members,
    )

    loss = jnp.exp(-dep_velocity[:, None, None] * surface_factor[None])
    if paired:
        lowest = (jnp.arange(levels, dtype=jnp.int32) == 0)[None, None, :, None]
        factor = jnp.where(lowest, jnp.moveaxis(loss, 1, 0)[:, :, None], 1.0).reshape(tile_rows, fields, columns)
        out = finish(*states, dev, mix, keep, edge, factor, slots, tile_rows)
        return out.reshape(ensemble.shape)

    width = next(w for w in (32, 16, fields) if fields % w == 0)
    wide_x = wide_rows(jnp.moveaxis(courant_x, 1, 0), SUBSTEPS)
    wide_y = wide_rows(jnp.moveaxis(courant_y, 1, 0), SUBSTEPS)
    out = analyse(states, dev, mix, keep, slots, 0, fields, width)
    back = lax.all_to_all(out[0][..., :per_dev], "mem", split_axis=0, concat_axis=2, tiled=True)
    rows = jnp.moveaxis(back.reshape(local_members, fields, tile_rows, columns), 2, 0)
    south, north = halo(rows, SUBSTEPS)
    shape = (local_members, species, levels, columns)
    now = [
        part[r].reshape(shape).astype(jnp.float32)
        for part in (south, rows, north)
        for r in range(part.shape[0])
    ]
    for repeat in range(SUBSTEPS):
        first = repeat + 1
        now = [
            col_step(
                row_step(now[r - 1], now[r], now[r + 1], wide_y[first + r - 1]),
                wide_x[first + r - 1],
            )
            for r in range(1, len(now) - 1)
        ]
    lowest = (jnp.arange(levels, dtype=jnp.int32) == 0)[:, None]
    now = [row * jnp.where(lowest, loss[:, r][:, None], 1.0) for r, row in enumerate(now)]
    joined = jnp.stack([row.astype(jnp.bfloat16) for row in now], axis=3)
    return joined.reshape(local_members, fields, tile_rows, columns)


def solution(mesh):
    in_specs = (
        P("mem", None, "space", None),
        P("space", None),
        P("space", None),
        P("space", None),
        P("space", None),
        P("space", "mem", None),
        P("space", "mem"),
        P(None, "space", None),
        P(None, "space", None),
        P(),
        P("space", None),
    )
    out_specs = P("mem", None, "space", None)
    return jax.shard_map(shards, mesh=mesh, in_specs=in_specs, out_specs=out_specs, check_vma=False)
```

```python
import functools
import math

import jax
import jax.numpy as jnp
from jax import lax
from jax.experimental import pallas as pl
from jax.experimental.pallas import tpu as pltpu
from jax.sharding import PartitionSpec as P

NEWTON = 8
SUBSTEPS = 2
LOC = 1
LANES = 128
GROUP = 8
PITCH = 40
WIDTH = 16
LAG = 3
UNROLL = 4
INTERPRET = False


def lane_product(left, right, depth, rows, width, finish, unroll=4, group=GROUP):
    def several(block, carry):
        first = pl.multiple_of(block * group, group)

        def step(k, sums):
            row = right(k)
            return tuple(sums[r] + left(k, first, r) * row for r in range(group))

        zero = jnp.zeros((width, LANES), jnp.float32)
        sums = lax.fori_loop(0, depth, step, (zero,) * group, unroll=unroll)
        finish(first, sums)
        return carry

    lax.fori_loop(0, rows // group, several, 0)


def weights_kernel(
    members, repeats, radius,
    pool_ref, idx_ref, cnt_ref, row_ref, col_ref,
    dev_ref, mix_ref, keep_ref,
    first_v, now_v, step_g, keys, tail, innov, scal,
):
    slots = idx_ref.shape[0]
    pooled = pool_ref.shape[1]
    blocks = slots // GROUP
    info = pool_ref[members:, :]
    high = info.astype(jnp.bfloat16).astype(jnp.float32)
    rest = info - high
    middle = rest.astype(jnp.bfloat16).astype(jnp.float32)
    low = rest - middle
    table = jnp.concatenate([pool_ref[:members, :], high, middle, low, jnp.zeros_like(low)], axis=0)
    table = table.astype(jnp.bfloat16)
    place = lax.broadcasted_iota(jnp.int32, (pooled, LANES), 0)
    extra = info.shape[0]

    def pick(k, total):
        hot = jnp.where(place == idx_ref[pl.ds(k, 1), :], 1.0, 0.0).astype(jnp.bfloat16)
        got = jnp.dot(table, hot, preferred_element_type=jnp.float32)
        equiv = got[:members]
        facts = (
            got[members : members + extra]
            + got[members + extra : members + 2 * extra]
            + got[members + 2 * extra : members + 3 * extra]
        )
        mean = jnp.sum(equiv, axis=0, keepdims=True) * (1.0 / members)
        dist = (facts[2:3] - row_ref[...]) ** 2 + (facts[3:4] - col_ref[...]) ** 2
        rho = jnp.exp(-dist / (2.0 * radius * radius)) / facts[1:2]
        scale = jnp.sqrt(jnp.where(k < cnt_ref[...], rho, 0.0))
        scaled = (equiv - mean) * scale
        dev_ref[pl.ds(k, members, stride=slots), :] = scaled
        innov[pl.ds(k, 1), :] = (facts[0:1] - mean) * scale
        return total + jnp.sum(scaled * scaled, axis=0, keepdims=True)

    spread = lax.fori_loop(0, slots, pick, jnp.zeros((1, LANES), jnp.float32), unroll=2)
    shift = members - 1.0
    inverse = 1.0 / (spread + shift * members)
    level = lax.broadcasted_iota(jnp.int32, (GROUP, LANES), 0)

    def eye(r, value):
        return jnp.where(level == r, value, 0.0)

    def at(ref, i, j, base=0):
        start = i * PITCH + j * GROUP
        start = start if isinstance(start, int) else pl.multiple_of(start, GROUP)
        return ref[pl.ds(base + start, GROUP), :]

    def put(ref, i, parts, base=0):
        for j, part in enumerate(parts):
            ref[pl.ds(base + i * PITCH + j * GROUP, GROUP), :] = part
            if j < i // GROUP:
                ref[pl.ds(base + j * GROUP * PITCH + i, GROUP, stride=PITCH), :] = part

    def product(left, right, depth, finish, unroll=4):
        for pair in range((blocks + 1) // 2):
            groups = sorted({pair, blocks - 1 - pair})

            def step(k, sums):
                wide = [right(k, j) for j in range(groups[-1] + 1)]
                out, spot = [], 0
                for g in groups:
                    for r in range(GROUP):
                        one = left(k, g * GROUP + r)
                        for j in range(g + 1):
                            out.append(sums[spot] + one * wide[j])
                            spot += 1
                return tuple(out)

            zero = jnp.zeros((GROUP, LANES), jnp.float32)
            count = sum((g + 1) * GROUP for g in groups)
            sums = lax.fori_loop(0, depth, step, (zero,) * count, unroll=unroll)
            spot = 0
            for g in groups:
                for r in range(GROUP):
                    finish(g * GROUP + r, sums[spot : spot + g + 1])
                    spot += g + 1

    def square(left, right, finish, left_base=0):
        product(
            lambda k, i: left[pl.ds(left_base + k * PITCH + i, 1), :],
            lambda k, j: at(right, k, j),
            slots, finish,
        )

    def gram_done(i, sums):
        parts = [part * inverse for part in sums]
        put(first_v, i, parts)
        put(now_v, i, parts)

    product(
        lambda k, i: dev_ref[pl.ds(k * slots + i, 1), :],
        lambda k, j: dev_ref[pl.ds(pl.multiple_of(k * slots, slots) + j * GROUP, GROUP), :],
        members, gram_done,
    )

    xi = shift * inverse
    mus = []
    for k in range(repeats):
        mu = 1.5 - 0.5 * xi
        scal[pl.ds(k, 1), :] = xi
        scal[pl.ds(repeats + k, 1), :] = mu
        mus.append(mu)
        xi = xi * mu * mu
    after = mus[-1]
    for k in reversed(range(repeats - 1)):
        scal[pl.ds(2 * repeats + k, 1), :] = after
        after = after * mus[k]
    last_z = after
    area = slots * PITCH

    def forward(n, carry):
        xi = scal[pl.ds(n, 1), :]
        mu = scal[pl.ds(repeats + n, 1), :]
        flat, slope = mu * mu - xi * mu, 0.25 * xi - mu
        base = pl.multiple_of(n * area, GROUP)

        def to_g(i, sums):
            parts = [0.25 * part + slope * at(now_v, i, j) for j, part in enumerate(sums)]
            parts[-1] = parts[-1] + eye(i % GROUP, flat)
            put(step_g, i, parts)

        square(now_v, now_v, to_g)

        def to_v(i, sums):
            put(tail, i, sums)
            put(keys, i, [mu * at(step_g, i, j) - 0.5 * part for j, part in enumerate(sums)], base)

        square(step_g, now_v, to_v)
        now_v[...] = tail[...]
        return carry

    lax.fori_loop(0, repeats - 1, forward, 0)

    after = scal[pl.ds(3 * repeats - 2, 1), :]
    for i in range(slots):
        parts = [-0.5 * at(keys, i, j, (repeats - 2) * area) for j in range(blocks)]
        parts[i // GROUP] = parts[i // GROUP] - eye(i % GROUP, 0.5 * after)
        for j, part in enumerate(parts):
            now_v[pl.ds(i * PITCH + j * GROUP, GROUP), :] = part

    def backward(m, carry):
        n = repeats - 3 - m
        base = pl.multiple_of(n * area, GROUP)
        half = 0.5 * scal[pl.ds(2 * repeats + n, 1), :]

        def to_h(i, sums):
            parts = list(sums)
            parts[-1] = parts[-1] - eye(i % GROUP, half)
            put(tail, i, parts)

        square(keys, now_v, to_h, base)
        now_v[...] = tail[...]
        return carry

    lax.fori_loop(0, repeats - 2, backward, 0)

    def whole(ref, k):
        return ref[pl.ds(pl.multiple_of(k * PITCH, GROUP), slots), :]

    none = jnp.zeros((slots, LANES), jnp.float32)

    def apply(ref):
        def step(k, total):
            return total + innov[pl.ds(k, 1), :] * whole(ref, k)

        return lax.fori_loop(0, slots, step, none)

    for _ in range(2):
        start = innov[...]
        innov[...] = apply(now_v)
        innov[...] = last_z * start + apply(first_v)
    gain = innov[...] * inverse
    factor = math.sqrt(shift) * jnp.sqrt(inverse)
    keep_ref[...] = factor * last_z
    both = factor * inverse

    def to_mix(first, sums):
        for r in range(GROUP):
            mix_ref[pl.ds(pl.multiple_of((first + r) * slots, slots), slots), :] = both * sums[r] + gain

    lane_product(
        lambda k, first, r: dev_ref[pl.ds((first + r) * slots + k, 1), :],
        lambda k: whole(now_v, k), slots, members, slots, to_mix,
    )


def solve_cells(pool, idx, counts, rows, cols, members):
    slots, cells = idx.shape
    lane = lambda height: pl.BlockSpec((height, LANES), lambda c: (0, c))
    square = pltpu.VMEM((slots * PITCH, LANES), jnp.float32)
    return pl.pallas_call(
        functools.partial(weights_kernel, members, NEWTON, LOC),
        grid=(cells // LANES,),
        in_specs=[pl.BlockSpec(pool.shape, lambda c: (0, 0)), lane(slots), lane(1), lane(1), lane(1)],
        out_specs=[lane(members * slots), lane(members * slots), lane(1)],
        out_shape=[
            jax.ShapeDtypeStruct((members * slots, cells), jnp.float32),
            jax.ShapeDtypeStruct((members * slots, cells), jnp.float32),
            jax.ShapeDtypeStruct((1, cells), jnp.float32),
        ],
        scratch_shapes=[square] * 3 + [
            pltpu.VMEM(((NEWTON - 1) * slots * PITCH, LANES), jnp.float32),
            square,
            pltpu.VMEM((slots, LANES), jnp.float32),
            pltpu.VMEM((3 * NEWTON, LANES), jnp.float32),
        ],
        compiler_params=pltpu.CompilerParams(vmem_limit_bytes=40 * 1024 * 1024),
        cost_estimate=pl.CostEstimate(flops=2 * 10**9, bytes_accessed=200 * 10**6, transcendentals=0),
        interpret=INTERPRET,
    )(pool, idx, counts, rows, cols)


def prep_kernel(rows, ens_ref, small_ref, pool_ref, edge_ref, mine_ref, theirs_ref, block, land, spread, send_sems, recv_sems):
    share, fields, _ = mine_ref.shape
    observed = small_ref.shape[1]
    span = fields * rows
    facts = small_ref.shape[0]
    me, place, count = lax.axis_index("mem"), lax.axis_index("space"), lax.axis_size("space")

    def exists(step):
        return (place + step >= 0) & (place + step < count)

    def guard(step, act):
        if step == 0:
            act()
        else:
            pl.when(exists(step))(act)

    ways = [(1, 0), (0, -1), (0, 1), (1, -1), (1, 1)]
    barrier = pltpu.get_barrier_semaphore()

    def target(flip, step):
        return (1 - me if flip else me, place + step)

    for flip, step in ways:
        def greet(flip=flip, step=step):
            pl.semaphore_signal(barrier, inc=1, device_id=target(flip, step), device_id_type=pl.DeviceIdType.MESH)

        guard(step, greet)

    block[pl.ds(share, facts), :] = small_ref[...]
    hot = jnp.where(
        lax.broadcasted_iota(jnp.int32, (LANES, observed), 0).astype(jnp.float32) == small_ref[3:4, :], 1.0, 0.0
    ).astype(jnp.bfloat16)
    wanted = lax.broadcasted_iota(jnp.int32, (span, observed), 0).astype(jnp.float32) == small_ref[4:5, :]

    def look(i, carry):
        got = jnp.dot(
            ens_ref[pl.ds(pl.multiple_of(i * span, span), span), :], hot, preferred_element_type=jnp.float32
        )
        block[pl.ds(i, 1), :] = jnp.sum(jnp.where(wanted, got, 0.0), axis=0, keepdims=True)
        return carry

    lax.fori_loop(0, share, look, 0)

    greeted = 1 + 2 * exists(-1).astype(jnp.int32) + 2 * exists(1).astype(jnp.int32)
    pl.semaphore_wait(barrier, greeted)

    def copy(n):
        flip, step = ways[n]
        return pltpu.make_async_remote_copy(
            src_ref=block, dst_ref=land.at[1 - step, flip],
            send_sem=send_sems.at[n], recv_sem=recv_sems.at[1 - step, flip],
            device_id=target(flip, step), device_id_type=pl.DeviceIdType.MESH,
        )

    for n, (flip, step) in enumerate(ways):
        guard(step, lambda n=n: copy(n).start())

    def split(pair, carry):
        for slot in range(2):
            i = 2 * pair + slot
            spread[slot] = ens_ref[pl.ds(pl.multiple_of(i * span, span), span), :].astype(jnp.float32)
            mine_ref[i] = spread[slot, pl.ds(me, fields, stride=rows), :].astype(jnp.bfloat16)
            theirs_ref[i] = spread[slot, pl.ds(1 - me, fields, stride=rows), :].astype(jnp.bfloat16)
        return carry

    lax.fori_loop(0, share // 2, split, 0)

    for n, (flip, step) in enumerate(ways):
        def arrive(n=n):
            copy(n).wait_send()

        guard(step, arrive)
    for n, (flip, step) in enumerate(ways):
        def landed(n=n):
            copy(n).wait_recv()

        guard(-step, landed)
    for step in (-1, 1):
        def blank(step=step):
            land[1 + step] = jnp.zeros_like(land[1 + step])

        pl.when(jnp.logical_not(exists(step)))(blank)
    line = lax.broadcasted_iota(jnp.int32, (GROUP, observed), 0)
    for part in range(3):
        own = block[...] if part == 1 else land[part, 0]
        lanes = pl.ds(part * observed, observed)
        pool_ref[pl.ds(0, share), lanes] = own[:share]
        pool_ref[pl.ds(share, share), lanes] = land[part, 1, pl.ds(0, share), :]
        pool_ref[pl.ds(2 * share, GROUP), lanes] = own[share : share + GROUP] + jnp.where(
            line == 2, float(rows * (part - 1)), 0.0
        )
        edge_ref[part] = own[share + GROUP :]


def prepare(flat, small, members, fields, rows):
    share = members // 2
    observed = small.shape[1]
    high = share + small.shape[0]
    vmem = pl.BlockSpec(memory_space=pltpu.VMEM)
    return pl.pallas_call(
        functools.partial(prep_kernel, rows),
        in_specs=[vmem] * 2,
        out_specs=[vmem] * 4,
        out_shape=[
            jax.ShapeDtypeStruct((members + GROUP, 3 * observed), jnp.float32),
            jax.ShapeDtypeStruct((3, small.shape[0] - GROUP, observed), jnp.float32),
            jax.ShapeDtypeStruct((share, fields, LANES), jnp.bfloat16),
            jax.ShapeDtypeStruct((share, fields, LANES), jnp.bfloat16),
        ],
        scratch_shapes=[
            pltpu.VMEM((high, observed), jnp.float32),
            pltpu.VMEM((3, 2, high, observed), jnp.float32),
            pltpu.VMEM((2, fields * rows, LANES), jnp.float32),
            pltpu.SemaphoreType.DMA((5,)),
            pltpu.SemaphoreType.DMA((3, 2)),
        ],
        compiler_params=pltpu.CompilerParams(
            vmem_limit_bytes=32 * 1024 * 1024, collective_id=0, has_side_effects=True
        ),
        cost_estimate=pl.CostEstimate(flops=10**8, bytes_accessed=8 * 10**6, transcendentals=0),
        interpret=INTERPRET,
    )(flat, small)


def analysis_kernel(parts, slots, *refs):
    states = refs[:parts]
    dev_ref, mix_ref, keep_ref = refs[parts : parts + 3]
    outs = refs[parts + 3 : 2 * parts + 3]
    anomaly, mapped, mean_ref = refs[2 * parts + 3 :]
    share, width, _ = states[0].shape
    members = share * parts
    total = jnp.zeros((width, LANES), jnp.float32)
    for state in states:
        total = lax.fori_loop(
            0, share, lambda i, t, s=state: t + s[i].astype(jnp.float32), total, unroll=4
        )
    mean = total * (1.0 / members)
    mean_ref[...] = mean
    for part, state in enumerate(states):

        def subtract(i, carry, s=state, base=part * share):
            anomaly[base + i] = s[i].astype(jnp.float32) - mean_ref[...]
            return carry

        lax.fori_loop(0, share, subtract, 0, unroll=4)

    def to_mapped(first, sums):
        for r in range(GROUP):
            mapped[first + r] = sums[r]

    lane_product(
        lambda i, first, r: dev_ref[pl.ds(i * slots + first + r, 1), :],
        lambda i: anomaly[i], members, slots, width, to_mapped,
    )
    for part, out in enumerate(outs):
        base = part * share

        def to_out(first, sums, out=out, base=base):
            for r in range(GROUP):
                held = mean_ref[...] + keep_ref[...] * anomaly[base + first + r]
                out[first + r] = (held + sums[r]).astype(jnp.bfloat16)

        lane_product(
            lambda k, first, r, base=base: mix_ref[pl.ds((base + first + r) * slots + k, 1), :],
            lambda k: mapped[k], slots, share, width, to_out,
        )


def finish_kernel(
    slots, width,
    mine_ref, other_ref, dev_ref, mix_ref, keep_ref, edge_ref, loss_ref, out_ref,
    rows, away, south, north, anomaly, mapped, mean_ref, coef, weave,
    away_sent, away_come, edge_sent, edge_come,
):
    share, fields, _ = mine_ref.shape
    members = 2 * share
    chunks = fields // width
    group = 2 * LANES // width
    me, place, count = lax.axis_index("mem"), lax.axis_index("space"), lax.axis_size("space")
    mesh_id = pl.DeviceIdType.MESH
    exists = (place > 0, place + 1 < count)
    sides = ((1 - me, place), (me, place - 1), (me, place + 1))
    barrier = pltpu.get_barrier_semaphore()
    pl.semaphore_signal(barrier, inc=1, device_id=sides[0], device_id_type=mesh_id)
    for side in range(2):
        @pl.when(exists[side])
        def _():
            pl.semaphore_signal(barrier, inc=1, device_id=sides[1 + side], device_id_type=mesh_id)

    for side, buffer in enumerate((south, north)):
        @pl.when(jnp.logical_not(exists[side]))
        def _():
            def clear(n, carry):
                for r in range(2):
                    buffer[r, n // share, n % share] = jnp.zeros((width, LANES), jnp.bfloat16)
                return carry

            lax.fori_loop(0, chunks * share, clear, 0)

    lane = lax.broadcasted_iota(jnp.int32, (GROUP, LANES), 1)
    for at, (part, r) in enumerate(((0, 1), (1, 0), (1, 1), (2, 0))):
        cut = pl.ds(r * LANES, LANES)
        cx = edge_ref[part, pl.ds(0, GROUP), cut]
        cy = edge_ref[part, pl.ds(GROUP, GROUP), cut]
        six = (
            1.0 - cy * cy,
            0.5 * cy * cy - 0.5 * cy,
            0.5 * cy * cy + 0.5 * cy,
            1.0 - cx * cx,
            jnp.where(lane == LANES - 1, 0.0, 0.5 * cx * cx - 0.5 * cx),
            jnp.where(lane == 0, 0.0, 0.5 * cx * cx + 0.5 * cx),
        )
        for n, value in enumerate(six):
            for piece in range(width // GROUP):
                coef[6 * at + n, pl.ds(piece * GROUP, GROUP), :] = value

    greeted = 1 + exists[0].astype(jnp.int32) + exists[1].astype(jnp.int32)
    pl.semaphore_wait(barrier, greeted)

    def swap(q):
        return pltpu.make_async_remote_copy(
            src_ref=away.at[q], dst_ref=rows.at[me, q],
            send_sem=away_sent.at[q], recv_sem=away_come.at[q],
            device_id=sides[0], device_id_type=mesh_id,
        )

    def pass_on(side, r, q):
        return pltpu.make_async_remote_copy(
            src_ref=rows.at[r, q], dst_ref=(north, south)[side].at[r, q],
            send_sem=edge_sent.at[side, r, q], recv_sem=edge_come.at[side, r, q],
            device_id=sides[1 + side], device_id_type=mesh_id,
        )

    def pass_both(r, q):
        for side in range(2):
            @pl.when(exists[side])
            def _():
                pass_on(side, r, q).start()

    def analyse_chunk(q):
        cut = pl.ds(pl.multiple_of(q * width, width), width)
        total = jnp.zeros((width, LANES), jnp.float32)
        for state in (mine_ref, other_ref):
            total = lax.fori_loop(
                0, share, lambda i, t, s=state: t + s[i, cut, :].astype(jnp.float32), total, unroll=4
            )
        mean_ref[...] = total * (1.0 / members)
        for part, state in enumerate((mine_ref, other_ref)):
            def subtract(i, carry, s=state, base=part * share):
                anomaly[base + i] = s[i, cut, :].astype(jnp.float32) - mean_ref[...]
                return carry

            lax.fori_loop(0, share, subtract, 0, unroll=4)

        def to_mapped(first, sums):
            for r in range(group):
                mapped[first + r] = sums[r]

        lane_product(
            lambda i, first, r: dev_ref[pl.ds(i * slots + first + r, 1), :],
            lambda i: anomaly[i], members, slots, width, to_mapped, group=group,
        )
        for part in (1, 0):
            base = part * share

            def to_out(first, sums, base=base, part=part):
                for r in range(group):
                    held = mean_ref[...] + keep_ref[...] * anomaly[base + first + r]
                    value = (held + sums[r]).astype(jnp.bfloat16)
                    if part:
                        away[q, first + r] = value
                    else:
                        rows[me, q, first + r] = value

            lane_product(
                lambda k, first, r, base=base: mix_ref[pl.ds((base + first + r) * slots + k, 1), :],
                lambda k: mapped[k], slots, share, width, to_out, group=group,
            )
            if part:
                swap(q).start()
            else:
                pass_both(me, q)

    def advect_chunk(q):
        cut = pl.ds(pl.multiple_of(q * width, width), width)

        def along(at, low, middle, high):
            now = coef[6 * at] * middle + coef[6 * at + 1] * high + coef[6 * at + 2] * low
            east = pltpu.roll(now, LANES - 1, 1)
            west = pltpu.roll(now, 1, 1)
            return coef[6 * at + 3] * now + coef[6 * at + 4] * east + coef[6 * at + 5] * west

        def several(n, carry):
            for slot in range(UNROLL):
                i = UNROLL * n + slot
                now = [
                    part[r, q, i].astype(jnp.float32) for part in (south, rows, north) for r in range(2)
                ]
                now = [along(at, *now[at : at + 3]) for at in range(4)]
                now = [along(1 + at, *now[at : at + 3]) for at in range(2)]
                for r in range(2):
                    weave[slot, pl.ds(r, width, stride=2), :] = now[r] * loss_ref[r, cut, :]
                start = pl.multiple_of((i * fields + q * width) * 2, 2 * width)
                out_ref[pl.ds(start, 2 * width), :] = weave[slot].astype(jnp.bfloat16)
            return carry

        lax.fori_loop(0, share // UNROLL, several, 0)

    def step(q, carry):
        @pl.when(q < chunks)
        def _():
            analyse_chunk(q)

        @pl.when((q >= 1) & (q - 1 < chunks))
        def _():
            swap(q - 1).wait_recv()
            pass_both(1 - me, q - 1)

        @pl.when((q >= LAG) & (q - LAG < chunks))
        def _():
            for side in range(2):
                @pl.when(exists[1 - side])
                def _():
                    for r in range(2):
                        pass_on(side, r, q - LAG).wait_recv()

            advect_chunk(q - LAG)

        return carry

    lax.fori_loop(0, chunks + LAG, step, 0)

    def drain(q, carry):
        swap(q).wait_send()
        for side in range(2):
            @pl.when(exists[side])
            def _():
                for r in range(2):
                    pass_on(side, r, q).wait_send()

        return carry

    lax.fori_loop(0, chunks, drain, 0)


def finish(mine, other, dev, mix, keep, edge, loss, slots, rows):
    share, fields, _ = mine.shape
    width = WIDTH
    chunks = fields // width
    vmem = pl.BlockSpec(memory_space=pltpu.VMEM)
    piece = (chunks, share, width, LANES)
    return pl.pallas_call(
        functools.partial(finish_kernel, slots, width),
        in_specs=[vmem] * 7,
        out_specs=vmem,
        out_shape=jax.ShapeDtypeStruct((share * fields * rows, LANES), jnp.bfloat16),
        scratch_shapes=[
            pltpu.VMEM((2,) + piece, jnp.bfloat16),
            pltpu.VMEM(piece, jnp.bfloat16),
            pltpu.VMEM((2,) + piece, jnp.bfloat16),
            pltpu.VMEM((2,) + piece, jnp.bfloat16),
            pltpu.VMEM((2 * share, width, LANES), jnp.float32),
            pltpu.VMEM((slots, width, LANES), jnp.float32),
            pltpu.VMEM((width, LANES), jnp.float32),
            pltpu.VMEM((24, width, LANES), jnp.float32),
            pltpu.VMEM((UNROLL, 2 * width, LANES), jnp.float32),
            pltpu.SemaphoreType.DMA((chunks,)),
            pltpu.SemaphoreType.DMA((chunks,)),
            pltpu.SemaphoreType.DMA((2, 2, chunks)),
            pltpu.SemaphoreType.DMA((2, 2, chunks)),
        ],
        compiler_params=pltpu.CompilerParams(
            vmem_limit_bytes=40 * 1024 * 1024, collective_id=1, has_side_effects=True
        ),
        cost_estimate=pl.CostEstimate(flops=10**9, bytes_accessed=10**7, transcendentals=0),
        interpret=INTERPRET,
    )(mine, other, dev, mix, keep, edge, loss)


def analyse(states, dev, mix, keep, slots, first, count, width):
    share, _, cells = states[0].shape
    parts = len(states)
    members = share * parts
    wide = lambda height: pl.BlockSpec((height, LANES), lambda c, f: (0, c))
    return pl.pallas_call(
        functools.partial(analysis_kernel, parts, slots),
        grid=(cells // LANES, count // width),
        in_specs=[
            pl.BlockSpec((share, width, LANES), lambda c, f: (0, f + first // width, c))
        ] * parts + [wide(members * slots), wide(members * slots), wide(1)],
        out_specs=[pl.BlockSpec((share, width, LANES), lambda c, f: (0, f, c))] * parts,
        out_shape=[jax.ShapeDtypeStruct((share, count, cells), jnp.bfloat16)] * parts,
        scratch_shapes=[
            pltpu.VMEM((members, width, LANES), jnp.float32),
            pltpu.VMEM((slots, width, LANES), jnp.float32),
            pltpu.VMEM((width, LANES), jnp.float32),
        ],
        compiler_params=pltpu.CompilerParams(vmem_limit_bytes=32 * 1024 * 1024),
        cost_estimate=pl.CostEstimate(flops=10**9, bytes_accessed=50 * 10**6, transcendentals=0),
        interpret=INTERPRET,
    )(*states, dev, mix, keep)


def halo(cells, width):
    count = lax.axis_size("space")
    before = lax.ppermute(cells[-width:], "space", [(i, i + 1) for i in range(count - 1)])
    after = lax.ppermute(cells[:width], "space", [(i + 1, i) for i in range(count - 1)])
    return before, after


def wide_rows(cells, width):
    before, after = halo(cells, width)
    return jnp.concatenate([before, cells, after], axis=0)


def row_step(south, middle, north, courant):
    return (
        middle
        - 0.5 * courant * (north - south)
        + 0.5 * courant * courant * (north - 2.0 * middle + south)
    )


def col_step(middle, courant):
    padded = jnp.pad(middle, [(0, 0)] * (middle.ndim - 1) + [(1, 1)])
    east, west = padded[..., 2:], padded[..., :-2]
    return (
        middle
        - 0.5 * courant * (east - west)
        + 0.5 * courant * courant * (east - 2.0 * middle + west)
    )


def shards(
    ensemble, obs_value, obs_error, obs_cell, obs_species, patch_index, patch_count,
    courant_x, courant_y, dep_velocity, surface_factor,
):
    local_members, fields, tile_rows, columns = ensemble.shape
    species = dep_velocity.shape[0]
    levels = fields // species
    tile_cells = tile_rows * columns
    groups = lax.axis_size("mem")
    members = local_members * groups
    me = lax.axis_index("mem")
    slots = patch_index.shape[2]
    per_dev = tile_cells // groups
    paired = groups == 2 and tile_rows == 2 and columns == LANES
    paired = paired and GROUP % levels == 0 and fields % WIDTH == 0
    swap = [(0, 1), (1, 0)]

    if paired:
        tall = GROUP // levels
        small = jnp.concatenate(
            [
                obs_value,
                obs_error,
                (obs_cell // columns).astype(jnp.float32),
                (obs_cell % columns).astype(jnp.float32),
                (obs_species * (levels * tile_rows) + obs_cell // columns).astype(jnp.float32),
                jnp.zeros((GROUP - 5, obs_value.shape[1]), jnp.float32),
            ]
            + [courant_x.reshape(levels, tile_cells)] * tall
            + [courant_y.reshape(levels, tile_cells)] * tall,
            axis=0,
        )
        pool, edge, mine, theirs = prepare(
            ensemble.reshape(-1, columns), small, members, fields, tile_rows
        )
    else:
        surface = ensemble.reshape(local_members, species, levels, tile_cells)[:, :, 0]
        position = obs_species[0] * tile_cells + obs_cell[0]
        equiv = jnp.take(surface.reshape(local_members, -1), position, axis=1).astype(jnp.float32)
        equiv = lax.all_gather(equiv, "mem", axis=0, tiled=True)
        zeros = jnp.zeros_like(obs_value[0])
        info = jnp.stack(
            [
                obs_value[0],
                obs_error[0],
                (obs_cell[0] // columns).astype(jnp.float32),
                (obs_cell[0] % columns).astype(jnp.float32),
            ]
            + [zeros] * 4
        )
        packed = jnp.concatenate([equiv, info], axis=0)
        before, after = halo(packed[None], 1)
        offset = jnp.zeros((packed.shape[0], 1), jnp.float32).at[members + 2, 0].set(float(tile_rows))
        pool = jnp.concatenate([before[0] - offset, packed, after[0] + offset], axis=1)

    if paired:
        states = (mine, lax.ppermute(theirs, "mem", swap))
    else:
        states = (
            lax.all_to_all(
                ensemble.reshape(local_members, fields, tile_cells),
                "mem", split_axis=2, concat_axis=0, tiled=True,
            ),
        )
    spare = -per_dev % LANES
    pad = lambda a: jnp.pad(a, [(0, 0)] * (a.ndim - 1) + [(0, spare)]) if spare else a
    states = tuple(pad(state) for state in states)
    cell = me * per_dev + jnp.arange(per_dev, dtype=jnp.int32)
    dev, mix, keep = solve_cells(
        pool,
        pad(jnp.transpose(patch_index[0])),
        pad(patch_count),
        pad((cell // columns).astype(jnp.float32)[None]),
        pad((cell % columns).astype(jnp.float32)[None]),
        members,
    )

    loss = jnp.exp(-dep_velocity[:, None, None] * surface_factor[None])
    if paired:
        lowest = (jnp.arange(levels, dtype=jnp.int32) == 0)[None, None, :, None]
        factor = jnp.where(lowest, jnp.moveaxis(loss, 1, 0)[:, :, None], 1.0).reshape(tile_rows, fields, columns)
        out = finish(*states, dev, mix, keep, edge, factor, slots, tile_rows)
        return out.reshape(ensemble.shape)

    width = next(w for w in (32, 16, fields) if fields % w == 0)
    wide_x = wide_rows(jnp.moveaxis(courant_x, 1, 0), SUBSTEPS)
    wide_y = wide_rows(jnp.moveaxis(courant_y, 1, 0), SUBSTEPS)
    out = analyse(states, dev, mix, keep, slots, 0, fields, width)
    back = lax.all_to_all(out[0][..., :per_dev], "mem", split_axis=0, concat_axis=2, tiled=True)
    rows = jnp.moveaxis(back.reshape(local_members, fields, tile_rows, columns), 2, 0)
    south, north = halo(rows, SUBSTEPS)
    shape = (local_members, species, levels, columns)
    now = [
        part[r].reshape(shape).astype(jnp.float32)
        for part in (south, rows, north)
        for r in range(part.shape[0])
    ]
    for repeat in range(SUBSTEPS):
        first = repeat + 1
        now = [
            col_step(
                row_step(now[r - 1], now[r], now[r + 1], wide_y[first + r - 1]),
                wide_x[first + r - 1],
            )
            for r in range(1, len(now) - 1)
        ]
    lowest = (jnp.arange(levels, dtype=jnp.int32) == 0)[:, None]
    now = [row * jnp.where(lowest, loss[:, r][:, None], 1.0) for r, row in enumerate(now)]
    joined = jnp.stack([row.astype(jnp.bfloat16) for row in now], axis=3)
    return joined.reshape(local_members, fields, tile_rows, columns)


def solution(mesh):
    in_specs = (
        P("mem", None, "space", None),
        P("space", None),
        P("space", None),
        P("space", None),
        P("space", None),
        P("space", "mem", None),
        P("space", "mem"),
        P(None, "space", None),
        P(None, "space", None),
        P(),
        P("space", None),
    )
    out_specs = P("mem", None, "space", None)
    return jax.shard_map(shards, mesh=mesh, in_specs=in_specs, out_specs=out_specs, check_vma=False)
```

```python
import functools
import math

import jax
import jax.numpy as jnp
from jax import lax
from jax.experimental import pallas as pl
from jax.experimental.pallas import tpu as pltpu
from jax.sharding import PartitionSpec as P

NEWTON = 8
SUBSTEPS = 2
LOC = 1
LANES = 128
GROUP = 8
PITCH = 40
WIDTH = 16
LAG = 3
UNROLL = 4
INTERPRET = False


def lane_product(left, right, depth, rows, width, finish, unroll=4, group=GROUP):
    def several(block, carry):
        first = pl.multiple_of(block * group, group)

        def step(k, sums):
            row = right(k)
            return tuple(sums[r] + left(k, first, r) * row for r in range(group))

        zero = jnp.zeros((width, LANES), jnp.float32)
        sums = lax.fori_loop(0, depth, step, (zero,) * group, unroll=unroll)
        finish(first, sums)
        return carry

    lax.fori_loop(0, rows // group, several, 0)


def weights_kernel(
    members, repeats, radius,
    pool_ref, idx_ref, cnt_ref, row_ref, col_ref,
    dev_ref, mix_ref, keep_ref,
    first_v, one_v, two_v, step_g, keys, innov, scal,
):
    slots = idx_ref.shape[0]
    pooled = pool_ref.shape[1]
    blocks = slots // GROUP
    info = pool_ref[members:, :]
    high = info.astype(jnp.bfloat16).astype(jnp.float32)
    rest = info - high
    middle = rest.astype(jnp.bfloat16).astype(jnp.float32)
    low = rest - middle
    table = jnp.concatenate([pool_ref[:members, :], high, middle, low, jnp.zeros_like(low)], axis=0)
    table = table.astype(jnp.bfloat16)
    place = lax.broadcasted_iota(jnp.int32, (pooled, LANES), 0)
    extra = info.shape[0]

    def pick(k, total):
        hot = jnp.where(place == idx_ref[pl.ds(k, 1), :], 1.0, 0.0).astype(jnp.bfloat16)
        got = jnp.dot(table, hot, preferred_element_type=jnp.float32)
        equiv = got[:members]
        facts = (
            got[members : members + extra]
            + got[members + extra : members + 2 * extra]
            + got[members + 2 * extra : members + 3 * extra]
        )
        mean = jnp.sum(equiv, axis=0, keepdims=True) * (1.0 / members)
        dist = (facts[2:3] - row_ref[...]) ** 2 + (facts[3:4] - col_ref[...]) ** 2
        rho = jnp.exp(-dist / (2.0 * radius * radius)) / facts[1:2]
        scale = jnp.sqrt(jnp.where(k < cnt_ref[...], rho, 0.0))
        scaled = (equiv - mean) * scale
        dev_ref[pl.ds(k, members, stride=PITCH), :] = scaled
        innov[pl.ds(k, 1), :] = (facts[0:1] - mean) * scale
        return total + jnp.sum(scaled * scaled, axis=0, keepdims=True)

    spread = lax.fori_loop(0, slots, pick, jnp.zeros((1, LANES), jnp.float32), unroll=8)
    shift = members - 1.0
    inverse = 1.0 / (spread + shift * members)
    level = lax.broadcasted_iota(jnp.int32, (GROUP, LANES), 0)

    def eye(r, value):
        return jnp.where(level == r, value, 0.0)

    def at(ref, i, j, base=0):
        start = i * PITCH + j * GROUP
        start = start if isinstance(start, int) else pl.multiple_of(start, GROUP)
        return ref[pl.ds(base + start, GROUP), :]

    def put(ref, i, parts, base=0):
        for j, part in enumerate(parts):
            ref[pl.ds(base + i * PITCH + j * GROUP, GROUP), :] = part
            if j < i // GROUP:
                ref[pl.ds(base + j * GROUP * PITCH + i, GROUP, stride=PITCH), :] = part

    def product(left, right, depth, finish, unroll=16):
        for pair in range((blocks + 1) // 2):
            groups = sorted({pair, blocks - 1 - pair})

            def step(k, sums):
                wide = [right(k, j) for j in range(groups[-1] + 1)]
                out, spot = [], 0
                for g in groups:
                    for r in range(GROUP):
                        one = left(k, g * GROUP + r)
                        for j in range(g + 1):
                            out.append(sums[spot] + one * wide[j])
                            spot += 1
                return tuple(out)

            zero = jnp.zeros((GROUP, LANES), jnp.float32)
            count = sum((g + 1) * GROUP for g in groups)
            sums = lax.fori_loop(0, depth, step, (zero,) * count, unroll=unroll)
            spot = 0
            for g in groups:
                for r in range(GROUP):
                    finish(g * GROUP + r, sums[spot : spot + g + 1])
                    spot += g + 1

    def square(left, right, finish, base=0):
        product(
            lambda k, i: left[pl.ds(base + k * PITCH + i, 1), :],
            lambda k, j: at(right, k, j),
            slots, finish,
        )

    def gram_done(i, sums):
        put(first_v, i, [part * inverse for part in sums])

    product(
        lambda k, i: dev_ref[pl.ds(k * PITCH + i, 1), :],
        lambda k, j: at(dev_ref, k, j),
        members, gram_done,
    )

    xi = shift * inverse
    mus = []
    for k in range(repeats):
        mu = 1.5 - 0.5 * xi
        scal[pl.ds(k, 1), :] = xi
        scal[pl.ds(repeats + k, 1), :] = mu
        mus.append(mu)
        xi = xi * mu * mu
    after = mus[-1]
    for k in reversed(range(repeats - 1)):
        scal[pl.ds(2 * repeats + k, 1), :] = after
        after = after * mus[k]
    last_z = after
    area = slots * PITCH

    def forward(n, old, new):
        xi = scal[pl.ds(n, 1), :]
        mu = scal[pl.ds(repeats + n, 1), :]
        flat, slope = mu * mu - xi * mu, 0.25 * xi - mu
        base = pl.multiple_of(n * area, GROUP)

        def to_g(i, sums):
            parts = [0.25 * part + slope * at(old, i, j) for j, part in enumerate(sums)]
            parts[-1] = parts[-1] + eye(i % GROUP, flat)
            put(step_g, i, parts)

        square(old, old, to_g)

        def to_v(i, sums):
            put(new, i, sums)
            put(keys, i, [mu * at(step_g, i, j) - 0.5 * part for j, part in enumerate(sums)], base)

        square(step_g, old, to_v)

    def forward_pair(n, carry):
        forward(2 * n + 1, one_v, two_v)
        forward(2 * n + 2, two_v, one_v)
        return carry

    forward(0, first_v, one_v)
    lax.fori_loop(0, repeats // 2 - 1, forward_pair, 0)

    after = scal[pl.ds(3 * repeats - 2, 1), :]
    for i in range(slots):
        parts = [-0.5 * at(keys, i, j, (repeats - 2) * area) for j in range(blocks)]
        parts[i // GROUP] = parts[i // GROUP] - eye(i % GROUP, 0.5 * after)
        for j, part in enumerate(parts):
            one_v[pl.ds(i * PITCH + j * GROUP, GROUP), :] = part

    def backward(n, old, new):
        base = pl.multiple_of(n * area, GROUP)
        half = 0.5 * scal[pl.ds(2 * repeats + n, 1), :]

        def to_h(i, sums):
            parts = list(sums)
            parts[-1] = parts[-1] - eye(i % GROUP, half)
            put(new, i, parts)

        square(keys, old, to_h, base)

    def backward_pair(m, carry):
        backward(repeats - 3 - 2 * m, one_v, two_v)
        backward(repeats - 4 - 2 * m, two_v, one_v)
        return carry

    lax.fori_loop(0, repeats // 2 - 1, backward_pair, 0)

    def whole(ref, k):
        return ref[pl.ds(pl.multiple_of(k * PITCH, GROUP), slots), :]

    none = jnp.zeros((slots, LANES), jnp.float32)

    def apply(ref):
        def step(k, total):
            return total + innov[pl.ds(k, 1), :] * whole(ref, k)

        return lax.fori_loop(0, slots, step, none)

    for _ in range(2):
        start = innov[...]
        innov[...] = apply(one_v)
        innov[...] = last_z * start + apply(first_v)
    gain = innov[...] * inverse
    factor = math.sqrt(shift) * jnp.sqrt(inverse)
    keep_ref[...] = factor * last_z
    both = factor * inverse

    def to_mix(first, sums):
        for r in range(GROUP):
            mix_ref[pl.ds(pl.multiple_of((first + r) * slots, slots), slots), :] = both * sums[r] + gain

    lane_product(
        lambda k, first, r: dev_ref[pl.ds((first + r) * PITCH + k, 1), :],
        lambda k: whole(one_v, k), slots, members, slots, to_mix, unroll=16,
    )


def solve_cells(pool, idx, counts, rows, cols, members):
    slots, cells = idx.shape
    lane = lambda height: pl.BlockSpec((height, LANES), lambda c: (0, c))
    square = pltpu.VMEM((slots * PITCH, LANES), jnp.float32)
    return pl.pallas_call(
        functools.partial(weights_kernel, members, NEWTON, LOC),
        grid=(cells // LANES,),
        in_specs=[pl.BlockSpec(pool.shape, lambda c: (0, 0)), lane(slots), lane(1), lane(1), lane(1)],
        out_specs=[lane(members * PITCH), lane(members * slots), lane(1)],
        out_shape=[
            jax.ShapeDtypeStruct((members * PITCH, cells), jnp.float32),
            jax.ShapeDtypeStruct((members * slots, cells), jnp.float32),
            jax.ShapeDtypeStruct((1, cells), jnp.float32),
        ],
        scratch_shapes=[
            square,
            square,
            square,
            square,
            pltpu.VMEM(((NEWTON - 1) * slots * PITCH, LANES), jnp.float32),
            pltpu.VMEM((slots, LANES), jnp.float32),
            pltpu.VMEM((3 * NEWTON, LANES), jnp.float32),
        ],
        compiler_params=pltpu.CompilerParams(vmem_limit_bytes=40 * 1024 * 1024),
        cost_estimate=pl.CostEstimate(flops=2 * 10**9, bytes_accessed=200 * 10**6, transcendentals=0),
        interpret=INTERPRET,
    )(pool, idx, counts, rows, cols)


def prep_kernel(rows, levels, ens_ref, small_ref, pool_ref, edge_ref, mine_ref, theirs_ref, block, land, spread, send_sems, recv_sems):
    share, fields, _ = mine_ref.shape
    observed = small_ref.shape[1]
    span = fields * rows
    facts = small_ref.shape[0]
    species = fields // levels
    me, place, count = lax.axis_index("mem"), lax.axis_index("space"), lax.axis_size("space")

    def exists(step):
        return (place + step >= 0) & (place + step < count)

    def guard(step, act):
        if step == 0:
            act()
        else:
            pl.when(exists(step))(act)

    ways = [(1, 0), (0, -1), (0, 1), (1, -1), (1, 1)]
    barrier = pltpu.get_barrier_semaphore()

    def target(flip, step):
        return (1 - me if flip else me, place + step)

    for flip, step in ways:
        def greet(flip=flip, step=step):
            pl.semaphore_signal(barrier, inc=1, device_id=target(flip, step), device_id_type=pl.DeviceIdType.MESH)

        guard(step, greet)

    block[pl.ds(share, facts), :] = small_ref[...]
    hot = jnp.where(
        lax.broadcasted_iota(jnp.int32, (LANES, observed), 0).astype(jnp.float32) == small_ref[3:4, :], 1.0, 0.0
    ).astype(jnp.bfloat16)
    wanted = lax.broadcasted_iota(jnp.int32, (rows * species, observed), 0).astype(jnp.float32) == small_ref[4:5, :]

    def look(n, carry):
        for slot in range(UNROLL):
            i = UNROLL * n + slot
            spread[slot] = ens_ref[pl.ds(pl.multiple_of(i * span, span), span), :].astype(jnp.float32)
            lowest = jnp.concatenate(
                [spread[slot, pl.ds(r, species, stride=rows * levels), :] for r in range(rows)], axis=0
            )
            got = jnp.dot(lowest.astype(jnp.bfloat16), hot, preferred_element_type=jnp.float32)
            block[pl.ds(i, 1), :] = jnp.sum(jnp.where(wanted, got, 0.0), axis=0, keepdims=True)
        return carry

    lax.fori_loop(0, share // UNROLL, look, 0)

    greeted = 1 + 2 * exists(-1).astype(jnp.int32) + 2 * exists(1).astype(jnp.int32)
    pl.semaphore_wait(barrier, greeted)

    def copy(n):
        flip, step = ways[n]
        return pltpu.make_async_remote_copy(
            src_ref=block, dst_ref=land.at[1 - step, flip],
            send_sem=send_sems.at[n], recv_sem=recv_sems.at[1 - step, flip],
            device_id=target(flip, step), device_id_type=pl.DeviceIdType.MESH,
        )

    for n, (flip, step) in enumerate(ways):
        guard(step, lambda n=n: copy(n).start())

    def split(n, carry):
        for slot in range(UNROLL):
            i = UNROLL * n + slot
            spread[slot] = ens_ref[pl.ds(pl.multiple_of(i * span, span), span), :].astype(jnp.float32)
            mine_ref[i] = spread[slot, pl.ds(me, fields, stride=rows), :].astype(jnp.bfloat16)
            theirs_ref[i] = spread[slot, pl.ds(1 - me, fields, stride=rows), :].astype(jnp.bfloat16)
        return carry

    lax.fori_loop(0, share // UNROLL, split, 0)

    for n, (flip, step) in enumerate(ways):
        def arrive(n=n):
            copy(n).wait_send()

        guard(step, arrive)
    for n, (flip, step) in enumerate(ways):
        def landed(n=n):
            copy(n).wait_recv()

        guard(-step, landed)
    for step in (-1, 1):
        def blank(step=step):
            land[1 + step] = jnp.zeros_like(land[1 + step])

        pl.when(jnp.logical_not(exists(step)))(blank)
    line = lax.broadcasted_iota(jnp.int32, (GROUP, observed), 0)
    for part in range(3):
        own = block[...] if part == 1 else land[part, 0]
        lanes = pl.ds(part * observed, observed)
        pool_ref[pl.ds(0, share), lanes] = own[:share]
        pool_ref[pl.ds(share, share), lanes] = land[part, 1, pl.ds(0, share), :]
        pool_ref[pl.ds(2 * share, GROUP), lanes] = own[share : share + GROUP] + jnp.where(
            line == 2, float(rows * (part - 1)), 0.0
        )
        edge_ref[part] = own[share + GROUP :]


def prepare(flat, small, members, fields, rows, levels):
    share = members // 2
    observed = small.shape[1]
    high = share + small.shape[0]
    vmem = pl.BlockSpec(memory_space=pltpu.VMEM)
    return pl.pallas_call(
        functools.partial(prep_kernel, rows, levels),
        in_specs=[vmem] * 2,
        out_specs=[vmem] * 4,
        out_shape=[
            jax.ShapeDtypeStruct((members + GROUP, 3 * observed), jnp.float32),
            jax.ShapeDtypeStruct((3, small.shape[0] - GROUP, observed), jnp.float32),
            jax.ShapeDtypeStruct((share, fields, LANES), jnp.bfloat16),
            jax.ShapeDtypeStruct((share, fields, LANES), jnp.bfloat16),
        ],
        scratch_shapes=[
            pltpu.VMEM((high, observed), jnp.float32),
            pltpu.VMEM((3, 2, high, observed), jnp.float32),
            pltpu.VMEM((UNROLL, fields * rows, LANES), jnp.float32),
            pltpu.SemaphoreType.DMA((5,)),
            pltpu.SemaphoreType.DMA((3, 2)),
        ],
        compiler_params=pltpu.CompilerParams(
            vmem_limit_bytes=32 * 1024 * 1024, collective_id=0, has_side_effects=True
        ),
        cost_estimate=pl.CostEstimate(flops=10**8, bytes_accessed=8 * 10**6, transcendentals=0),
        interpret=INTERPRET,
    )(flat, small)


def analysis_kernel(parts, slots, *refs):
    states = refs[:parts]
    dev_ref, mix_ref, keep_ref = refs[parts : parts + 3]
    outs = refs[parts + 3 : 2 * parts + 3]
    anomaly, mapped, mean_ref = refs[2 * parts + 3 :]
    share, width, _ = states[0].shape
    members = share * parts
    total = jnp.zeros((width, LANES), jnp.float32)
    for state in states:
        total = lax.fori_loop(
            0, share, lambda i, t, s=state: t + s[i].astype(jnp.float32), total, unroll=4
        )
    mean = total * (1.0 / members)
    mean_ref[...] = mean
    for part, state in enumerate(states):

        def subtract(i, carry, s=state, base=part * share):
            anomaly[base + i] = s[i].astype(jnp.float32) - mean_ref[...]
            return carry

        lax.fori_loop(0, share, subtract, 0, unroll=4)

    def to_mapped(first, sums):
        for r in range(GROUP):
            mapped[first + r] = sums[r]

    lane_product(
        lambda i, first, r: dev_ref[pl.ds(i * PITCH + first + r, 1), :],
        lambda i: anomaly[i], members, slots, width, to_mapped,
    )
    for part, out in enumerate(outs):
        base = part * share

        def to_out(first, sums, out=out, base=base):
            for r in range(GROUP):
                held = mean_ref[...] + keep_ref[...] * anomaly[base + first + r]
                out[first + r] = (held + sums[r]).astype(jnp.bfloat16)

        lane_product(
            lambda k, first, r, base=base: mix_ref[pl.ds((base + first + r) * slots + k, 1), :],
            lambda k: mapped[k], slots, share, width, to_out,
        )


def finish_kernel(
    slots, width,
    mine_ref, other_ref, dev_ref, mix_ref, keep_ref, edge_ref, loss_ref, out_ref,
    rows, away, south, north, anomaly, mapped, mean_ref, coef, weave,
    away_sent, away_come, edge_sent, edge_come,
):
    share, fields, _ = mine_ref.shape
    members = 2 * share
    chunks = fields // width
    group = 2 * LANES // width
    me, place, count = lax.axis_index("mem"), lax.axis_index("space"), lax.axis_size("space")
    mesh_id = pl.DeviceIdType.MESH
    exists = (place > 0, place + 1 < count)
    sides = ((1 - me, place), (me, place - 1), (me, place + 1))
    barrier = pltpu.get_barrier_semaphore()
    pl.semaphore_signal(barrier, inc=1, device_id=sides[0], device_id_type=mesh_id)
    for side in range(2):
        @pl.when(exists[side])
        def _():
            pl.semaphore_signal(barrier, inc=1, device_id=sides[1 + side], device_id_type=mesh_id)

    for side, buffer in enumerate((south, north)):
        @pl.when(jnp.logical_not(exists[side]))
        def _():
            def clear(n, carry):
                for r in range(2):
                    buffer[r, n // share, n % share] = jnp.zeros((width, LANES), jnp.bfloat16)
                return carry

            lax.fori_loop(0, chunks * share, clear, 0)

    lane = lax.broadcasted_iota(jnp.int32, (GROUP, LANES), 1)
    for at, (part, r) in enumerate(((0, 1), (1, 0), (1, 1), (2, 0))):
        cut = pl.ds(r * LANES, LANES)
        cx = edge_ref[part, pl.ds(0, GROUP), cut]
        cy = edge_ref[part, pl.ds(GROUP, GROUP), cut]
        six = (
            1.0 - cy * cy,
            0.5 * cy * cy - 0.5 * cy,
            0.5 * cy * cy + 0.5 * cy,
            1.0 - cx * cx,
            jnp.where(lane == LANES - 1, 0.0, 0.5 * cx * cx - 0.5 * cx),
            jnp.where(lane == 0, 0.0, 0.5 * cx * cx + 0.5 * cx),
        )
        for n, value in enumerate(six):
            for piece in range(width // GROUP):
                coef[6 * at + n, pl.ds(piece * GROUP, GROUP), :] = value

    greeted = 1 + exists[0].astype(jnp.int32) + exists[1].astype(jnp.int32)
    pl.semaphore_wait(barrier, greeted)

    def swap(q):
        return pltpu.make_async_remote_copy(
            src_ref=away.at[q], dst_ref=rows.at[me, q],
            send_sem=away_sent.at[q], recv_sem=away_come.at[q],
            device_id=sides[0], device_id_type=mesh_id,
        )

    def pass_on(side, r, q):
        return pltpu.make_async_remote_copy(
            src_ref=rows.at[r, q], dst_ref=(north, south)[side].at[r, q],
            send_sem=edge_sent.at[side, r, q], recv_sem=edge_come.at[side, r, q],
            device_id=sides[1 + side], device_id_type=mesh_id,
        )

    def pass_both(r, q):
        for side in range(2):
            @pl.when(exists[side])
            def _():
                pass_on(side, r, q).start()

    def analyse_chunk(q):
        cut = pl.ds(pl.multiple_of(q * width, width), width)
        total = jnp.zeros((width, LANES), jnp.float32)
        for state in (mine_ref, other_ref):
            total = lax.fori_loop(
                0, share, lambda i, t, s=state: t + s[i, cut, :].astype(jnp.float32), total, unroll=4
            )
        mean_ref[...] = total * (1.0 / members)
        for part, state in enumerate((mine_ref, other_ref)):
            def subtract(i, carry, s=state, base=part * share):
                anomaly[base + i] = s[i, cut, :].astype(jnp.float32) - mean_ref[...]
                return carry

            lax.fori_loop(0, share, subtract, 0, unroll=4)

        def to_mapped(first, sums):
            for r in range(group):
                mapped[first + r] = sums[r]

        lane_product(
            lambda i, first, r: dev_ref[pl.ds(i * PITCH + first + r, 1), :],
            lambda i: anomaly[i], members, slots, width, to_mapped, group=group,
        )
        for part in (1, 0):
            base = part * share

            def to_out(first, sums, base=base, part=part):
                for r in range(group):
                    held = mean_ref[...] + keep_ref[...] * anomaly[base + first + r]
                    value = (held + sums[r]).astype(jnp.bfloat16)
                    if part:
                        away[q, first + r] = value
                    else:
                        rows[me, q, first + r] = value

            lane_product(
                lambda k, first, r, base=base: mix_ref[pl.ds((base + first + r) * slots + k, 1), :],
                lambda k: mapped[k], slots, share, width, to_out, group=group,
            )
            if part:
                swap(q).start()
            else:
                pass_both(me, q)

    def advect_chunk(q):
        cut = pl.ds(pl.multiple_of(q * width, width), width)

        def along(at, low, middle, high):
            now = coef[6 * at] * middle + coef[6 * at + 1] * high + coef[6 * at + 2] * low
            east = pltpu.roll(now, LANES - 1, 1)
            west = pltpu.roll(now, 1, 1)
            return coef[6 * at + 3] * now + coef[6 * at + 4] * east + coef[6 * at + 5] * west

        def several(n, carry):
            for slot in range(UNROLL):
                i = UNROLL * n + slot
                now = [
                    part[r, q, i].astype(jnp.float32) for part in (south, rows, north) for r in range(2)
                ]
                now = [along(at, *now[at : at + 3]) for at in range(4)]
                now = [along(1 + at, *now[at : at + 3]) for at in range(2)]
                for r in range(2):
                    weave[slot, pl.ds(r, width, stride=2), :] = now[r] * loss_ref[r, cut, :]
                start = pl.multiple_of((i * fields + q * width) * 2, 2 * width)
                out_ref[pl.ds(start, 2 * width), :] = weave[slot].astype(jnp.bfloat16)
            return carry

        lax.fori_loop(0, share // UNROLL, several, 0)

    def step(q, carry):
        @pl.when(q < chunks)
        def _():
            analyse_chunk(q)

        @pl.when((q >= 1) & (q - 1 < chunks))
        def _():
            swap(q - 1).wait_recv()
            pass_both(1 - me, q - 1)

        @pl.when((q >= LAG) & (q - LAG < chunks))
        def _():
            for side in range(2):
                @pl.when(exists[1 - side])
                def _():
                    for r in range(2):
                        pass_on(side, r, q - LAG).wait_recv()

            advect_chunk(q - LAG)

        return carry

    lax.fori_loop(0, chunks + LAG, step, 0)

    def drain(q, carry):
        swap(q).wait_send()
        for side in range(2):
            @pl.when(exists[side])
            def _():
                for r in range(2):
                    pass_on(side, r, q).wait_send()

        return carry

    lax.fori_loop(0, chunks, drain, 0)


def finish(mine, other, dev, mix, keep, edge, loss, slots, rows):
    share, fields, _ = mine.shape
    width = WIDTH
    chunks = fields // width
    vmem = pl.BlockSpec(memory_space=pltpu.VMEM)
    piece = (chunks, share, width, LANES)
    return pl.pallas_call(
        functools.partial(finish_kernel, slots, width),
        in_specs=[vmem] * 7,
        out_specs=vmem,
        out_shape=jax.ShapeDtypeStruct((share * fields * rows, LANES), jnp.bfloat16),
        scratch_shapes=[
            pltpu.VMEM((2,) + piece, jnp.bfloat16),
            pltpu.VMEM(piece, jnp.bfloat16),
            pltpu.VMEM((2,) + piece, jnp.bfloat16),
            pltpu.VMEM((2,) + piece, jnp.bfloat16),
            pltpu.VMEM((2 * share, width, LANES), jnp.float32),
            pltpu.VMEM((slots, width, LANES), jnp.float32),
            pltpu.VMEM((width, LANES), jnp.float32),
            pltpu.VMEM((24, width, LANES), jnp.float32),
            pltpu.VMEM((UNROLL, 2 * width, LANES), jnp.float32),
            pltpu.SemaphoreType.DMA((chunks,)),
            pltpu.SemaphoreType.DMA((chunks,)),
            pltpu.SemaphoreType.DMA((2, 2, chunks)),
            pltpu.SemaphoreType.DMA((2, 2, chunks)),
        ],
        compiler_params=pltpu.CompilerParams(
            vmem_limit_bytes=40 * 1024 * 1024, collective_id=1, has_side_effects=True
        ),
        cost_estimate=pl.CostEstimate(flops=10**9, bytes_accessed=10**7, transcendentals=0),
        interpret=INTERPRET,
    )(mine, other, dev, mix, keep, edge, loss)


def analyse(states, dev, mix, keep, slots, first, count, width):
    share, _, cells = states[0].shape
    parts = len(states)
    members = share * parts
    wide = lambda height: pl.BlockSpec((height, LANES), lambda c, f: (0, c))
    return pl.pallas_call(
        functools.partial(analysis_kernel, parts, slots),
        grid=(cells // LANES, count // width),
        in_specs=[
            pl.BlockSpec((share, width, LANES), lambda c, f: (0, f + first // width, c))
        ] * parts + [wide(members * PITCH), wide(members * slots), wide(1)],
        out_specs=[pl.BlockSpec((share, width, LANES), lambda c, f: (0, f, c))] * parts,
        out_shape=[jax.ShapeDtypeStruct((share, count, cells), jnp.bfloat16)] * parts,
        scratch_shapes=[
            pltpu.VMEM((members, width, LANES), jnp.float32),
            pltpu.VMEM((slots, width, LANES), jnp.float32),
            pltpu.VMEM((width, LANES), jnp.float32),
        ],
        compiler_params=pltpu.CompilerParams(vmem_limit_bytes=32 * 1024 * 1024),
        cost_estimate=pl.CostEstimate(flops=10**9, bytes_accessed=50 * 10**6, transcendentals=0),
        interpret=INTERPRET,
    )(*states, dev, mix, keep)


def halo(cells, width):
    count = lax.axis_size("space")
    before = lax.ppermute(cells[-width:], "space", [(i, i + 1) for i in range(count - 1)])
    after = lax.ppermute(cells[:width], "space", [(i + 1, i) for i in range(count - 1)])
    return before, after


def wide_rows(cells, width):
    before, after = halo(cells, width)
    return jnp.concatenate([before, cells, after], axis=0)


def row_step(south, middle, north, courant):
    return (
        middle
        - 0.5 * courant * (north - south)
        + 0.5 * courant * courant * (north - 2.0 * middle + south)
    )


def col_step(middle, courant):
    padded = jnp.pad(middle, [(0, 0)] * (middle.ndim - 1) + [(1, 1)])
    east, west = padded[..., 2:], padded[..., :-2]
    return (
        middle
        - 0.5 * courant * (east - west)
        + 0.5 * courant * courant * (east - 2.0 * middle + west)
    )


def shards(
    ensemble, obs_value, obs_error, obs_cell, obs_species, patch_index, patch_count,
    courant_x, courant_y, dep_velocity, surface_factor,
):
    local_members, fields, tile_rows, columns = ensemble.shape
    species = dep_velocity.shape[0]
    levels = fields // species
    tile_cells = tile_rows * columns
    groups = lax.axis_size("mem")
    members = local_members * groups
    me = lax.axis_index("mem")
    slots = patch_index.shape[2]
    per_dev = tile_cells // groups
    paired = groups == 2 and tile_rows == 2 and columns == LANES
    paired = paired and GROUP % levels == 0 and fields % WIDTH == 0 and species % GROUP == 0
    paired = paired and local_members % UNROLL == 0
    swap = [(0, 1), (1, 0)]

    if paired:
        tall = GROUP // levels
        small = jnp.concatenate(
            [
                obs_value,
                obs_error,
                (obs_cell // columns).astype(jnp.float32),
                (obs_cell % columns).astype(jnp.float32),
                (obs_cell // columns * species + obs_species).astype(jnp.float32),
                jnp.zeros((GROUP - 5, obs_value.shape[1]), jnp.float32),
            ]
            + [courant_x.reshape(levels, tile_cells)] * tall
            + [courant_y.reshape(levels, tile_cells)] * tall,
            axis=0,
        )
        pool, edge, mine, theirs = prepare(
            ensemble.reshape(-1, columns), small, members, fields, tile_rows, levels
        )
    else:
        surface = ensemble.reshape(local_members, species, levels, tile_cells)[:, :, 0]
        position = obs_species[0] * tile_cells + obs_cell[0]
        equiv = jnp.take(surface.reshape(local_members, -1), position, axis=1).astype(jnp.float32)
        equiv = lax.all_gather(equiv, "mem", axis=0, tiled=True)
        zeros = jnp.zeros_like(obs_value[0])
        info = jnp.stack(
            [
                obs_value[0],
                obs_error[0],
                (obs_cell[0] // columns).astype(jnp.float32),
                (obs_cell[0] % columns).astype(jnp.float32),
            ]
            + [zeros] * 4
        )
        packed = jnp.concatenate([equiv, info], axis=0)
        before, after = halo(packed[None], 1)
        offset = jnp.zeros((packed.shape[0], 1), jnp.float32).at[members + 2, 0].set(float(tile_rows))
        pool = jnp.concatenate([before[0] - offset, packed, after[0] + offset], axis=1)

    if paired:
        states = (mine, lax.ppermute(theirs, "mem", swap))
    else:
        states = (
            lax.all_to_all(
                ensemble.reshape(local_members, fields, tile_cells),
                "mem", split_axis=2, concat_axis=0, tiled=True,
            ),
        )
    spare = -per_dev % LANES
    pad = lambda a: jnp.pad(a, [(0, 0)] * (a.ndim - 1) + [(0, spare)]) if spare else a
    states = tuple(pad(state) for state in states)
    cell = me * per_dev + jnp.arange(per_dev, dtype=jnp.int32)
    dev, mix, keep = solve_cells(
        pool,
        pad(jnp.transpose(patch_index[0])),
        pad(patch_count),
        pad((cell // columns).astype(jnp.float32)[None]),
        pad((cell % columns).astype(jnp.float32)[None]),
        members,
    )

    loss = jnp.exp(-dep_velocity[:, None, None] * surface_factor[None])
    if paired:
        lowest = (jnp.arange(levels, dtype=jnp.int32) == 0)[None, None, :, None]
        factor = jnp.where(lowest, jnp.moveaxis(loss, 1, 0)[:, :, None], 1.0).reshape(tile_rows, fields, columns)
        out = finish(*states, dev, mix, keep, edge, factor, slots, tile_rows)
        return out.reshape(ensemble.shape)

    width = next(w for w in (32, 16, fields) if fields % w == 0)
    wide_x = wide_rows(jnp.moveaxis(courant_x, 1, 0), SUBSTEPS)
    wide_y = wide_rows(jnp.moveaxis(courant_y, 1, 0), SUBSTEPS)
    out = analyse(states, dev, mix, keep, slots, 0, fields, width)
    back = lax.all_to_all(out[0][..., :per_dev], "mem", split_axis=0, concat_axis=2, tiled=True)
    rows = jnp.moveaxis(back.reshape(local_members, fields, tile_rows, columns), 2, 0)
    south, north = halo(rows, SUBSTEPS)
    shape = (local_members, species, levels, columns)
    now = [
        part[r].reshape(shape).astype(jnp.float32)
        for part in (south, rows, north)
        for r in range(part.shape[0])
    ]
    for repeat in range(SUBSTEPS):
        first = repeat + 1
        now = [
            col_step(
                row_step(now[r - 1], now[r], now[r + 1], wide_y[first + r - 1]),
                wide_x[first + r - 1],
            )
            for r in range(1, len(now) - 1)
        ]
    lowest = (jnp.arange(levels, dtype=jnp.int32) == 0)[:, None]
    now = [row * jnp.where(lowest, loss[:, r][:, None], 1.0) for r, row in enumerate(now)]
    joined = jnp.stack([row.astype(jnp.bfloat16) for row in now], axis=3)
    return joined.reshape(local_members, fields, tile_rows, columns)


def solution(mesh):
    in_specs = (
        P("mem", None, "space", None),
        P("space", None),
        P("space", None),
        P("space", None),
        P("space", None),
        P("space", "mem", None),
        P("space", "mem"),
        P(None, "space", None),
        P(None, "space", None),
        P(),
        P("space", None),
    )
    out_specs = P("mem", None, "space", None)
    return jax.shard_map(shards, mesh=mesh, in_specs=in_specs, out_specs=out_specs, check_vma=False)
```

```python
import functools
import math

import jax
import jax.numpy as jnp
from jax import lax
from jax.experimental import pallas as pl
from jax.experimental.pallas import tpu as pltpu
from jax.sharding import PartitionSpec as P

NEWTON = 8
SUBSTEPS = 2
LOC = 1
LANES = 128
GROUP = 8
PITCH = 40
WIDTH = 16
LAG = 6
RELAY = 3
QUAD = 4
UNROLL = 8
INTERPRET = False


def lane_product(left, right, depth, rows, width, finish, unroll=4, group=GROUP):
    def several(block, carry):
        first = pl.multiple_of(block * group, group)

        def step(k, sums):
            row = right(k)
            return tuple(sums[r] + left(k, first, r) * row for r in range(group))

        zero = jnp.zeros((width, LANES), jnp.float32)
        sums = lax.fori_loop(0, depth, step, (zero,) * group, unroll=unroll)
        finish(first, sums)
        return carry

    lax.fori_loop(0, rows // group, several, 0)


def weights_kernel(
    members, repeats, radius,
    pool_ref, idx_ref, cnt_ref, row_ref, col_ref,
    dev_ref, mix_ref, keep_ref,
    first_v, one_v, two_v, step_g, keys, innov, scal,
):
    slots = idx_ref.shape[0]
    pooled = pool_ref.shape[1]
    blocks = slots // GROUP
    info = pool_ref[members:, :]
    high = info.astype(jnp.bfloat16).astype(jnp.float32)
    rest = info - high
    middle = rest.astype(jnp.bfloat16).astype(jnp.float32)
    low = rest - middle
    table = jnp.concatenate([pool_ref[:members, :], high, middle, low, jnp.zeros_like(low)], axis=0)
    table = table.astype(jnp.bfloat16)
    place = lax.broadcasted_iota(jnp.int32, (pooled, LANES), 0)
    extra = info.shape[0]

    def pick(k, total):
        hot = jnp.where(place == idx_ref[pl.ds(k, 1), :], 1.0, 0.0).astype(jnp.bfloat16)
        got = jnp.dot(table, hot, preferred_element_type=jnp.float32)
        equiv = got[:members]
        facts = (
            got[members : members + extra]
            + got[members + extra : members + 2 * extra]
            + got[members + 2 * extra : members + 3 * extra]
        )
        mean = jnp.sum(equiv, axis=0, keepdims=True) * (1.0 / members)
        dist = (facts[2:3] - row_ref[...]) ** 2 + (facts[3:4] - col_ref[...]) ** 2
        rho = jnp.exp(-dist / (2.0 * radius * radius)) / facts[1:2]
        scale = jnp.sqrt(jnp.where(k < cnt_ref[...], rho, 0.0))
        scaled = (equiv - mean) * scale
        dev_ref[pl.ds(k, members, stride=PITCH), :] = scaled
        innov[pl.ds(k, 1), :] = (facts[0:1] - mean) * scale
        return total + jnp.sum(scaled * scaled, axis=0, keepdims=True)

    spread = lax.fori_loop(0, slots, pick, jnp.zeros((1, LANES), jnp.float32), unroll=8)
    shift = members - 1.0
    inverse = 1.0 / (spread + shift * members)
    level = lax.broadcasted_iota(jnp.int32, (GROUP, LANES), 0)

    def eye(r, value):
        return jnp.where(level == r, value, 0.0)

    def at(ref, i, j, base=0):
        start = i * PITCH + j * GROUP
        start = start if isinstance(start, int) else pl.multiple_of(start, GROUP)
        return ref[pl.ds(base + start, GROUP), :]

    def put(ref, i, parts, base=0):
        for j, part in enumerate(parts):
            ref[pl.ds(base + i * PITCH + j * GROUP, GROUP), :] = part
            if j < i // GROUP:
                ref[pl.ds(base + j * GROUP * PITCH + i, GROUP, stride=PITCH), :] = part

    def product(left, right, depth, finish, unroll=16):
        for pair in range((blocks + 1) // 2):
            groups = sorted({pair, blocks - 1 - pair})

            def step(k, sums):
                wide = [right(k, j) for j in range(groups[-1] + 1)]
                out, spot = [], 0
                for g in groups:
                    for r in range(GROUP):
                        one = left(k, g * GROUP + r)
                        for j in range(g + 1):
                            out.append(sums[spot] + one * wide[j])
                            spot += 1
                return tuple(out)

            zero = jnp.zeros((GROUP, LANES), jnp.float32)
            count = sum((g + 1) * GROUP for g in groups)
            sums = lax.fori_loop(0, depth, step, (zero,) * count, unroll=unroll)
            spot = 0
            for g in groups:
                for r in range(GROUP):
                    finish(g * GROUP + r, sums[spot : spot + g + 1])
                    spot += g + 1

    def square(left, right, finish, base=0):
        product(
            lambda k, i: left[pl.ds(base + k * PITCH + i, 1), :],
            lambda k, j: at(right, k, j),
            slots, finish,
        )

    def gram_done(i, sums):
        put(first_v, i, [part * inverse for part in sums])

    product(
        lambda k, i: dev_ref[pl.ds(k * PITCH + i, 1), :],
        lambda k, j: at(dev_ref, k, j),
        members, gram_done,
    )

    xi = shift * inverse
    mus = []
    for k in range(repeats):
        mu = 1.5 - 0.5 * xi
        scal[pl.ds(k, 1), :] = xi
        scal[pl.ds(repeats + k, 1), :] = mu
        mus.append(mu)
        xi = xi * mu * mu
    after = mus[-1]
    for k in reversed(range(repeats - 1)):
        scal[pl.ds(2 * repeats + k, 1), :] = after
        after = after * mus[k]
    last_z = after
    area = slots * PITCH

    def forward(n, old, new):
        xi = scal[pl.ds(n, 1), :]
        mu = scal[pl.ds(repeats + n, 1), :]
        flat, slope = mu * mu - xi * mu, 0.25 * xi - mu
        base = pl.multiple_of(n * area, GROUP)

        def to_g(i, sums):
            parts = [0.25 * part + slope * at(old, i, j) for j, part in enumerate(sums)]
            parts[-1] = parts[-1] + eye(i % GROUP, flat)
            put(step_g, i, parts)

        square(old, old, to_g)

        def to_v(i, sums):
            put(new, i, sums)
            put(keys, i, [mu * at(step_g, i, j) - 0.5 * part for j, part in enumerate(sums)], base)

        square(step_g, old, to_v)

    def forward_pair(n, carry):
        forward(2 * n + 1, one_v, two_v)
        forward(2 * n + 2, two_v, one_v)
        return carry

    forward(0, first_v, one_v)
    lax.fori_loop(0, repeats // 2 - 1, forward_pair, 0)

    after = scal[pl.ds(3 * repeats - 2, 1), :]
    for i in range(slots):
        parts = [-0.5 * at(keys, i, j, (repeats - 2) * area) for j in range(blocks)]
        parts[i // GROUP] = parts[i // GROUP] - eye(i % GROUP, 0.5 * after)
        for j, part in enumerate(parts):
            one_v[pl.ds(i * PITCH + j * GROUP, GROUP), :] = part

    def backward(n, old, new):
        base = pl.multiple_of(n * area, GROUP)
        half = 0.5 * scal[pl.ds(2 * repeats + n, 1), :]

        def to_h(i, sums):
            parts = list(sums)
            parts[-1] = parts[-1] - eye(i % GROUP, half)
            put(new, i, parts)

        square(keys, old, to_h, base)

    def backward_pair(m, carry):
        backward(repeats - 3 - 2 * m, one_v, two_v)
        backward(repeats - 4 - 2 * m, two_v, one_v)
        return carry

    lax.fori_loop(0, repeats // 2 - 1, backward_pair, 0)

    def whole(ref, k):
        return ref[pl.ds(pl.multiple_of(k * PITCH, GROUP), slots), :]

    none = jnp.zeros((slots, LANES), jnp.float32)

    def apply(ref):
        def step(k, total):
            return total + innov[pl.ds(k, 1), :] * whole(ref, k)

        return lax.fori_loop(0, slots, step, none)

    for _ in range(2):
        start = innov[...]
        innov[...] = apply(one_v)
        innov[...] = last_z * start + apply(first_v)
    gain = innov[...] * inverse
    factor = math.sqrt(shift) * jnp.sqrt(inverse)
    keep_ref[...] = factor * last_z
    both = factor * inverse

    def to_mix(first, sums):
        for r in range(GROUP):
            mix_ref[pl.ds(pl.multiple_of((first + r) * slots, slots), slots), :] = both * sums[r] + gain

    lane_product(
        lambda k, first, r: dev_ref[pl.ds((first + r) * PITCH + k, 1), :],
        lambda k: whole(one_v, k), slots, members, slots, to_mix, unroll=16,
    )


def solve_cells(pool, idx, counts, rows, cols, members):
    slots, cells = idx.shape
    lane = lambda height: pl.BlockSpec((height, LANES), lambda c: (0, c))
    square = pltpu.VMEM((slots * PITCH, LANES), jnp.float32)
    return pl.pallas_call(
        functools.partial(weights_kernel, members, NEWTON, LOC),
        grid=(cells // LANES,),
        in_specs=[pl.BlockSpec(pool.shape, lambda c: (0, 0)), lane(slots), lane(1), lane(1), lane(1)],
        out_specs=[lane(members * PITCH), lane(members * slots), lane(1)],
        out_shape=[
            jax.ShapeDtypeStruct((members * PITCH, cells), jnp.float32),
            jax.ShapeDtypeStruct((members * slots, cells), jnp.float32),
            jax.ShapeDtypeStruct((1, cells), jnp.float32),
        ],
        scratch_shapes=[
            square,
            square,
            square,
            square,
            pltpu.VMEM(((NEWTON - 1) * slots * PITCH, LANES), jnp.float32),
            pltpu.VMEM((slots, LANES), jnp.float32),
            pltpu.VMEM((3 * NEWTON, LANES), jnp.float32),
        ],
        compiler_params=pltpu.CompilerParams(vmem_limit_bytes=40 * 1024 * 1024),
        cost_estimate=pl.CostEstimate(flops=2 * 10**9, bytes_accessed=200 * 10**6, transcendentals=0),
        interpret=INTERPRET,
    )(pool, idx, counts, rows, cols)


def prep_kernel(rows, levels, ens_ref, small_ref, pool_ref, edge_ref, mine_ref, theirs_ref, block, land, spread, send_sems, recv_sems):
    share, fields, _ = mine_ref.shape
    observed = small_ref.shape[1]
    span = fields * rows
    facts = small_ref.shape[0]
    species = fields // levels
    me, place, count = lax.axis_index("mem"), lax.axis_index("space"), lax.axis_size("space")

    def exists(step):
        return (place + step >= 0) & (place + step < count)

    def guard(step, act):
        if step == 0:
            act()
        else:
            pl.when(exists(step))(act)

    ways = [(1, 0), (0, -1), (0, 1), (1, -1), (1, 1)]
    barrier = pltpu.get_barrier_semaphore()

    def target(flip, step):
        return (1 - me if flip else me, place + step)

    for flip, step in ways:
        def greet(flip=flip, step=step):
            pl.semaphore_signal(barrier, inc=1, device_id=target(flip, step), device_id_type=pl.DeviceIdType.MESH)

        guard(step, greet)

    block[pl.ds(share, facts), :] = small_ref[...]
    hot = jnp.where(
        lax.broadcasted_iota(jnp.int32, (LANES, observed), 0).astype(jnp.float32) == small_ref[3:4, :], 1.0, 0.0
    ).astype(jnp.bfloat16)
    wanted = lax.broadcasted_iota(jnp.int32, (rows * species, observed), 0).astype(jnp.float32) == small_ref[4:5, :]

    def look(n, carry):
        for slot in range(UNROLL):
            i = UNROLL * n + slot
            spread[slot] = ens_ref[pl.ds(pl.multiple_of(i * span, span), span), :].astype(jnp.float32)
            lowest = jnp.concatenate(
                [spread[slot, pl.ds(r, species, stride=rows * levels), :] for r in range(rows)], axis=0
            )
            got = jnp.dot(lowest.astype(jnp.bfloat16), hot, preferred_element_type=jnp.float32)
            block[pl.ds(i, 1), :] = jnp.sum(jnp.where(wanted, got, 0.0), axis=0, keepdims=True)
        return carry

    lax.fori_loop(0, share // UNROLL, look, 0)

    greeted = 1 + 2 * exists(-1).astype(jnp.int32) + 2 * exists(1).astype(jnp.int32)
    pl.semaphore_wait(barrier, greeted)

    def copy(n):
        flip, step = ways[n]
        return pltpu.make_async_remote_copy(
            src_ref=block, dst_ref=land.at[1 - step, flip],
            send_sem=send_sems.at[n], recv_sem=recv_sems.at[1 - step, flip],
            device_id=target(flip, step), device_id_type=pl.DeviceIdType.MESH,
        )

    for n, (flip, step) in enumerate(ways):
        guard(step, lambda n=n: copy(n).start())

    def split(n, carry):
        for slot in range(UNROLL):
            i = UNROLL * n + slot
            spread[slot] = ens_ref[pl.ds(pl.multiple_of(i * span, span), span), :].astype(jnp.float32)
            mine_ref[i] = spread[slot, pl.ds(me, fields, stride=rows), :].astype(jnp.bfloat16)
            theirs_ref[i] = spread[slot, pl.ds(1 - me, fields, stride=rows), :].astype(jnp.bfloat16)
        return carry

    lax.fori_loop(0, share // UNROLL, split, 0)

    for n, (flip, step) in enumerate(ways):
        def arrive(n=n):
            copy(n).wait_send()

        guard(step, arrive)
    for n, (flip, step) in enumerate(ways):
        def landed(n=n):
            copy(n).wait_recv()

        guard(-step, landed)
    for step in (-1, 1):
        def blank(step=step):
            land[1 + step] = jnp.zeros_like(land[1 + step])

        pl.when(jnp.logical_not(exists(step)))(blank)
    line = lax.broadcasted_iota(jnp.int32, (GROUP, observed), 0)
    for part in range(3):
        own = block[...] if part == 1 else land[part, 0]
        lanes = pl.ds(part * observed, observed)
        pool_ref[pl.ds(0, share), lanes] = own[:share]
        pool_ref[pl.ds(share, share), lanes] = land[part, 1, pl.ds(0, share), :]
        pool_ref[pl.ds(2 * share, GROUP), lanes] = own[share : share + GROUP] + jnp.where(
            line == 2, float(rows * (part - 1)), 0.0
        )
        edge_ref[part] = own[share + GROUP :]


def prepare(flat, small, members, fields, rows, levels):
    share = members // 2
    observed = small.shape[1]
    high = share + small.shape[0]
    vmem = pl.BlockSpec(memory_space=pltpu.VMEM)
    return pl.pallas_call(
        functools.partial(prep_kernel, rows, levels),
        in_specs=[vmem] * 2,
        out_specs=[vmem] * 4,
        out_shape=[
            jax.ShapeDtypeStruct((members + GROUP, 3 * observed), jnp.float32),
            jax.ShapeDtypeStruct((3, small.shape[0] - GROUP, observed), jnp.float32),
            jax.ShapeDtypeStruct((share, fields, LANES), jnp.bfloat16),
            jax.ShapeDtypeStruct((share, fields, LANES), jnp.bfloat16),
        ],
        scratch_shapes=[
            pltpu.VMEM((high, observed), jnp.float32),
            pltpu.VMEM((3, 2, high, observed), jnp.float32),
            pltpu.VMEM((UNROLL, fields * rows, LANES), jnp.float32),
            pltpu.SemaphoreType.DMA((5,)),
            pltpu.SemaphoreType.DMA((3, 2)),
        ],
        compiler_params=pltpu.CompilerParams(
            vmem_limit_bytes=32 * 1024 * 1024, collective_id=0, has_side_effects=True
        ),
        cost_estimate=pl.CostEstimate(flops=10**8, bytes_accessed=8 * 10**6, transcendentals=0),
        interpret=INTERPRET,
    )(flat, small)


def analysis_kernel(parts, slots, *refs):
    states = refs[:parts]
    dev_ref, mix_ref, keep_ref = refs[parts : parts + 3]
    outs = refs[parts + 3 : 2 * parts + 3]
    anomaly, mapped, mean_ref = refs[2 * parts + 3 :]
    share, width, _ = states[0].shape
    members = share * parts
    total = jnp.zeros((width, LANES), jnp.float32)
    for state in states:
        total = lax.fori_loop(
            0, share, lambda i, t, s=state: t + s[i].astype(jnp.float32), total, unroll=4
        )
    mean = total * (1.0 / members)
    mean_ref[...] = mean
    for part, state in enumerate(states):

        def subtract(i, carry, s=state, base=part * share):
            anomaly[base + i] = s[i].astype(jnp.float32) - mean_ref[...]
            return carry

        lax.fori_loop(0, share, subtract, 0, unroll=4)

    def to_mapped(first, sums):
        for r in range(GROUP):
            mapped[first + r] = sums[r]

    lane_product(
        lambda i, first, r: dev_ref[pl.ds(i * PITCH + first + r, 1), :],
        lambda i: anomaly[i], members, slots, width, to_mapped,
    )
    for part, out in enumerate(outs):
        base = part * share

        def to_out(first, sums, out=out, base=base):
            for r in range(GROUP):
                held = mean_ref[...] + keep_ref[...] * anomaly[base + first + r]
                out[first + r] = (held + sums[r]).astype(jnp.bfloat16)

        lane_product(
            lambda k, first, r, base=base: mix_ref[pl.ds((base + first + r) * slots + k, 1), :],
            lambda k: mapped[k], slots, share, width, to_out,
        )


def finish_kernel(
    slots, width,
    mine_ref, other_ref, dev_ref, mix_ref, keep_ref, edge_ref, loss_ref, out_ref,
    rows, away, south, north, held_ref, anomaly, mapped, mean_ref, coef, weave,
    away_sent, away_come, edge_sent, edge_come, held_sent, held_come,
):
    share, fields, _ = mine_ref.shape
    members = 2 * share
    chunks = fields // width
    group = 2 * LANES // width
    me, place, count = lax.axis_index("mem"), lax.axis_index("space"), lax.axis_size("space")
    mesh_id = pl.DeviceIdType.MESH
    exists = (place > 0, place + 1 < count)
    sides = ((1 - me, place), (me, place - 1), (me, place + 1))
    relays = count % QUAD == 0 and count > QUAD
    floors, floor, corner = count // QUAD, place // QUAD, place % QUAD
    near, far = corner == 0, corner == QUAD - 1
    across = (me, jnp.where(far, place - (QUAD - 1), place + (QUAD - 1)))
    ahead = (me, jnp.where(far, place - QUAD, place + QUAD))
    behind = (me, jnp.where(far, place + QUAD, place - QUAD))
    goes = jnp.where(far, floor > 0, floor < floors - 1)
    comes = jnp.where(far, floor < floors - 1, floor > 0)
    barrier = pltpu.get_barrier_semaphore()
    pl.semaphore_signal(barrier, inc=1, device_id=sides[0], device_id_type=mesh_id)
    for side in range(2):
        @pl.when(exists[side])
        def _():
            pl.semaphore_signal(barrier, inc=1, device_id=sides[1 + side], device_id_type=mesh_id)

    if relays:
        for there, device in ((True, across), (goes, ahead), (comes, behind)):
            @pl.when((near | far) & there)
            def _():
                pl.semaphore_signal(barrier, inc=1, device_id=device, device_id_type=mesh_id)

    for side, buffer in enumerate((south, north)):
        @pl.when(jnp.logical_not(exists[side]))
        def _():
            def clear(n, carry):
                for r in range(2):
                    buffer[r, n // share, n % share] = jnp.zeros((width, LANES), jnp.bfloat16)
                return carry

            lax.fori_loop(0, chunks * share, clear, 0)

    lane = lax.broadcasted_iota(jnp.int32, (GROUP, LANES), 1)
    for at, (part, r) in enumerate(((0, 1), (1, 0), (1, 1), (2, 0))):
        cut = pl.ds(r * LANES, LANES)
        cx = edge_ref[part, pl.ds(0, GROUP), cut]
        cy = edge_ref[part, pl.ds(GROUP, GROUP), cut]
        six = (
            1.0 - cy * cy,
            0.5 * cy * cy - 0.5 * cy,
            0.5 * cy * cy + 0.5 * cy,
            1.0 - cx * cx,
            jnp.where(lane == LANES - 1, 0.0, 0.5 * cx * cx - 0.5 * cx),
            jnp.where(lane == 0, 0.0, 0.5 * cx * cx + 0.5 * cx),
        )
        for n, value in enumerate(six):
            for piece in range(width // GROUP):
                coef[6 * at + n, pl.ds(piece * GROUP, GROUP), :] = value

    greeted = 1 + exists[0].astype(jnp.int32) + exists[1].astype(jnp.int32)
    if relays:
        more = 1 + goes.astype(jnp.int32) + comes.astype(jnp.int32)
        greeted = greeted + jnp.where(near | far, more, 0)
    pl.semaphore_wait(barrier, greeted)

    def share_of(r, q, part):
        return (2 * r + q % 2) * floors < 4 * part

    def detours(side, r, q):
        if side:
            return far & share_of(r, q, floors - 1 - floor)
        return near & share_of(r, q, floor)

    def hand_over(side, r, q):
        return pltpu.make_async_remote_copy(
            src_ref=rows.at[r, q], dst_ref=held_ref.at[r, q],
            send_sem=edge_sent.at[side, r, q], recv_sem=held_come.at[r, q],
            device_id=across, device_id_type=mesh_id,
        )

    def hand_on(side, r, q):
        return pltpu.make_async_remote_copy(
            src_ref=held_ref.at[r, q], dst_ref=(north, south)[side].at[r, q],
            send_sem=held_sent.at[r, q], recv_sem=edge_come.at[side, r, q],
            device_id=ahead, device_id_type=mesh_id,
        )

    def relayed(side, r, q):
        if side:
            return near & share_of(r, q, floors - 1 - floor)
        return far & share_of(r, q, floor)

    def relay(r, q):
        for side in range(2):
            @pl.when(relayed(side, r, q))
            def _():
                hand_over(side, r, q).wait_recv()
                hand_on(side, r, q).start()

    def swap(q):
        return pltpu.make_async_remote_copy(
            src_ref=away.at[q], dst_ref=rows.at[me, q],
            send_sem=away_sent.at[q], recv_sem=away_come.at[q],
            device_id=sides[0], device_id_type=mesh_id,
        )

    def pass_on(side, r, q):
        return pltpu.make_async_remote_copy(
            src_ref=rows.at[r, q], dst_ref=(north, south)[side].at[r, q],
            send_sem=edge_sent.at[side, r, q], recv_sem=edge_come.at[side, r, q],
            device_id=sides[1 + side], device_id_type=mesh_id,
        )

    def pass_both(r, q):
        for side in range(2):
            if not relays:
                pl.when(exists[side])(pass_on(side, r, q).start)
                continue
            turn = detours(side, r, q)

            @pl.when(turn)
            def _():
                hand_over(side, r, q).start()

            @pl.when(exists[side] & jnp.logical_not(turn))
            def _():
                pass_on(side, r, q).start()

    def analyse_chunk(q):
        cut = pl.ds(pl.multiple_of(q * width, width), width)
        total = jnp.zeros((width, LANES), jnp.float32)
        for state in (mine_ref, other_ref):
            total = lax.fori_loop(
                0, share, lambda i, t, s=state: t + s[i, cut, :].astype(jnp.float32), total, unroll=4
            )
        mean_ref[...] = total * (1.0 / members)
        for part, state in enumerate((mine_ref, other_ref)):
            def subtract(i, carry, s=state, base=part * share):
                anomaly[base + i] = s[i, cut, :].astype(jnp.float32) - mean_ref[...]
                return carry

            lax.fori_loop(0, share, subtract, 0, unroll=4)

        def to_mapped(first, sums):
            for r in range(group):
                mapped[first + r] = sums[r]

        lane_product(
            lambda i, first, r: dev_ref[pl.ds(i * PITCH + first + r, 1), :],
            lambda i: anomaly[i], members, slots, width, to_mapped, group=group,
        )
        for part in (0, 1):
            base = part * share

            def to_out(first, sums, base=base, part=part):
                for r in range(group):
                    held = mean_ref[...] + keep_ref[...] * anomaly[base + first + r]
                    value = (held + sums[r]).astype(jnp.bfloat16)
                    if part:
                        away[q, first + r] = value
                    else:
                        rows[me, q, first + r] = value

            lane_product(
                lambda k, first, r, base=base: mix_ref[pl.ds((base + first + r) * slots + k, 1), :],
                lambda k: mapped[k], slots, share, width, to_out, group=group,
            )
            if part:
                swap(q).start()
            else:
                pass_both(me, q)

    def advect_chunk(q):
        cut = pl.ds(pl.multiple_of(q * width, width), width)

        def along(at, low, middle, high):
            now = coef[6 * at] * middle + coef[6 * at + 1] * high + coef[6 * at + 2] * low
            thin = now.astype(jnp.bfloat16)
            east = pltpu.roll(thin, LANES - 1, 1).astype(jnp.float32)
            west = pltpu.roll(thin, 1, 1).astype(jnp.float32)
            return coef[6 * at + 3] * now + coef[6 * at + 4] * east + coef[6 * at + 5] * west

        def several(n, carry):
            for slot in range(UNROLL):
                i = UNROLL * n + slot
                now = [
                    part[r, q, i].astype(jnp.float32) for part in (south, rows, north) for r in range(2)
                ]
                now = [along(at, *now[at : at + 3]) for at in range(4)]
                now = [along(1 + at, *now[at : at + 3]) for at in range(2)]
                for r in range(2):
                    weave[slot, pl.ds(r, width, stride=2), :] = now[r] * loss_ref[r, cut, :]
                start = pl.multiple_of((i * fields + q * width) * 2, 2 * width)
                out_ref[pl.ds(start, 2 * width), :] = weave[slot].astype(jnp.bfloat16)
            return carry

        lax.fori_loop(0, share // UNROLL, several, 0)

    def step(q, carry):
        @pl.when(q < chunks)
        def _():
            analyse_chunk(q)

        @pl.when((q >= 1) & (q - 1 < chunks))
        def _():
            swap(q - 1).wait_recv()
            pass_both(1 - me, q - 1)

        if relays:
            @pl.when((q >= RELAY) & (q - RELAY < chunks))
            def _():
                relay(me, q - RELAY)
                relay(1 - me, q - RELAY)

        @pl.when((q >= LAG) & (q - LAG < chunks))
        def _():
            for side in range(2):
                @pl.when(exists[1 - side])
                def _():
                    for r in range(2):
                        pass_on(side, r, q - LAG).wait_recv()

            advect_chunk(q - LAG)

        return carry

    lax.fori_loop(0, chunks + LAG, step, 0)

    def drain(q, carry):
        swap(q).wait_send()
        for side in range(2):
            @pl.when(exists[side])
            def _():
                for r in range(2):
                    pass_on(side, r, q).wait_send()

            if relays:
                for r in range(2):
                    @pl.when(relayed(side, r, q))
                    def _():
                        hand_on(side, r, q).wait_send()

        return carry

    lax.fori_loop(0, chunks, drain, 0)


def finish(mine, other, dev, mix, keep, edge, loss, slots, rows):
    share, fields, _ = mine.shape
    width = WIDTH
    chunks = fields // width
    vmem = pl.BlockSpec(memory_space=pltpu.VMEM)
    piece = (chunks, share, width, LANES)
    return pl.pallas_call(
        functools.partial(finish_kernel, slots, width),
        in_specs=[vmem] * 7,
        out_specs=vmem,
        out_shape=jax.ShapeDtypeStruct((share * fields * rows, LANES), jnp.bfloat16),
        scratch_shapes=[
            pltpu.VMEM((2,) + piece, jnp.bfloat16),
            pltpu.VMEM(piece, jnp.bfloat16),
            pltpu.VMEM((2,) + piece, jnp.bfloat16),
            pltpu.VMEM((2,) + piece, jnp.bfloat16),
            pltpu.VMEM((2,) + piece, jnp.bfloat16),
            pltpu.VMEM((2 * share, width, LANES), jnp.float32),
            pltpu.VMEM((slots, width, LANES), jnp.float32),
            pltpu.VMEM((width, LANES), jnp.float32),
            pltpu.VMEM((24, width, LANES), jnp.float32),
            pltpu.VMEM((UNROLL, 2 * width, LANES), jnp.float32),
            pltpu.SemaphoreType.DMA((chunks,)),
            pltpu.SemaphoreType.DMA((chunks,)),
            pltpu.SemaphoreType.DMA((2, 2, chunks)),
            pltpu.SemaphoreType.DMA((2, 2, chunks)),
            pltpu.SemaphoreType.DMA((2, chunks)),
            pltpu.SemaphoreType.DMA((2, chunks)),
        ],
        compiler_params=pltpu.CompilerParams(
            vmem_limit_bytes=40 * 1024 * 1024, collective_id=1, has_side_effects=True
        ),
        cost_estimate=pl.CostEstimate(flops=10**9, bytes_accessed=10**7, transcendentals=0),
        interpret=INTERPRET,
    )(mine, other, dev, mix, keep, edge, loss)


def analyse(states, dev, mix, keep, slots, first, count, width):
    share, _, cells = states[0].shape
    parts = len(states)
    members = share * parts
    wide = lambda height: pl.BlockSpec((height, LANES), lambda c, f: (0, c))
    return pl.pallas_call(
        functools.partial(analysis_kernel, parts, slots),
        grid=(cells // LANES, count // width),
        in_specs=[
            pl.BlockSpec((share, width, LANES), lambda c, f: (0, f + first // width, c))
        ] * parts + [wide(members * PITCH), wide(members * slots), wide(1)],
        out_specs=[pl.BlockSpec((share, width, LANES), lambda c, f: (0, f, c))] * parts,
        out_shape=[jax.ShapeDtypeStruct((share, count, cells), jnp.bfloat16)] * parts,
        scratch_shapes=[
            pltpu.VMEM((members, width, LANES), jnp.float32),
            pltpu.VMEM((slots, width, LANES), jnp.float32),
            pltpu.VMEM((width, LANES), jnp.float32),
        ],
        compiler_params=pltpu.CompilerParams(vmem_limit_bytes=32 * 1024 * 1024),
        cost_estimate=pl.CostEstimate(flops=10**9, bytes_accessed=50 * 10**6, transcendentals=0),
        interpret=INTERPRET,
    )(*states, dev, mix, keep)


def halo(cells, width):
    count = lax.axis_size("space")
    before = lax.ppermute(cells[-width:], "space", [(i, i + 1) for i in range(count - 1)])
    after = lax.ppermute(cells[:width], "space", [(i + 1, i) for i in range(count - 1)])
    return before, after


def wide_rows(cells, width):
    before, after = halo(cells, width)
    return jnp.concatenate([before, cells, after], axis=0)


def row_step(south, middle, north, courant):
    return (
        middle
        - 0.5 * courant * (north - south)
        + 0.5 * courant * courant * (north - 2.0 * middle + south)
    )


def col_step(middle, courant):
    padded = jnp.pad(middle, [(0, 0)] * (middle.ndim - 1) + [(1, 1)])
    east, west = padded[..., 2:], padded[..., :-2]
    return (
        middle
        - 0.5 * courant * (east - west)
        + 0.5 * courant * courant * (east - 2.0 * middle + west)
    )


def shards(
    ensemble, obs_value, obs_error, obs_cell, obs_species, patch_index, patch_count,
    courant_x, courant_y, dep_velocity, surface_factor,
):
    local_members, fields, tile_rows, columns = ensemble.shape
    species = dep_velocity.shape[0]
    levels = fields // species
    tile_cells = tile_rows * columns
    groups = lax.axis_size("mem")
    members = local_members * groups
    me = lax.axis_index("mem")
    slots = patch_index.shape[2]
    per_dev = tile_cells // groups
    paired = groups == 2 and tile_rows == 2 and columns == LANES
    paired = paired and GROUP % levels == 0 and fields % WIDTH == 0 and species % GROUP == 0
    paired = paired and local_members % UNROLL == 0
    swap = [(0, 1), (1, 0)]

    if paired:
        tall = GROUP // levels
        small = jnp.concatenate(
            [
                obs_value,
                obs_error,
                (obs_cell // columns).astype(jnp.float32),
                (obs_cell % columns).astype(jnp.float32),
                (obs_cell // columns * species + obs_species).astype(jnp.float32),
                jnp.zeros((GROUP - 5, obs_value.shape[1]), jnp.float32),
            ]
            + [courant_x.reshape(levels, tile_cells)] * tall
            + [courant_y.reshape(levels, tile_cells)] * tall,
            axis=0,
        )
        pool, edge, mine, theirs = prepare(
            ensemble.reshape(-1, columns), small, members, fields, tile_rows, levels
        )
    else:
        surface = ensemble.reshape(local_members, species, levels, tile_cells)[:, :, 0]
        position = obs_species[0] * tile_cells + obs_cell[0]
        equiv = jnp.take(surface.reshape(local_members, -1), position, axis=1).astype(jnp.float32)
        equiv = lax.all_gather(equiv, "mem", axis=0, tiled=True)
        zeros = jnp.zeros_like(obs_value[0])
        info = jnp.stack(
            [
                obs_value[0],
                obs_error[0],
                (obs_cell[0] // columns).astype(jnp.float32),
                (obs_cell[0] % columns).astype(jnp.float32),
            ]
            + [zeros] * 4
        )
        packed = jnp.concatenate([equiv, info], axis=0)
        before, after = halo(packed[None], 1)
        offset = jnp.zeros((packed.shape[0], 1), jnp.float32).at[members + 2, 0].set(float(tile_rows))
        pool = jnp.concatenate([before[0] - offset, packed, after[0] + offset], axis=1)

    if paired:
        states = (mine, lax.ppermute(theirs, "mem", swap))
    else:
        states = (
            lax.all_to_all(
                ensemble.reshape(local_members, fields, tile_cells),
                "mem", split_axis=2, concat_axis=0, tiled=True,
            ),
        )
    spare = -per_dev % LANES
    pad = lambda a: jnp.pad(a, [(0, 0)] * (a.ndim - 1) + [(0, spare)]) if spare else a
    states = tuple(pad(state) for state in states)
    cell = me * per_dev + jnp.arange(per_dev, dtype=jnp.int32)
    dev, mix, keep = solve_cells(
        pool,
        pad(jnp.transpose(patch_index[0])),
        pad(patch_count),
        pad((cell // columns).astype(jnp.float32)[None]),
        pad((cell % columns).astype(jnp.float32)[None]),
        members,
    )

    loss = jnp.exp(-dep_velocity[:, None, None] * surface_factor[None])
    if paired:
        lowest = (jnp.arange(levels, dtype=jnp.int32) == 0)[None, None, :, None]
        factor = jnp.where(lowest, jnp.moveaxis(loss, 1, 0)[:, :, None], 1.0).reshape(tile_rows, fields, columns)
        out = finish(*states, dev, mix, keep, edge, factor, slots, tile_rows)
        return out.reshape(ensemble.shape)

    width = next(w for w in (32, 16, fields) if fields % w == 0)
    wide_x = wide_rows(jnp.moveaxis(courant_x, 1, 0), SUBSTEPS)
    wide_y = wide_rows(jnp.moveaxis(courant_y, 1, 0), SUBSTEPS)
    out = analyse(states, dev, mix, keep, slots, 0, fields, width)
    back = lax.all_to_all(out[0][..., :per_dev], "mem", split_axis=0, concat_axis=2, tiled=True)
    rows = jnp.moveaxis(back.reshape(local_members, fields, tile_rows, columns), 2, 0)
    south, north = halo(rows, SUBSTEPS)
    shape = (local_members, species, levels, columns)
    now = [
        part[r].reshape(shape).astype(jnp.float32)
        for part in (south, rows, north)
        for r in range(part.shape[0])
    ]
    for repeat in range(SUBSTEPS):
        first = repeat + 1
        now = [
            col_step(
                row_step(now[r - 1], now[r], now[r + 1], wide_y[first + r - 1]),
                wide_x[first + r - 1],
            )
            for r in range(1, len(now) - 1)
        ]
    lowest = (jnp.arange(levels, dtype=jnp.int32) == 0)[:, None]
    now = [row * jnp.where(lowest, loss[:, r][:, None], 1.0) for r, row in enumerate(now)]
    joined = jnp.stack([row.astype(jnp.bfloat16) for row in now], axis=3)
    return joined.reshape(local_members, fields, tile_rows, columns)


def solution(mesh):
    in_specs = (
        P("mem", None, "space", None),
        P("space", None),
        P("space", None),
        P("space", None),
        P("space", None),
        P("space", "mem", None),
        P("space", "mem"),
        P(None, "space", None),
        P(None, "space", None),
        P(),
        P("space", None),
    )
    out_specs = P("mem", None, "space", None)
    return jax.shard_map(shards, mesh=mesh, in_specs=in_specs, out_specs=out_specs, check_vma=False)
```

```python
import functools
import math

import jax
import jax.numpy as jnp
from jax import lax
from jax.experimental import pallas as pl
from jax.experimental.pallas import tpu as pltpu
from jax.sharding import PartitionSpec as P

NEWTON = 8
SUBSTEPS = 2
LOC = 1
LANES = 128
GROUP = 8
PITCH = 40
WIDTH = 16
LAG = 6
RELAY = 3
LATE = 3
QUAD = 4
UNROLL = 8
INTERPRET = False


def lane_product(left, right, depth, rows, width, finish, unroll=4, group=GROUP):
    def several(block, carry):
        first = pl.multiple_of(block * group, group)

        def step(k, sums):
            row = right(k)
            return tuple(sums[r] + left(k, first, r) * row for r in range(group))

        zero = jnp.zeros((width, LANES), jnp.float32)
        sums = lax.fori_loop(0, depth, step, (zero,) * group, unroll=unroll)
        finish(first, sums)
        return carry

    lax.fori_loop(0, rows // group, several, 0)


def weights_kernel(
    members, repeats, radius,
    pool_ref, idx_ref, cnt_ref, row_ref, col_ref,
    dev_ref, mix_ref, keep_ref,
    first_v, one_v, two_v, step_g, keys, innov, scal,
):
    slots = idx_ref.shape[0]
    pooled = pool_ref.shape[1]
    blocks = slots // GROUP
    info = pool_ref[members:, :]
    high = info.astype(jnp.bfloat16).astype(jnp.float32)
    rest = info - high
    middle = rest.astype(jnp.bfloat16).astype(jnp.float32)
    low = rest - middle
    table = jnp.concatenate([pool_ref[:members, :], high, middle, low, jnp.zeros_like(low)], axis=0)
    table = table.astype(jnp.bfloat16)
    place = lax.broadcasted_iota(jnp.int32, (pooled, LANES), 0)
    extra = info.shape[0]

    def pick(k, total):
        hot = jnp.where(place == idx_ref[pl.ds(k, 1), :], 1.0, 0.0).astype(jnp.bfloat16)
        got = jnp.dot(table, hot, preferred_element_type=jnp.float32)
        equiv = got[:members]
        facts = (
            got[members : members + extra]
            + got[members + extra : members + 2 * extra]
            + got[members + 2 * extra : members + 3 * extra]
        )
        mean = jnp.sum(equiv, axis=0, keepdims=True) * (1.0 / members)
        dist = (facts[2:3] - row_ref[...]) ** 2 + (facts[3:4] - col_ref[...]) ** 2
        rho = jnp.exp(-dist / (2.0 * radius * radius)) / facts[1:2]
        scale = jnp.sqrt(jnp.where(k < cnt_ref[...], rho, 0.0))
        scaled = (equiv - mean) * scale
        dev_ref[pl.ds(k, members, stride=PITCH), :] = scaled
        innov[pl.ds(k, 1), :] = (facts[0:1] - mean) * scale
        return total + jnp.sum(scaled * scaled, axis=0, keepdims=True)

    spread = lax.fori_loop(0, slots, pick, jnp.zeros((1, LANES), jnp.float32), unroll=8)
    shift = members - 1.0
    inverse = 1.0 / (spread + shift * members)
    level = lax.broadcasted_iota(jnp.int32, (GROUP, LANES), 0)

    def eye(r, value):
        return jnp.where(level == r, value, 0.0)

    def at(ref, i, j, base=0):
        start = i * PITCH + j * GROUP
        start = start if isinstance(start, int) else pl.multiple_of(start, GROUP)
        return ref[pl.ds(base + start, GROUP), :]

    def put(ref, i, parts, base=0):
        for j, part in enumerate(parts):
            ref[pl.ds(base + i * PITCH + j * GROUP, GROUP), :] = part
            if j < i // GROUP:
                ref[pl.ds(base + j * GROUP * PITCH + i, GROUP, stride=PITCH), :] = part

    def product(left, right, depth, finish, unroll=16):
        for pair in range((blocks + 1) // 2):
            groups = sorted({pair, blocks - 1 - pair})

            def step(k, sums):
                wide = [right(k, j) for j in range(groups[-1] + 1)]
                out, spot = [], 0
                for g in groups:
                    for r in range(GROUP):
                        one = left(k, g * GROUP + r)
                        for j in range(g + 1):
                            out.append(sums[spot] + one * wide[j])
                            spot += 1
                return tuple(out)

            zero = jnp.zeros((GROUP, LANES), jnp.float32)
            count = sum((g + 1) * GROUP for g in groups)
            sums = lax.fori_loop(0, depth, step, (zero,) * count, unroll=unroll)
            spot = 0
            for g in groups:
                for r in range(GROUP):
                    finish(g * GROUP + r, sums[spot : spot + g + 1])
                    spot += g + 1

    def square(left, right, finish, base=0):
        product(
            lambda k, i: left[pl.ds(base + k * PITCH + i, 1), :],
            lambda k, j: at(right, k, j),
            slots, finish,
        )

    def gram_done(i, sums):
        put(first_v, i, [part * inverse for part in sums])

    product(
        lambda k, i: dev_ref[pl.ds(k * PITCH + i, 1), :],
        lambda k, j: at(dev_ref, k, j),
        members, gram_done,
    )

    xi = shift * inverse
    mus = []
    for k in range(repeats):
        mu = 1.5 - 0.5 * xi
        scal[pl.ds(k, 1), :] = xi
        scal[pl.ds(repeats + k, 1), :] = mu
        mus.append(mu)
        xi = xi * mu * mu
    after = mus[-1]
    for k in reversed(range(repeats - 1)):
        scal[pl.ds(2 * repeats + k, 1), :] = after
        after = after * mus[k]
    last_z = after
    area = slots * PITCH

    def forward(n, old, new):
        xi = scal[pl.ds(n, 1), :]
        mu = scal[pl.ds(repeats + n, 1), :]
        flat, slope = mu * mu - xi * mu, 0.25 * xi - mu
        base = pl.multiple_of(n * area, GROUP)

        def to_g(i, sums):
            parts = [0.25 * part + slope * at(old, i, j) for j, part in enumerate(sums)]
            parts[-1] = parts[-1] + eye(i % GROUP, flat)
            put(step_g, i, parts)

        square(old, old, to_g)

        def to_v(i, sums):
            put(new, i, sums)
            put(keys, i, [mu * at(step_g, i, j) - 0.5 * part for j, part in enumerate(sums)], base)

        square(step_g, old, to_v)

    def forward_pair(n, carry):
        forward(2 * n + 1, one_v, two_v)
        forward(2 * n + 2, two_v, one_v)
        return carry

    forward(0, first_v, one_v)
    lax.fori_loop(0, repeats // 2 - 1, forward_pair, 0)

    after = scal[pl.ds(3 * repeats - 2, 1), :]
    for i in range(slots):
        parts = [-0.5 * at(keys, i, j, (repeats - 2) * area) for j in range(blocks)]
        parts[i // GROUP] = parts[i // GROUP] - eye(i % GROUP, 0.5 * after)
        for j, part in enumerate(parts):
            one_v[pl.ds(i * PITCH + j * GROUP, GROUP), :] = part

    def backward(n, old, new):
        base = pl.multiple_of(n * area, GROUP)
        half = 0.5 * scal[pl.ds(2 * repeats + n, 1), :]

        def to_h(i, sums):
            parts = list(sums)
            parts[-1] = parts[-1] - eye(i % GROUP, half)
            put(new, i, parts)

        square(keys, old, to_h, base)

    def backward_pair(m, carry):
        backward(repeats - 3 - 2 * m, one_v, two_v)
        backward(repeats - 4 - 2 * m, two_v, one_v)
        return carry

    lax.fori_loop(0, repeats // 2 - 1, backward_pair, 0)

    def whole(ref, k):
        return ref[pl.ds(pl.multiple_of(k * PITCH, GROUP), slots), :]

    none = jnp.zeros((slots, LANES), jnp.float32)

    def apply(ref):
        def step(k, total):
            return total + innov[pl.ds(k, 1), :] * whole(ref, k)

        return lax.fori_loop(0, slots, step, none)

    for _ in range(2):
        start = innov[...]
        innov[...] = apply(one_v)
        innov[...] = last_z * start + apply(first_v)
    gain = innov[...] * inverse
    factor = math.sqrt(shift) * jnp.sqrt(inverse)
    keep_ref[...] = factor * last_z
    both = factor * inverse

    def to_mix(first, sums):
        for r in range(GROUP):
            mix_ref[pl.ds(pl.multiple_of((first + r) * slots, slots), slots), :] = both * sums[r] + gain

    lane_product(
        lambda k, first, r: dev_ref[pl.ds((first + r) * PITCH + k, 1), :],
        lambda k: whole(one_v, k), slots, members, slots, to_mix, unroll=16,
    )


def solve_cells(pool, idx, counts, rows, cols, members):
    slots, cells = idx.shape
    lane = lambda height: pl.BlockSpec((height, LANES), lambda c: (0, c))
    square = pltpu.VMEM((slots * PITCH, LANES), jnp.float32)
    return pl.pallas_call(
        functools.partial(weights_kernel, members, NEWTON, LOC),
        grid=(cells // LANES,),
        in_specs=[pl.BlockSpec(pool.shape, lambda c: (0, 0)), lane(slots), lane(1), lane(1), lane(1)],
        out_specs=[lane(members * PITCH), lane(members * slots), lane(1)],
        out_shape=[
            jax.ShapeDtypeStruct((members * PITCH, cells), jnp.float32),
            jax.ShapeDtypeStruct((members * slots, cells), jnp.float32),
            jax.ShapeDtypeStruct((1, cells), jnp.float32),
        ],
        scratch_shapes=[
            square,
            square,
            square,
            square,
            pltpu.VMEM(((NEWTON - 1) * slots * PITCH, LANES), jnp.float32),
            pltpu.VMEM((slots, LANES), jnp.float32),
            pltpu.VMEM((3 * NEWTON, LANES), jnp.float32),
        ],
        compiler_params=pltpu.CompilerParams(vmem_limit_bytes=40 * 1024 * 1024),
        cost_estimate=pl.CostEstimate(flops=2 * 10**9, bytes_accessed=200 * 10**6, transcendentals=0),
        interpret=INTERPRET,
    )(pool, idx, counts, rows, cols)


def split_kernel(rows, levels, flat_ref, mine_ref, early_ref, late_ref, lowest_ref, spread):
    me = lax.axis_index("mem")
    batch, fields, _ = mine_ref.shape
    species = fields // levels
    span = fields * rows
    for slot in range(batch):
        spread[slot] = flat_ref[pl.ds(slot * span, span), :].astype(jnp.float32)
        mine_ref[slot] = spread[slot, pl.ds(me, fields, stride=rows), :].astype(jnp.bfloat16)
        theirs = spread[slot, pl.ds(1 - me, fields, stride=rows), :].astype(jnp.bfloat16)
        early_ref[slot] = theirs[: early_ref.shape[1]]
        late_ref[slot] = theirs[early_ref.shape[1] :]
        lowest_ref[slot] = jnp.concatenate(
            [spread[slot, pl.ds(r, species, stride=rows * levels), :] for r in range(rows)], axis=0
        ).astype(jnp.bfloat16)


def separate(flat, share, fields, rows, levels):
    span = fields * rows
    block = lambda height: pl.BlockSpec((UNROLL, height, LANES), lambda n: (n, 0, 0))
    out = lambda height: jax.ShapeDtypeStruct((share, height, LANES), jnp.bfloat16)
    late = LATE * WIDTH
    heights = (fields, fields - late, late, rows * fields // levels)
    return pl.pallas_call(
        functools.partial(split_kernel, rows, levels),
        grid=(share // UNROLL,),
        in_specs=[pl.BlockSpec((UNROLL * span, LANES), lambda n: (n, 0))],
        out_specs=[block(height) for height in heights],
        out_shape=[out(height) for height in heights],
        scratch_shapes=[pltpu.VMEM((UNROLL, span, LANES), jnp.float32)],
        compiler_params=pltpu.CompilerParams(vmem_limit_bytes=16 * 1024 * 1024),
        cost_estimate=pl.CostEstimate(flops=10**7, bytes_accessed=6 * 10**6, transcendentals=0),
        interpret=INTERPRET,
    )(flat)


def prep_kernel(
    rows, species,
    lowest_ref, value_ref, error_ref, cell_ref, species_ref, courant_x_ref, courant_y_ref,
    pool_ref, edge_ref, found, block, facts_ref, land, land_facts, send_sems, recv_sems, facts_sent, facts_come,
):
    share = lowest_ref.shape[0]
    observed = value_ref.shape[1]
    levels = courant_x_ref.shape[0] // rows
    me, place, count = lax.axis_index("mem"), lax.axis_index("space"), lax.axis_size("space")

    def exists(step):
        return (place + step >= 0) & (place + step < count)

    def guard(step, act):
        if step == 0:
            act()
        else:
            pl.when(exists(step))(act)

    ways = [(1, 0), (0, -1), (0, 1), (1, -1), (1, 1)]
    barrier = pltpu.get_barrier_semaphore()

    def target(flip, step):
        return (1 - me if flip else me, place + step)

    for flip, step in ways:
        def greet(flip=flip, step=step):
            pl.semaphore_signal(barrier, inc=1, device_id=target(flip, step), device_id_type=pl.DeviceIdType.MESH)

        guard(step, greet)

    cell = cell_ref[...]
    row, column = lax.shift_right_logical(cell, LANES.bit_length() - 1), cell & (LANES - 1)
    facts_ref[pl.ds(0, GROUP), :] = jnp.zeros((GROUP, observed), jnp.float32)
    facts = (value_ref[...], error_ref[...], row.astype(jnp.float32), column.astype(jnp.float32))
    for n, fact in enumerate(facts):
        facts_ref[pl.ds(n, 1), :] = fact
    for n, courant in enumerate((courant_x_ref, courant_y_ref)):
        for copy in range(GROUP // levels):
            for r in range(rows):
                start = (n + 1) * GROUP + copy * levels
                facts_ref[pl.ds(start, levels), pl.ds(r * LANES, LANES)] = courant[pl.ds(r, levels, stride=rows), :]
    hot = jnp.where(lax.broadcasted_iota(jnp.int32, (LANES, observed), 0) == column, 1.0, 0.0).astype(jnp.bfloat16)
    wanted = lax.broadcasted_iota(jnp.int32, (rows * species, observed), 0) == row * species + species_ref[...]

    def look(n, carry):
        for slot in range(UNROLL):
            i = UNROLL * n + slot
            got = jnp.dot(lowest_ref[i], hot, preferred_element_type=jnp.float32)
            found[pl.ds(i, 1), :] = jnp.sum(jnp.where(wanted, got, 0.0), axis=0, keepdims=True)
        return carry

    lax.fori_loop(0, share // UNROLL, look, 0)
    block[...] = found[...].astype(jnp.bfloat16)

    greeted = 1 + 2 * exists(-1).astype(jnp.int32) + 2 * exists(1).astype(jnp.int32)
    pl.semaphore_wait(barrier, greeted)

    def copy(n):
        flip, step = ways[n]
        return pltpu.make_async_remote_copy(
            src_ref=block, dst_ref=land.at[1 - step, flip],
            send_sem=send_sems.at[n], recv_sem=recv_sems.at[1 - step, flip],
            device_id=target(flip, step), device_id_type=pl.DeviceIdType.MESH,
        )

    def copy_facts(step):
        return pltpu.make_async_remote_copy(
            src_ref=facts_ref, dst_ref=land_facts.at[1 - step],
            send_sem=facts_sent.at[1 - step], recv_sem=facts_come.at[1 - step],
            device_id=(me, place + step), device_id_type=pl.DeviceIdType.MESH,
        )

    for n, (flip, step) in enumerate(ways):
        guard(step, lambda n=n: copy(n).start())
    for step in (-1, 1):
        guard(step, lambda step=step: copy_facts(step).start())
    for step in (-1, 1):
        def blank(step=step):
            land[1 + step] = jnp.zeros_like(land[1 + step])
            land_facts[1 + step] = jnp.zeros_like(land_facts[1 + step])

        pl.when(jnp.logical_not(exists(step)))(blank)
    for n, (flip, step) in enumerate(ways):
        def landed(n=n):
            copy(n).wait_recv()

        guard(-step, landed)
    for step in (-1, 1):
        guard(-step, lambda step=step: copy_facts(step).wait_recv())
    line = lax.broadcasted_iota(jnp.int32, (GROUP, observed), 0)
    for part in range(3):
        lanes = pl.ds(part * observed, observed)
        own = found[...] if part == 1 else land[part, 0].astype(jnp.float32)
        facts = (facts_ref if part == 1 else land_facts.at[part])[...]
        pool_ref[pl.ds(0, share), lanes] = own
        pool_ref[pl.ds(share, share), lanes] = land[part, 1].astype(jnp.float32)
        pool_ref[pl.ds(2 * share, GROUP), lanes] = facts[:GROUP] + jnp.where(
            line == 2, float(rows * (part - 1)), 0.0
        )
        edge_ref[part] = facts[GROUP:]
    for n, (flip, step) in enumerate(ways):
        def sent(n=n):
            copy(n).wait_send()

        guard(step, sent)
    for step in (-1, 1):
        guard(step, lambda step=step: copy_facts(step).wait_send())


def prepare(lowest, facts, courants, rows, species):
    share = lowest.shape[0]
    observed = facts[0].shape[1]
    vmem = pl.BlockSpec(memory_space=pltpu.VMEM)
    return pl.pallas_call(
        functools.partial(prep_kernel, rows, species),
        in_specs=[vmem] * 7,
        out_specs=[vmem] * 2,
        out_shape=[
            jax.ShapeDtypeStruct((2 * share + GROUP, 3 * observed), jnp.float32),
            jax.ShapeDtypeStruct((3, 2 * GROUP, observed), jnp.float32),
        ],
        scratch_shapes=[
            pltpu.VMEM((share, observed), jnp.float32),
            pltpu.VMEM((share, observed), jnp.bfloat16),
            pltpu.VMEM((3 * GROUP, observed), jnp.float32),
            pltpu.VMEM((3, 2, share, observed), jnp.bfloat16),
            pltpu.VMEM((3, 3 * GROUP, observed), jnp.float32),
            pltpu.SemaphoreType.DMA((5,)),
            pltpu.SemaphoreType.DMA((3, 2)),
            pltpu.SemaphoreType.DMA((3,)),
            pltpu.SemaphoreType.DMA((3,)),
        ],
        compiler_params=pltpu.CompilerParams(
            vmem_limit_bytes=16 * 1024 * 1024, collective_id=0, has_side_effects=True
        ),
        cost_estimate=pl.CostEstimate(flops=10**8, bytes_accessed=10**6, transcendentals=0),
        interpret=INTERPRET,
    )(lowest, *facts, *courants)


def analysis_kernel(parts, slots, *refs):
    states = refs[:parts]
    dev_ref, mix_ref, keep_ref = refs[parts : parts + 3]
    outs = refs[parts + 3 : 2 * parts + 3]
    anomaly, mapped, mean_ref = refs[2 * parts + 3 :]
    share, width, _ = states[0].shape
    members = share * parts
    total = jnp.zeros((width, LANES), jnp.float32)
    for state in states:
        total = lax.fori_loop(
            0, share, lambda i, t, s=state: t + s[i].astype(jnp.float32), total, unroll=4
        )
    mean = total * (1.0 / members)
    mean_ref[...] = mean
    for part, state in enumerate(states):

        def subtract(i, carry, s=state, base=part * share):
            anomaly[base + i] = s[i].astype(jnp.float32) - mean_ref[...]
            return carry

        lax.fori_loop(0, share, subtract, 0, unroll=4)

    def to_mapped(first, sums):
        for r in range(GROUP):
            mapped[first + r] = sums[r]

    lane_product(
        lambda i, first, r: dev_ref[pl.ds(i * PITCH + first + r, 1), :],
        lambda i: anomaly[i], members, slots, width, to_mapped,
    )
    for part, out in enumerate(outs):
        base = part * share

        def to_out(first, sums, out=out, base=base):
            for r in range(GROUP):
                held = mean_ref[...] + keep_ref[...] * anomaly[base + first + r]
                out[first + r] = (held + sums[r]).astype(jnp.bfloat16)

        lane_product(
            lambda k, first, r, base=base: mix_ref[pl.ds((base + first + r) * slots + k, 1), :],
            lambda k: mapped[k], slots, share, width, to_out,
        )


def finish_kernel(
    slots, width,
    mine_ref, other_ref, theirs_ref, dev_ref, mix_ref, keep_ref, edge_ref, loss_ref, out_ref,
    rows, away, south, north, held_ref, late_ref, anomaly, mapped, mean_ref, coef, weave,
    away_sent, away_come, edge_sent, edge_come, held_sent, held_come, late_sent, late_come,
):
    share, fields, _ = mine_ref.shape
    members = 2 * share
    chunks = fields // width
    early = other_ref.shape[1] // width
    group = 2 * LANES // width
    me, place, count = lax.axis_index("mem"), lax.axis_index("space"), lax.axis_size("space")
    mesh_id = pl.DeviceIdType.MESH
    exists = (place > 0, place + 1 < count)
    sides = ((1 - me, place), (me, place - 1), (me, place + 1))
    relays = count % QUAD == 0 and count > QUAD
    floors, floor, corner = count // QUAD, place // QUAD, place % QUAD
    near, far = corner == 0, corner == QUAD - 1
    across = (me, jnp.where(far, place - (QUAD - 1), place + (QUAD - 1)))
    ahead = (me, jnp.where(far, place - QUAD, place + QUAD))
    behind = (me, jnp.where(far, place + QUAD, place - QUAD))
    goes = jnp.where(far, floor > 0, floor < floors - 1)
    comes = jnp.where(far, floor < floors - 1, floor > 0)
    barrier = pltpu.get_barrier_semaphore()
    pl.semaphore_signal(barrier, inc=1, device_id=sides[0], device_id_type=mesh_id)
    for side in range(2):
        @pl.when(exists[side])
        def _():
            pl.semaphore_signal(barrier, inc=1, device_id=sides[1 + side], device_id_type=mesh_id)

    if relays:
        for there, device in ((True, across), (goes, ahead), (comes, behind)):
            @pl.when((near | far) & there)
            def _():
                pl.semaphore_signal(barrier, inc=1, device_id=device, device_id_type=mesh_id)

    for side, buffer in enumerate((south, north)):
        @pl.when(jnp.logical_not(exists[side]))
        def _():
            def clear(n, carry):
                for r in range(2):
                    buffer[r, n // share, n % share] = jnp.zeros((width, LANES), jnp.bfloat16)
                return carry

            lax.fori_loop(0, chunks * share, clear, 0)

    lane = lax.broadcasted_iota(jnp.int32, (GROUP, LANES), 1)
    for at, (part, r) in enumerate(((0, 1), (1, 0), (1, 1), (2, 0))):
        cut = pl.ds(r * LANES, LANES)
        cx = edge_ref[part, pl.ds(0, GROUP), cut]
        cy = edge_ref[part, pl.ds(GROUP, GROUP), cut]
        six = (
            1.0 - cy * cy,
            0.5 * cy * cy - 0.5 * cy,
            0.5 * cy * cy + 0.5 * cy,
            1.0 - cx * cx,
            jnp.where(lane == LANES - 1, 0.0, 0.5 * cx * cx - 0.5 * cx),
            jnp.where(lane == 0, 0.0, 0.5 * cx * cx + 0.5 * cx),
        )
        for n, value in enumerate(six):
            for piece in range(width // GROUP):
                coef[6 * at + n, pl.ds(piece * GROUP, GROUP), :] = value

    greeted = 1 + exists[0].astype(jnp.int32) + exists[1].astype(jnp.int32)
    if relays:
        more = 1 + goes.astype(jnp.int32) + comes.astype(jnp.int32)
        greeted = greeted + jnp.where(near | far, more, 0)
    pl.semaphore_wait(barrier, greeted)

    def share_of(r, q, part):
        return (2 * r + q % 2) * floors < 4 * part

    def detours(side, r, q):
        if side:
            return far & share_of(r, q, floors - 1 - floor)
        return near & share_of(r, q, floor)

    def hand_over(side, r, q):
        return pltpu.make_async_remote_copy(
            src_ref=rows.at[r, q], dst_ref=held_ref.at[r, q],
            send_sem=edge_sent.at[side, r, q], recv_sem=held_come.at[r, q],
            device_id=across, device_id_type=mesh_id,
        )

    def hand_on(side, r, q):
        return pltpu.make_async_remote_copy(
            src_ref=held_ref.at[r, q], dst_ref=(north, south)[side].at[r, q],
            send_sem=held_sent.at[r, q], recv_sem=edge_come.at[side, r, q],
            device_id=ahead, device_id_type=mesh_id,
        )

    def relayed(side, r, q):
        if side:
            return near & share_of(r, q, floors - 1 - floor)
        return far & share_of(r, q, floor)

    def relay(r, q):
        for side in range(2):
            @pl.when(relayed(side, r, q))
            def _():
                hand_over(side, r, q).wait_recv()
                hand_on(side, r, q).start()

    def swap(q):
        return pltpu.make_async_remote_copy(
            src_ref=away.at[q], dst_ref=rows.at[me, q],
            send_sem=away_sent.at[q], recv_sem=away_come.at[q],
            device_id=sides[0], device_id_type=mesh_id,
        )

    def pass_on(side, r, q):
        return pltpu.make_async_remote_copy(
            src_ref=rows.at[r, q], dst_ref=(north, south)[side].at[r, q],
            send_sem=edge_sent.at[side, r, q], recv_sem=edge_come.at[side, r, q],
            device_id=sides[1 + side], device_id_type=mesh_id,
        )

    def pass_both(r, q):
        for side in range(2):
            if not relays:
                pl.when(exists[side])(pass_on(side, r, q).start)
                continue
            turn = detours(side, r, q)

            @pl.when(turn)
            def _():
                hand_over(side, r, q).start()

            @pl.when(exists[side] & jnp.logical_not(turn))
            def _():
                pass_on(side, r, q).start()

    def follow(n):
        return pltpu.make_async_remote_copy(
            src_ref=theirs_ref.at[:, pl.ds(pl.multiple_of(n * width, width), width), :], dst_ref=late_ref.at[n],
            send_sem=late_sent.at[n], recv_sem=late_come.at[n],
            device_id=sides[0], device_id_type=mesh_id,
        )

    def analyse_chunk(q):
        cut = pl.ds(pl.multiple_of(q * width, width), width)
        zero = jnp.zeros((width, LANES), jnp.float32)

        def fill(load, base):
            def one(i, total):
                value = load(i).astype(jnp.float32)
                anomaly[base + i] = value
                return total + value

            return lax.fori_loop(0, share, one, zero, unroll=4)

        mean_ref[...] = fill(lambda i: mine_ref[i, cut, :], 0)

        @pl.when(q < early)
        def _():
            mean_ref[...] += fill(lambda i: other_ref[i, cut, :], share)

        @pl.when(q >= early)
        def _():
            follow(q - early).wait_recv()
            mean_ref[...] += fill(lambda i: late_ref[q - early, i], share)

        mean = mean_ref[...] * (1.0 / members)
        mean_ref[...] = mean

        def subtract(i, carry):
            anomaly[i] = anomaly[i] - mean
            return carry

        lax.fori_loop(0, members, subtract, 0, unroll=8)

        def to_mapped(first, sums):
            for r in range(group):
                mapped[first + r] = sums[r]

        lane_product(
            lambda i, first, r: dev_ref[pl.ds(i * PITCH + first + r, 1), :],
            lambda i: anomaly[i], members, slots, width, to_mapped, group=group,
        )
        for part in (0, 1):
            base = part * share

            def to_out(first, sums, base=base, part=part):
                for r in range(group):
                    held = mean_ref[...] + keep_ref[...] * anomaly[base + first + r]
                    value = (held + sums[r]).astype(jnp.bfloat16)
                    if part:
                        away[q, first + r] = value
                    else:
                        rows[me, q, first + r] = value

            lane_product(
                lambda k, first, r, base=base: mix_ref[pl.ds((base + first + r) * slots + k, 1), :],
                lambda k: mapped[k], slots, share, width, to_out, group=group,
            )
            if part:
                swap(q).start()

                @pl.when(q < chunks - early)
                def _():
                    follow(q).start()
            else:
                pass_both(me, q)

    def advect_chunk(q):
        cut = pl.ds(pl.multiple_of(q * width, width), width)

        def along(at, low, middle, high):
            now = coef[6 * at] * middle + coef[6 * at + 1] * high + coef[6 * at + 2] * low
            thin = now.astype(jnp.bfloat16)
            east = pltpu.roll(thin, LANES - 1, 1).astype(jnp.float32)
            west = pltpu.roll(thin, 1, 1).astype(jnp.float32)
            return coef[6 * at + 3] * now + coef[6 * at + 4] * east + coef[6 * at + 5] * west

        def several(n, carry):
            for slot in range(UNROLL):
                i = UNROLL * n + slot
                now = [
                    part[r, q, i].astype(jnp.float32) for part in (south, rows, north) for r in range(2)
                ]
                now = [along(at, *now[at : at + 3]) for at in range(4)]
                now = [along(1 + at, *now[at : at + 3]) for at in range(2)]
                for r in range(2):
                    weave[slot, pl.ds(r, width, stride=2), :] = now[r] * loss_ref[r, cut, :]
                start = pl.multiple_of((i * fields + q * width) * 2, 2 * width)
                out_ref[pl.ds(start, 2 * width), :] = weave[slot].astype(jnp.bfloat16)
            return carry

        lax.fori_loop(0, share // UNROLL, several, 0)

    def step(q, carry):
        @pl.when(q < chunks)
        def _():
            analyse_chunk(q)

        @pl.when((q >= 1) & (q - 1 < chunks))
        def _():
            swap(q - 1).wait_recv()
            pass_both(1 - me, q - 1)

        if relays:
            @pl.when((q >= RELAY) & (q - RELAY < chunks))
            def _():
                relay(me, q - RELAY)
                relay(1 - me, q - RELAY)

        @pl.when((q >= LAG) & (q - LAG < chunks))
        def _():
            for side in range(2):
                @pl.when(exists[1 - side])
                def _():
                    for r in range(2):
                        pass_on(side, r, q - LAG).wait_recv()

            advect_chunk(q - LAG)

        return carry

    lax.fori_loop(0, chunks + LAG, step, 0)

    def drain(q, carry):
        swap(q).wait_send()

        @pl.when(q < chunks - early)
        def _():
            follow(q).wait_send()

        for side in range(2):
            @pl.when(exists[side])
            def _():
                for r in range(2):
                    pass_on(side, r, q).wait_send()

            if relays:
                for r in range(2):
                    @pl.when(relayed(side, r, q))
                    def _():
                        hand_on(side, r, q).wait_send()

        return carry

    lax.fori_loop(0, chunks, drain, 0)


def finish(mine, other, theirs, dev, mix, keep, edge, loss, slots, rows):
    share, fields, _ = mine.shape
    width = WIDTH
    chunks = fields // width
    late = theirs.shape[1] // width
    vmem = pl.BlockSpec(memory_space=pltpu.VMEM)
    piece = (chunks, share, width, LANES)
    return pl.pallas_call(
        functools.partial(finish_kernel, slots, width),
        in_specs=[vmem] * 8,
        out_specs=vmem,
        out_shape=jax.ShapeDtypeStruct((share * fields * rows, LANES), jnp.bfloat16),
        scratch_shapes=[
            pltpu.VMEM((2,) + piece, jnp.bfloat16),
            pltpu.VMEM(piece, jnp.bfloat16),
            pltpu.VMEM((2,) + piece, jnp.bfloat16),
            pltpu.VMEM((2,) + piece, jnp.bfloat16),
            pltpu.VMEM((2,) + piece, jnp.bfloat16),
            pltpu.VMEM((late,) + piece[1:], jnp.bfloat16),
            pltpu.VMEM((2 * share, width, LANES), jnp.float32),
            pltpu.VMEM((slots, width, LANES), jnp.float32),
            pltpu.VMEM((width, LANES), jnp.float32),
            pltpu.VMEM((24, width, LANES), jnp.float32),
            pltpu.VMEM((UNROLL, 2 * width, LANES), jnp.float32),
            pltpu.SemaphoreType.DMA((chunks,)),
            pltpu.SemaphoreType.DMA((chunks,)),
            pltpu.SemaphoreType.DMA((2, 2, chunks)),
            pltpu.SemaphoreType.DMA((2, 2, chunks)),
            pltpu.SemaphoreType.DMA((2, chunks)),
            pltpu.SemaphoreType.DMA((2, chunks)),
            pltpu.SemaphoreType.DMA((late,)),
            pltpu.SemaphoreType.DMA((late,)),
        ],
        compiler_params=pltpu.CompilerParams(
            vmem_limit_bytes=40 * 1024 * 1024, collective_id=1, has_side_effects=True
        ),
        cost_estimate=pl.CostEstimate(flops=10**9, bytes_accessed=10**7, transcendentals=0),
        interpret=INTERPRET,
    )(mine, other, theirs, dev, mix, keep, edge, loss)


def analyse(states, dev, mix, keep, slots, first, count, width):
    share, _, cells = states[0].shape
    parts = len(states)
    members = share * parts
    wide = lambda height: pl.BlockSpec((height, LANES), lambda c, f: (0, c))
    return pl.pallas_call(
        functools.partial(analysis_kernel, parts, slots),
        grid=(cells // LANES, count // width),
        in_specs=[
            pl.BlockSpec((share, width, LANES), lambda c, f: (0, f + first // width, c))
        ] * parts + [wide(members * PITCH), wide(members * slots), wide(1)],
        out_specs=[pl.BlockSpec((share, width, LANES), lambda c, f: (0, f, c))] * parts,
        out_shape=[jax.ShapeDtypeStruct((share, count, cells), jnp.bfloat16)] * parts,
        scratch_shapes=[
            pltpu.VMEM((members, width, LANES), jnp.float32),
            pltpu.VMEM((slots, width, LANES), jnp.float32),
            pltpu.VMEM((width, LANES), jnp.float32),
        ],
        compiler_params=pltpu.CompilerParams(vmem_limit_bytes=32 * 1024 * 1024),
        cost_estimate=pl.CostEstimate(flops=10**9, bytes_accessed=50 * 10**6, transcendentals=0),
        interpret=INTERPRET,
    )(*states, dev, mix, keep)


def halo(cells, width):
    count = lax.axis_size("space")
    before = lax.ppermute(cells[-width:], "space", [(i, i + 1) for i in range(count - 1)])
    after = lax.ppermute(cells[:width], "space", [(i + 1, i) for i in range(count - 1)])
    return before, after


def wide_rows(cells, width):
    before, after = halo(cells, width)
    return jnp.concatenate([before, cells, after], axis=0)


def row_step(south, middle, north, courant):
    return (
        middle
        - 0.5 * courant * (north - south)
        + 0.5 * courant * courant * (north - 2.0 * middle + south)
    )


def col_step(middle, courant):
    padded = jnp.pad(middle, [(0, 0)] * (middle.ndim - 1) + [(1, 1)])
    east, west = padded[..., 2:], padded[..., :-2]
    return (
        middle
        - 0.5 * courant * (east - west)
        + 0.5 * courant * courant * (east - 2.0 * middle + west)
    )


def shards(
    ensemble, obs_value, obs_error, obs_cell, obs_species, patch_index, patch_count,
    courant_x, courant_y, dep_velocity, surface_factor,
):
    local_members, fields, tile_rows, columns = ensemble.shape
    species = dep_velocity.shape[0]
    levels = fields // species
    tile_cells = tile_rows * columns
    groups = lax.axis_size("mem")
    members = local_members * groups
    me = lax.axis_index("mem")
    slots = patch_index.shape[2]
    per_dev = tile_cells // groups
    paired = groups == 2 and tile_rows == 2 and columns == LANES
    paired = paired and GROUP % levels == 0 and fields % WIDTH == 0 and fields > 2 * LATE * WIDTH and species % GROUP == 0
    paired = paired and local_members % UNROLL == 0
    swap = [(0, 1), (1, 0)]

    if paired:
        mine, theirs, late, lowest = separate(
            ensemble.reshape(-1, columns), local_members, fields, tile_rows, levels
        )
        pool, edge = prepare(
            lowest,
            (obs_value, obs_error, obs_cell, obs_species),
            (courant_x.reshape(-1, columns), courant_y.reshape(-1, columns)),
            tile_rows, species,
        )
        theirs, pool = lax.optimization_barrier((theirs, pool))
    else:
        surface = ensemble.reshape(local_members, species, levels, tile_cells)[:, :, 0]
        position = obs_species[0] * tile_cells + obs_cell[0]
        equiv = jnp.take(surface.reshape(local_members, -1), position, axis=1).astype(jnp.float32)
        equiv = lax.all_gather(equiv, "mem", axis=0, tiled=True)
        zeros = jnp.zeros_like(obs_value[0])
        info = jnp.stack(
            [
                obs_value[0],
                obs_error[0],
                (obs_cell[0] // columns).astype(jnp.float32),
                (obs_cell[0] % columns).astype(jnp.float32),
            ]
            + [zeros] * 4
        )
        packed = jnp.concatenate([equiv, info], axis=0)
        before, after = halo(packed[None], 1)
        offset = jnp.zeros((packed.shape[0], 1), jnp.float32).at[members + 2, 0].set(float(tile_rows))
        pool = jnp.concatenate([before[0] - offset, packed, after[0] + offset], axis=1)

    if paired:
        states = (mine, lax.ppermute(theirs, "mem", swap))
    else:
        states = (
            lax.all_to_all(
                ensemble.reshape(local_members, fields, tile_cells),
                "mem", split_axis=2, concat_axis=0, tiled=True,
            ),
        )
    spare = -per_dev % LANES
    pad = lambda a: jnp.pad(a, [(0, 0)] * (a.ndim - 1) + [(0, spare)]) if spare else a
    states = tuple(pad(state) for state in states)
    cell = me * per_dev + jnp.arange(per_dev, dtype=jnp.int32)
    dev, mix, keep = solve_cells(
        pool,
        pad(jnp.transpose(patch_index[0])),
        pad(patch_count),
        pad((cell // columns).astype(jnp.float32)[None]),
        pad((cell % columns).astype(jnp.float32)[None]),
        members,
    )

    loss = jnp.exp(-dep_velocity[:, None, None] * surface_factor[None])
    if paired:
        lowest = (jnp.arange(levels, dtype=jnp.int32) == 0)[None, None, :, None]
        factor = jnp.where(lowest, jnp.moveaxis(loss, 1, 0)[:, :, None], 1.0).reshape(tile_rows, fields, columns)
        out = finish(*states, late, dev, mix, keep, edge, factor, slots, tile_rows)
        return out.reshape(ensemble.shape)

    width = next(w for w in (32, 16, fields) if fields % w == 0)
    wide_x = wide_rows(jnp.moveaxis(courant_x, 1, 0), SUBSTEPS)
    wide_y = wide_rows(jnp.moveaxis(courant_y, 1, 0), SUBSTEPS)
    out = analyse(states, dev, mix, keep, slots, 0, fields, width)
    back = lax.all_to_all(out[0][..., :per_dev], "mem", split_axis=0, concat_axis=2, tiled=True)
    rows = jnp.moveaxis(back.reshape(local_members, fields, tile_rows, columns), 2, 0)
    south, north = halo(rows, SUBSTEPS)
    shape = (local_members, species, levels, columns)
    now = [
        part[r].reshape(shape).astype(jnp.float32)
        for part in (south, rows, north)
        for r in range(part.shape[0])
    ]
    for repeat in range(SUBSTEPS):
        first = repeat + 1
        now = [
            col_step(
                row_step(now[r - 1], now[r], now[r + 1], wide_y[first + r - 1]),
                wide_x[first + r - 1],
            )
            for r in range(1, len(now) - 1)
        ]
    lowest = (jnp.arange(levels, dtype=jnp.int32) == 0)[:, None]
    now = [row * jnp.where(lowest, loss[:, r][:, None], 1.0) for r, row in enumerate(now)]
    joined = jnp.stack([row.astype(jnp.bfloat16) for row in now], axis=3)
    return joined.reshape(local_members, fields, tile_rows, columns)


def solution(mesh):
    in_specs = (
        P("mem", None, "space", None),
        P("space", None),
        P("space", None),
        P("space", None),
        P("space", None),
        P("space", "mem", None),
        P("space", "mem"),
        P(None, "space", None),
        P(None, "space", None),
        P(),
        P("space", None),
    )
    out_specs = P("mem", None, "space", None)
    return jax.shard_map(shards, mesh=mesh, in_specs=in_specs, out_specs=out_specs, check_vma=False)
```

```python
import functools
import math

import jax
import jax.numpy as jnp
from jax import lax
from jax.experimental import pallas as pl
from jax.experimental.pallas import tpu as pltpu
from jax.sharding import PartitionSpec as P

NEWTON = 8
SUBSTEPS = 2
LOC = 1
LANES = 128
GROUP = 8
PITCH = 40
WIDTH = 16
LAG = 8
RELAY = 3
LATE = 2
QUAD = 4
UNROLL = 8
INTERPRET = False


def lane_product(left, right, depth, rows, width, finish, unroll=4, group=GROUP):
    def several(block, carry):
        first = pl.multiple_of(block * group, group)

        def step(k, sums):
            row = right(k)
            return tuple(sums[r] + left(k, first, r) * row for r in range(group))

        zero = jnp.zeros((width, LANES), jnp.float32)
        sums = lax.fori_loop(0, depth, step, (zero,) * group, unroll=unroll)
        finish(first, sums)
        return carry

    lax.fori_loop(0, rows // group, several, 0)


def weights_kernel(
    members, repeats, radius,
    pool_ref, idx_ref, cnt_ref, row_ref, col_ref,
    dev_ref, mix_ref, keep_ref,
    first_v, one_v, two_v, step_g, keys, innov, scal,
):
    slots = idx_ref.shape[0]
    pooled = pool_ref.shape[1]
    blocks = slots // GROUP
    info = pool_ref[members:, :]
    high = info.astype(jnp.bfloat16).astype(jnp.float32)
    rest = info - high
    middle = rest.astype(jnp.bfloat16).astype(jnp.float32)
    low = rest - middle
    table = jnp.concatenate([pool_ref[:members, :], high, middle, low, jnp.zeros_like(low)], axis=0)
    table = table.astype(jnp.bfloat16)
    place = lax.broadcasted_iota(jnp.int32, (pooled, LANES), 0)
    extra = info.shape[0]

    def pick(k, total):
        hot = jnp.where(place == idx_ref[pl.ds(k, 1), :], 1.0, 0.0).astype(jnp.bfloat16)
        got = jnp.dot(table, hot, preferred_element_type=jnp.float32)
        equiv = got[:members]
        facts = (
            got[members : members + extra]
            + got[members + extra : members + 2 * extra]
            + got[members + 2 * extra : members + 3 * extra]
        )
        mean = jnp.sum(equiv, axis=0, keepdims=True) * (1.0 / members)
        dist = (facts[2:3] - row_ref[...]) ** 2 + (facts[3:4] - col_ref[...]) ** 2
        rho = jnp.exp(-dist / (2.0 * radius * radius)) / facts[1:2]
        scale = jnp.sqrt(jnp.where(k < cnt_ref[...], rho, 0.0))
        scaled = (equiv - mean) * scale
        dev_ref[pl.ds(k, members, stride=PITCH), :] = scaled
        innov[pl.ds(k, 1), :] = (facts[0:1] - mean) * scale
        return total + jnp.sum(scaled * scaled, axis=0, keepdims=True)

    spread = lax.fori_loop(0, slots, pick, jnp.zeros((1, LANES), jnp.float32), unroll=8)
    shift = members - 1.0
    inverse = 1.0 / (spread + shift * members)
    level = lax.broadcasted_iota(jnp.int32, (GROUP, LANES), 0)

    def eye(r, value):
        return jnp.where(level == r, value, 0.0)

    def at(ref, i, j, base=0):
        start = i * PITCH + j * GROUP
        start = start if isinstance(start, int) else pl.multiple_of(start, GROUP)
        return ref[pl.ds(base + start, GROUP), :]

    def put(ref, i, parts, base=0):
        for j, part in enumerate(parts):
            ref[pl.ds(base + i * PITCH + j * GROUP, GROUP), :] = part
            if j < i // GROUP:
                ref[pl.ds(base + j * GROUP * PITCH + i, GROUP, stride=PITCH), :] = part

    def product(left, right, depth, finish, unroll=16):
        for pair in range((blocks + 1) // 2):
            groups = sorted({pair, blocks - 1 - pair})

            def step(k, sums):
                wide = [right(k, j) for j in range(groups[-1] + 1)]
                out, spot = [], 0
                for g in groups:
                    for r in range(GROUP):
                        one = left(k, g * GROUP + r)
                        for j in range(g + 1):
                            out.append(sums[spot] + one * wide[j])
                            spot += 1
                return tuple(out)

            zero = jnp.zeros((GROUP, LANES), jnp.float32)
            count = sum((g + 1) * GROUP for g in groups)
            sums = lax.fori_loop(0, depth, step, (zero,) * count, unroll=unroll)
            spot = 0
            for g in groups:
                for r in range(GROUP):
                    finish(g * GROUP + r, sums[spot : spot + g + 1])
                    spot += g + 1

    def square(left, right, finish, base=0):
        product(
            lambda k, i: left[pl.ds(base + k * PITCH + i, 1), :],
            lambda k, j: at(right, k, j),
            slots, finish,
        )

    def gram_done(i, sums):
        put(first_v, i, [part * inverse for part in sums])

    product(
        lambda k, i: dev_ref[pl.ds(k * PITCH + i, 1), :],
        lambda k, j: at(dev_ref, k, j),
        members, gram_done,
    )

    xi = shift * inverse
    mus = []
    for k in range(repeats):
        mu = 1.5 - 0.5 * xi
        scal[pl.ds(k, 1), :] = xi
        scal[pl.ds(repeats + k, 1), :] = mu
        mus.append(mu)
        xi = xi * mu * mu
    after = mus[-1]
    for k in reversed(range(repeats - 1)):
        scal[pl.ds(2 * repeats + k, 1), :] = after
        after = after * mus[k]
    last_z = after
    area = slots * PITCH

    def forward(n, old, new):
        xi = scal[pl.ds(n, 1), :]
        mu = scal[pl.ds(repeats + n, 1), :]
        flat, slope = mu * mu - xi * mu, 0.25 * xi - mu
        base = pl.multiple_of(n * area, GROUP)

        def to_g(i, sums):
            parts = [0.25 * part + slope * at(old, i, j) for j, part in enumerate(sums)]
            parts[-1] = parts[-1] + eye(i % GROUP, flat)
            put(step_g, i, parts)

        square(old, old, to_g)

        def to_v(i, sums):
            put(new, i, sums)
            put(keys, i, [mu * at(step_g, i, j) - 0.5 * part for j, part in enumerate(sums)], base)

        square(step_g, old, to_v)

    def forward_pair(n, carry):
        forward(2 * n + 1, one_v, two_v)
        forward(2 * n + 2, two_v, one_v)
        return carry

    forward(0, first_v, one_v)
    lax.fori_loop(0, repeats // 2 - 1, forward_pair, 0)

    after = scal[pl.ds(3 * repeats - 2, 1), :]
    for i in range(slots):
        parts = [-0.5 * at(keys, i, j, (repeats - 2) * area) for j in range(blocks)]
        parts[i // GROUP] = parts[i // GROUP] - eye(i % GROUP, 0.5 * after)
        for j, part in enumerate(parts):
            one_v[pl.ds(i * PITCH + j * GROUP, GROUP), :] = part

    def backward(n, old, new):
        base = pl.multiple_of(n * area, GROUP)
        half = 0.5 * scal[pl.ds(2 * repeats + n, 1), :]

        def to_h(i, sums):
            parts = list(sums)
            parts[-1] = parts[-1] - eye(i % GROUP, half)
            put(new, i, parts)

        square(keys, old, to_h, base)

    def backward_pair(m, carry):
        backward(repeats - 3 - 2 * m, one_v, two_v)
        backward(repeats - 4 - 2 * m, two_v, one_v)
        return carry

    lax.fori_loop(0, repeats // 2 - 1, backward_pair, 0)

    def whole(ref, k):
        return ref[pl.ds(pl.multiple_of(k * PITCH, GROUP), slots), :]

    none = jnp.zeros((slots, LANES), jnp.float32)

    def apply(ref):
        def step(k, total):
            return total + innov[pl.ds(k, 1), :] * whole(ref, k)

        return lax.fori_loop(0, slots, step, none)

    for _ in range(2):
        start = innov[...]
        innov[...] = apply(one_v)
        innov[...] = last_z * start + apply(first_v)
    gain = innov[...] * inverse
    factor = math.sqrt(shift) * jnp.sqrt(inverse)
    keep_ref[...] = factor * last_z
    both = factor * inverse

    def to_mix(first, sums):
        for r in range(GROUP):
            mix_ref[pl.ds(pl.multiple_of((first + r) * slots, slots), slots), :] = both * sums[r] + gain

    lane_product(
        lambda k, first, r: dev_ref[pl.ds((first + r) * PITCH + k, 1), :],
        lambda k: whole(one_v, k), slots, members, slots, to_mix, unroll=16,
    )


def solve_cells(pool, idx, counts, rows, cols, members):
    slots, cells = idx.shape
    lane = lambda height: pl.BlockSpec((height, LANES), lambda c: (0, c))
    square = pltpu.VMEM((slots * PITCH, LANES), jnp.float32)
    return pl.pallas_call(
        functools.partial(weights_kernel, members, NEWTON, LOC),
        grid=(cells // LANES,),
        in_specs=[pl.BlockSpec(pool.shape, lambda c: (0, 0)), lane(slots), lane(1), lane(1), lane(1)],
        out_specs=[lane(members * PITCH), lane(members * slots), lane(1)],
        out_shape=[
            jax.ShapeDtypeStruct((members * PITCH, cells), jnp.float32),
            jax.ShapeDtypeStruct((members * slots, cells), jnp.float32),
            jax.ShapeDtypeStruct((1, cells), jnp.float32),
        ],
        scratch_shapes=[
            square,
            square,
            square,
            square,
            pltpu.VMEM(((NEWTON - 1) * slots * PITCH, LANES), jnp.float32),
            pltpu.VMEM((slots, LANES), jnp.float32),
            pltpu.VMEM((3 * NEWTON, LANES), jnp.float32),
        ],
        compiler_params=pltpu.CompilerParams(vmem_limit_bytes=40 * 1024 * 1024),
        cost_estimate=pl.CostEstimate(flops=2 * 10**9, bytes_accessed=200 * 10**6, transcendentals=0),
        interpret=INTERPRET,
    )(pool, idx, counts, rows, cols)


def split_kernel(rows, levels, flat_ref, mine_ref, early_ref, late_ref, lowest_ref, spread):
    me = lax.axis_index("mem")
    batch, fields, _ = mine_ref.shape
    species = fields // levels
    span = fields * rows
    for slot in range(batch):
        spread[slot] = flat_ref[pl.ds(slot * span, span), :].astype(jnp.float32)
        mine_ref[slot] = spread[slot, pl.ds(me, fields, stride=rows), :].astype(jnp.bfloat16)
        theirs = spread[slot, pl.ds(1 - me, fields, stride=rows), :].astype(jnp.bfloat16)
        early_ref[slot] = theirs[: early_ref.shape[1]]
        late_ref[slot] = theirs[early_ref.shape[1] :]
        lowest_ref[slot] = jnp.concatenate(
            [spread[slot, pl.ds(r, species, stride=rows * levels), :] for r in range(rows)], axis=0
        ).astype(jnp.bfloat16)


def separate(flat, share, fields, rows, levels):
    span = fields * rows
    block = lambda height: pl.BlockSpec((UNROLL, height, LANES), lambda n: (n, 0, 0))
    out = lambda height: jax.ShapeDtypeStruct((share, height, LANES), jnp.bfloat16)
    late = LATE * WIDTH
    heights = (fields, fields - late, late, rows * fields // levels)
    return pl.pallas_call(
        functools.partial(split_kernel, rows, levels),
        grid=(share // UNROLL,),
        in_specs=[pl.BlockSpec((UNROLL * span, LANES), lambda n: (n, 0))],
        out_specs=[block(height) for height in heights],
        out_shape=[out(height) for height in heights],
        scratch_shapes=[pltpu.VMEM((UNROLL, span, LANES), jnp.float32)],
        compiler_params=pltpu.CompilerParams(vmem_limit_bytes=16 * 1024 * 1024),
        cost_estimate=pl.CostEstimate(flops=10**7, bytes_accessed=6 * 10**6, transcendentals=0),
        interpret=INTERPRET,
    )(flat)


def prep_kernel(
    rows, species,
    lowest_ref, value_ref, error_ref, cell_ref, species_ref, courant_x_ref, courant_y_ref,
    pool_ref, edge_ref, found, block, facts_ref, land, land_facts, send_sems, recv_sems, facts_sent, facts_come,
):
    share = lowest_ref.shape[0]
    observed = value_ref.shape[1]
    levels = courant_x_ref.shape[0] // rows
    me, place, count = lax.axis_index("mem"), lax.axis_index("space"), lax.axis_size("space")

    def exists(step):
        return (place + step >= 0) & (place + step < count)

    def guard(step, act):
        if step == 0:
            act()
        else:
            pl.when(exists(step))(act)

    ways = [(1, 0), (0, -1), (0, 1), (1, -1), (1, 1)]
    barrier = pltpu.get_barrier_semaphore()

    def target(flip, step):
        return (1 - me if flip else me, place + step)

    for flip, step in ways:
        def greet(flip=flip, step=step):
            pl.semaphore_signal(barrier, inc=1, device_id=target(flip, step), device_id_type=pl.DeviceIdType.MESH)

        guard(step, greet)

    cell = cell_ref[...]
    row, column = lax.shift_right_logical(cell, LANES.bit_length() - 1), cell & (LANES - 1)
    facts_ref[pl.ds(0, GROUP), :] = jnp.zeros((GROUP, observed), jnp.float32)
    facts = (value_ref[...], error_ref[...], row.astype(jnp.float32), column.astype(jnp.float32))
    for n, fact in enumerate(facts):
        facts_ref[pl.ds(n, 1), :] = fact
    for n, courant in enumerate((courant_x_ref, courant_y_ref)):
        for copy in range(GROUP // levels):
            for r in range(rows):
                start = (n + 1) * GROUP + copy * levels
                facts_ref[pl.ds(start, levels), pl.ds(r * LANES, LANES)] = courant[pl.ds(r, levels, stride=rows), :]
    hot = jnp.where(lax.broadcasted_iota(jnp.int32, (LANES, observed), 0) == column, 1.0, 0.0).astype(jnp.bfloat16)
    wanted = lax.broadcasted_iota(jnp.int32, (rows * species, observed), 0) == row * species + species_ref[...]

    def look(n, carry):
        for slot in range(UNROLL):
            i = UNROLL * n + slot
            got = jnp.dot(lowest_ref[i], hot, preferred_element_type=jnp.float32)
            found[pl.ds(i, 1), :] = jnp.sum(jnp.where(wanted, got, 0.0), axis=0, keepdims=True)
        return carry

    lax.fori_loop(0, share // UNROLL, look, 0)
    block[...] = found[...].astype(jnp.bfloat16)

    greeted = 1 + 2 * exists(-1).astype(jnp.int32) + 2 * exists(1).astype(jnp.int32)
    pl.semaphore_wait(barrier, greeted)

    def copy(n):
        flip, step = ways[n]
        return pltpu.make_async_remote_copy(
            src_ref=block, dst_ref=land.at[1 - step, flip],
            send_sem=send_sems.at[n], recv_sem=recv_sems.at[1 - step, flip],
            device_id=target(flip, step), device_id_type=pl.DeviceIdType.MESH,
        )

    def copy_facts(step):
        return pltpu.make_async_remote_copy(
            src_ref=facts_ref, dst_ref=land_facts.at[1 - step],
            send_sem=facts_sent.at[1 - step], recv_sem=facts_come.at[1 - step],
            device_id=(me, place + step), device_id_type=pl.DeviceIdType.MESH,
        )

    for n, (flip, step) in enumerate(ways):
        guard(step, lambda n=n: copy(n).start())
    for step in (-1, 1):
        guard(step, lambda step=step: copy_facts(step).start())
    for step in (-1, 1):
        def blank(step=step):
            land[1 + step] = jnp.zeros_like(land[1 + step])
            land_facts[1 + step] = jnp.zeros_like(land_facts[1 + step])

        pl.when(jnp.logical_not(exists(step)))(blank)
    for n, (flip, step) in enumerate(ways):
        def landed(n=n):
            copy(n).wait_recv()

        guard(-step, landed)
    for step in (-1, 1):
        guard(-step, lambda step=step: copy_facts(step).wait_recv())
    line = lax.broadcasted_iota(jnp.int32, (GROUP, observed), 0)
    for part in range(3):
        lanes = pl.ds(part * observed, observed)
        own = found[...] if part == 1 else land[part, 0].astype(jnp.float32)
        facts = (facts_ref if part == 1 else land_facts.at[part])[...]
        pool_ref[pl.ds(0, share), lanes] = own
        pool_ref[pl.ds(share, share), lanes] = land[part, 1].astype(jnp.float32)
        pool_ref[pl.ds(2 * share, GROUP), lanes] = facts[:GROUP] + jnp.where(
            line == 2, float(rows * (part - 1)), 0.0
        )
        edge_ref[part] = facts[GROUP:]
    for n, (flip, step) in enumerate(ways):
        def sent(n=n):
            copy(n).wait_send()

        guard(step, sent)
    for step in (-1, 1):
        guard(step, lambda step=step: copy_facts(step).wait_send())


def prepare(lowest, facts, courants, rows, species):
    share = lowest.shape[0]
    observed = facts[0].shape[1]
    vmem = pl.BlockSpec(memory_space=pltpu.VMEM)
    return pl.pallas_call(
        functools.partial(prep_kernel, rows, species),
        in_specs=[vmem] * 7,
        out_specs=[vmem] * 2,
        out_shape=[
            jax.ShapeDtypeStruct((2 * share + GROUP, 3 * observed), jnp.float32),
            jax.ShapeDtypeStruct((3, 2 * GROUP, observed), jnp.float32),
        ],
        scratch_shapes=[
            pltpu.VMEM((share, observed), jnp.float32),
            pltpu.VMEM((share, observed), jnp.bfloat16),
            pltpu.VMEM((3 * GROUP, observed), jnp.float32),
            pltpu.VMEM((3, 2, share, observed), jnp.bfloat16),
            pltpu.VMEM((3, 3 * GROUP, observed), jnp.float32),
            pltpu.SemaphoreType.DMA((5,)),
            pltpu.SemaphoreType.DMA((3, 2)),
            pltpu.SemaphoreType.DMA((3,)),
            pltpu.SemaphoreType.DMA((3,)),
        ],
        compiler_params=pltpu.CompilerParams(
            vmem_limit_bytes=16 * 1024 * 1024, collective_id=0, has_side_effects=True
        ),
        cost_estimate=pl.CostEstimate(flops=10**8, bytes_accessed=10**6, transcendentals=0),
        interpret=INTERPRET,
    )(lowest, *facts, *courants)


def analysis_kernel(parts, slots, *refs):
    states = refs[:parts]
    dev_ref, mix_ref, keep_ref = refs[parts : parts + 3]
    outs = refs[parts + 3 : 2 * parts + 3]
    anomaly, mapped, mean_ref = refs[2 * parts + 3 :]
    share, width, _ = states[0].shape
    members = share * parts
    total = jnp.zeros((width, LANES), jnp.float32)
    for state in states:
        total = lax.fori_loop(
            0, share, lambda i, t, s=state: t + s[i].astype(jnp.float32), total, unroll=4
        )
    mean = total * (1.0 / members)
    mean_ref[...] = mean
    for part, state in enumerate(states):

        def subtract(i, carry, s=state, base=part * share):
            anomaly[base + i] = s[i].astype(jnp.float32) - mean_ref[...]
            return carry

        lax.fori_loop(0, share, subtract, 0, unroll=4)

    def to_mapped(first, sums):
        for r in range(GROUP):
            mapped[first + r] = sums[r]

    lane_product(
        lambda i, first, r: dev_ref[pl.ds(i * PITCH + first + r, 1), :],
        lambda i: anomaly[i], members, slots, width, to_mapped,
    )
    for part, out in enumerate(outs):
        base = part * share

        def to_out(first, sums, out=out, base=base):
            for r in range(GROUP):
                held = mean_ref[...] + keep_ref[...] * anomaly[base + first + r]
                out[first + r] = (held + sums[r]).astype(jnp.bfloat16)

        lane_product(
            lambda k, first, r, base=base: mix_ref[pl.ds((base + first + r) * slots + k, 1), :],
            lambda k: mapped[k], slots, share, width, to_out,
        )


def finish_kernel(
    slots, width,
    mine_ref, other_ref, theirs_ref, dev_ref, mix_ref, keep_ref, edge_ref, loss_ref, out_ref,
    rows, away, south, north, held_ref, late_ref, values, mapped, mean_ref, coef, weave,
    away_sent, away_come, edge_sent, edge_come, held_sent, held_come, late_sent, late_come,
):
    share, fields, _ = mine_ref.shape
    members = 2 * share
    chunks = fields // width
    early = other_ref.shape[1] // width
    group = 2 * LANES // width
    me, place, count = lax.axis_index("mem"), lax.axis_index("space"), lax.axis_size("space")
    mesh_id = pl.DeviceIdType.MESH
    exists = (place > 0, place + 1 < count)
    sides = ((1 - me, place), (me, place - 1), (me, place + 1))
    relays = count % QUAD == 0 and count > QUAD
    floors, floor, corner = count // QUAD, place // QUAD, place % QUAD
    near, far = corner == 0, corner == QUAD - 1
    across = (me, jnp.where(far, place - (QUAD - 1), place + (QUAD - 1)))
    ahead = (me, jnp.where(far, place - QUAD, place + QUAD))
    behind = (me, jnp.where(far, place + QUAD, place - QUAD))
    goes = jnp.where(far, floor > 0, floor < floors - 1)
    comes = jnp.where(far, floor < floors - 1, floor > 0)
    barrier = pltpu.get_barrier_semaphore()
    pl.semaphore_signal(barrier, inc=1, device_id=sides[0], device_id_type=mesh_id)
    for side in range(2):
        @pl.when(exists[side])
        def _():
            pl.semaphore_signal(barrier, inc=1, device_id=sides[1 + side], device_id_type=mesh_id)

    if relays:
        for there, device in ((True, across), (goes, ahead), (comes, behind)):
            @pl.when((near | far) & there)
            def _():
                pl.semaphore_signal(barrier, inc=1, device_id=device, device_id_type=mesh_id)

    for side, buffer in enumerate((south, north)):
        @pl.when(jnp.logical_not(exists[side]))
        def _():
            def clear(n, carry):
                for r in range(2):
                    buffer[r, n // share, n % share] = jnp.zeros((width, LANES), jnp.bfloat16)
                return carry

            lax.fori_loop(0, chunks * share, clear, 0)

    lane = lax.broadcasted_iota(jnp.int32, (GROUP, LANES), 1)
    for at, (part, r) in enumerate(((0, 1), (1, 0), (1, 1), (2, 0))):
        cut = pl.ds(r * LANES, LANES)
        cx = edge_ref[part, pl.ds(0, GROUP), cut]
        cy = edge_ref[part, pl.ds(GROUP, GROUP), cut]
        six = (
            1.0 - cy * cy,
            0.5 * cy * cy - 0.5 * cy,
            0.5 * cy * cy + 0.5 * cy,
            1.0 - cx * cx,
            jnp.where(lane == LANES - 1, 0.0, 0.5 * cx * cx - 0.5 * cx),
            jnp.where(lane == 0, 0.0, 0.5 * cx * cx + 0.5 * cx),
        )
        for n, value in enumerate(six):
            for piece in range(width // GROUP):
                coef[6 * at + n, pl.ds(piece * GROUP, GROUP), :] = value

    greeted = 1 + exists[0].astype(jnp.int32) + exists[1].astype(jnp.int32)
    if relays:
        more = 1 + goes.astype(jnp.int32) + comes.astype(jnp.int32)
        greeted = greeted + jnp.where(near | far, more, 0)
    pl.semaphore_wait(barrier, greeted)

    def share_of(r, q, part):
        return (2 * r + q % 2) * floors < 4 * part

    def detours(side, r, q):
        if side:
            return far & share_of(r, q, floors - 1 - floor)
        return near & share_of(r, q, floor)

    def hand_over(side, r, q):
        return pltpu.make_async_remote_copy(
            src_ref=rows.at[r, q], dst_ref=held_ref.at[r, q],
            send_sem=edge_sent.at[side, r, q], recv_sem=held_come.at[r, q],
            device_id=across, device_id_type=mesh_id,
        )

    def hand_on(side, r, q):
        return pltpu.make_async_remote_copy(
            src_ref=held_ref.at[r, q], dst_ref=(north, south)[side].at[r, q],
            send_sem=held_sent.at[r, q], recv_sem=edge_come.at[side, r, q],
            device_id=ahead, device_id_type=mesh_id,
        )

    def relayed(side, r, q):
        if side:
            return near & share_of(r, q, floors - 1 - floor)
        return far & share_of(r, q, floor)

    def relay(r, q):
        for side in range(2):
            @pl.when(relayed(side, r, q))
            def _():
                hand_over(side, r, q).wait_recv()
                hand_on(side, r, q).start()

    def swap(q):
        return pltpu.make_async_remote_copy(
            src_ref=away.at[q], dst_ref=rows.at[me, q],
            send_sem=away_sent.at[q], recv_sem=away_come.at[q],
            device_id=sides[0], device_id_type=mesh_id,
        )

    def pass_on(side, r, q):
        return pltpu.make_async_remote_copy(
            src_ref=rows.at[r, q], dst_ref=(north, south)[side].at[r, q],
            send_sem=edge_sent.at[side, r, q], recv_sem=edge_come.at[side, r, q],
            device_id=sides[1 + side], device_id_type=mesh_id,
        )

    def pass_both(r, q):
        for side in range(2):
            if not relays:
                pl.when(exists[side])(pass_on(side, r, q).start)
                continue
            turn = detours(side, r, q)

            @pl.when(turn)
            def _():
                hand_over(side, r, q).start()

            @pl.when(exists[side] & jnp.logical_not(turn))
            def _():
                pass_on(side, r, q).start()

    def follow(n):
        return pltpu.make_async_remote_copy(
            src_ref=theirs_ref.at[:, pl.ds(pl.multiple_of(n * width, width), width), :], dst_ref=late_ref.at[n],
            send_sem=late_sent.at[n], recv_sem=late_come.at[n],
            device_id=sides[0], device_id_type=mesh_id,
        )

    def analyse_chunk(q):
        cut = pl.ds(pl.multiple_of(q * width, width), width)
        zero = jnp.zeros((width, LANES), jnp.float32)

        def fill(load, base):
            def one(i, total):
                value = load(i).astype(jnp.float32)
                values[base + i] = value
                return total + value

            return lax.fori_loop(0, share, one, zero, unroll=8)

        mean_ref[...] = fill(lambda i: mine_ref[i, cut, :], 0)

        @pl.when(q < early)
        def _():
            mean_ref[...] += fill(lambda i: other_ref[i, cut, :], share)

        @pl.when(q >= early)
        def _():
            follow(q - early).wait_recv()
            mean_ref[...] += fill(lambda i: late_ref[q - early, i], share)

        mean_ref[...] = (1.0 - keep_ref[...]) * (mean_ref[...] * (1.0 / members))

        def to_mapped(first, sums):
            for r in range(group):
                mapped[first + r] = sums[r]

        lane_product(
            lambda i, first, r: dev_ref[pl.ds(i * PITCH + first + r, 1), :],
            lambda i: values[i], members, slots, width, to_mapped, group=group,
        )
        for part in (0, 1):
            base = part * share

            def to_out(first, sums, base=base, part=part):
                for r in range(group):
                    held = mean_ref[...] + keep_ref[...] * values[base + first + r]
                    value = (held + sums[r]).astype(jnp.bfloat16)
                    if part:
                        away[q, first + r] = value
                    else:
                        rows[me, q, first + r] = value

            lane_product(
                lambda k, first, r, base=base: mix_ref[pl.ds((base + first + r) * slots + k, 1), :],
                lambda k: mapped[k], slots, share, width, to_out, group=group,
            )
            if part:
                swap(q).start()

                @pl.when(q < chunks - early)
                def _():
                    follow(q).start()
            else:
                pass_both(me, q)

    def advect_chunk(q):
        cut = pl.ds(pl.multiple_of(q * width, width), width)

        def along(at, low, middle, high):
            now = coef[6 * at] * middle + coef[6 * at + 1] * high + coef[6 * at + 2] * low
            thin = now.astype(jnp.bfloat16)
            east = pltpu.roll(thin, LANES - 1, 1).astype(jnp.float32)
            west = pltpu.roll(thin, 1, 1).astype(jnp.float32)
            return coef[6 * at + 3] * now + coef[6 * at + 4] * east + coef[6 * at + 5] * west

        def several(n, carry):
            for slot in range(UNROLL):
                i = UNROLL * n + slot
                now = [
                    part[r, q, i].astype(jnp.float32) for part in (south, rows, north) for r in range(2)
                ]
                now = [along(at, *now[at : at + 3]) for at in range(4)]
                now = [along(1 + at, *now[at : at + 3]) for at in range(2)]
                for r in range(2):
                    weave[slot, pl.ds(r, width, stride=2), :] = now[r] * loss_ref[r, cut, :]
                start = pl.multiple_of((i * fields + q * width) * 2, 2 * width)
                out_ref[pl.ds(start, 2 * width), :] = weave[slot].astype(jnp.bfloat16)
            return carry

        lax.fori_loop(0, share // UNROLL, several, 0)

    def step(q, carry):
        @pl.when(q < chunks)
        def _():
            analyse_chunk(q)

        @pl.when((q >= 1) & (q - 1 < chunks))
        def _():
            swap(q - 1).wait_recv()
            pass_both(1 - me, q - 1)

        if relays:
            @pl.when((q >= RELAY) & (q - RELAY < chunks))
            def _():
                relay(me, q - RELAY)
                relay(1 - me, q - RELAY)

        @pl.when((q >= LAG) & (q - LAG < chunks))
        def _():
            for side in range(2):
                @pl.when(exists[1 - side])
                def _():
                    for r in range(2):
                        pass_on(side, r, q - LAG).wait_recv()

            advect_chunk(q - LAG)

        return carry

    lax.fori_loop(0, chunks + LAG, step, 0)

    def drain(q, carry):
        swap(q).wait_send()

        @pl.when(q < chunks - early)
        def _():
            follow(q).wait_send()

        for side in range(2):
            @pl.when(exists[side])
            def _():
                for r in range(2):
                    pass_on(side, r, q).wait_send()

            if relays:
                for r in range(2):
                    @pl.when(relayed(side, r, q))
                    def _():
                        hand_on(side, r, q).wait_send()

        return carry

    lax.fori_loop(0, chunks, drain, 0)


def finish(mine, other, theirs, dev, mix, keep, edge, loss, slots, rows):
    share, fields, _ = mine.shape
    width = WIDTH
    chunks = fields // width
    late = theirs.shape[1] // width
    vmem = pl.BlockSpec(memory_space=pltpu.VMEM)
    piece = (chunks, share, width, LANES)
    return pl.pallas_call(
        functools.partial(finish_kernel, slots, width),
        in_specs=[vmem] * 8,
        out_specs=vmem,
        out_shape=jax.ShapeDtypeStruct((share * fields * rows, LANES), jnp.bfloat16),
        scratch_shapes=[
            pltpu.VMEM((2,) + piece, jnp.bfloat16),
            pltpu.VMEM(piece, jnp.bfloat16),
            pltpu.VMEM((2,) + piece, jnp.bfloat16),
            pltpu.VMEM((2,) + piece, jnp.bfloat16),
            pltpu.VMEM((2,) + piece, jnp.bfloat16),
            pltpu.VMEM((late,) + piece[1:], jnp.bfloat16),
            pltpu.VMEM((2 * share, width, LANES), jnp.float32),
            pltpu.VMEM((slots, width, LANES), jnp.float32),
            pltpu.VMEM((width, LANES), jnp.float32),
            pltpu.VMEM((24, width, LANES), jnp.float32),
            pltpu.VMEM((UNROLL, 2 * width, LANES), jnp.float32),
            pltpu.SemaphoreType.DMA((chunks,)),
            pltpu.SemaphoreType.DMA((chunks,)),
            pltpu.SemaphoreType.DMA((2, 2, chunks)),
            pltpu.SemaphoreType.DMA((2, 2, chunks)),
            pltpu.SemaphoreType.DMA((2, chunks)),
            pltpu.SemaphoreType.DMA((2, chunks)),
            pltpu.SemaphoreType.DMA((late,)),
            pltpu.SemaphoreType.DMA((late,)),
        ],
        compiler_params=pltpu.CompilerParams(
            vmem_limit_bytes=40 * 1024 * 1024, collective_id=1, has_side_effects=True
        ),
        cost_estimate=pl.CostEstimate(flops=10**9, bytes_accessed=10**7, transcendentals=0),
        interpret=INTERPRET,
    )(mine, other, theirs, dev, mix, keep, edge, loss)


def analyse(states, dev, mix, keep, slots, first, count, width):
    share, _, cells = states[0].shape
    parts = len(states)
    members = share * parts
    wide = lambda height: pl.BlockSpec((height, LANES), lambda c, f: (0, c))
    return pl.pallas_call(
        functools.partial(analysis_kernel, parts, slots),
        grid=(cells // LANES, count // width),
        in_specs=[
            pl.BlockSpec((share, width, LANES), lambda c, f: (0, f + first // width, c))
        ] * parts + [wide(members * PITCH), wide(members * slots), wide(1)],
        out_specs=[pl.BlockSpec((share, width, LANES), lambda c, f: (0, f, c))] * parts,
        out_shape=[jax.ShapeDtypeStruct((share, count, cells), jnp.bfloat16)] * parts,
        scratch_shapes=[
            pltpu.VMEM((members, width, LANES), jnp.float32),
            pltpu.VMEM((slots, width, LANES), jnp.float32),
            pltpu.VMEM((width, LANES), jnp.float32),
        ],
        compiler_params=pltpu.CompilerParams(vmem_limit_bytes=32 * 1024 * 1024),
        cost_estimate=pl.CostEstimate(flops=10**9, bytes_accessed=50 * 10**6, transcendentals=0),
        interpret=INTERPRET,
    )(*states, dev, mix, keep)


def halo(cells, width):
    count = lax.axis_size("space")
    before = lax.ppermute(cells[-width:], "space", [(i, i + 1) for i in range(count - 1)])
    after = lax.ppermute(cells[:width], "space", [(i + 1, i) for i in range(count - 1)])
    return before, after


def wide_rows(cells, width):
    before, after = halo(cells, width)
    return jnp.concatenate([before, cells, after], axis=0)


def row_step(south, middle, north, courant):
    return (
        middle
        - 0.5 * courant * (north - south)
        + 0.5 * courant * courant * (north - 2.0 * middle + south)
    )


def col_step(middle, courant):
    padded = jnp.pad(middle, [(0, 0)] * (middle.ndim - 1) + [(1, 1)])
    east, west = padded[..., 2:], padded[..., :-2]
    return (
        middle
        - 0.5 * courant * (east - west)
        + 0.5 * courant * courant * (east - 2.0 * middle + west)
    )


def shards(
    ensemble, obs_value, obs_error, obs_cell, obs_species, patch_index, patch_count,
    courant_x, courant_y, dep_velocity, surface_factor,
):
    local_members, fields, tile_rows, columns = ensemble.shape
    species = dep_velocity.shape[0]
    levels = fields // species
    tile_cells = tile_rows * columns
    groups = lax.axis_size("mem")
    members = local_members * groups
    me = lax.axis_index("mem")
    slots = patch_index.shape[2]
    per_dev = tile_cells // groups
    paired = groups == 2 and tile_rows == 2 and columns == LANES
    paired = paired and GROUP % levels == 0 and fields % WIDTH == 0 and fields > 2 * LATE * WIDTH and species % GROUP == 0
    paired = paired and local_members % UNROLL == 0
    swap = [(0, 1), (1, 0)]

    if paired:
        mine, theirs, late, lowest = separate(
            ensemble.reshape(-1, columns), local_members, fields, tile_rows, levels
        )
        pool, edge = prepare(
            lowest,
            (obs_value, obs_error, obs_cell, obs_species),
            (courant_x.reshape(-1, columns), courant_y.reshape(-1, columns)),
            tile_rows, species,
        )
        theirs, pool = lax.optimization_barrier((theirs, pool))
    else:
        surface = ensemble.reshape(local_members, species, levels, tile_cells)[:, :, 0]
        position = obs_species[0] * tile_cells + obs_cell[0]
        equiv = jnp.take(surface.reshape(local_members, -1), position, axis=1).astype(jnp.float32)
        equiv = lax.all_gather(equiv, "mem", axis=0, tiled=True)
        zeros = jnp.zeros_like(obs_value[0])
        info = jnp.stack(
            [
                obs_value[0],
                obs_error[0],
                (obs_cell[0] // columns).astype(jnp.float32),
                (obs_cell[0] % columns).astype(jnp.float32),
            ]
            + [zeros] * 4
        )
        packed = jnp.concatenate([equiv, info], axis=0)
        before, after = halo(packed[None], 1)
        offset = jnp.zeros((packed.shape[0], 1), jnp.float32).at[members + 2, 0].set(float(tile_rows))
        pool = jnp.concatenate([before[0] - offset, packed, after[0] + offset], axis=1)

    if paired:
        states = (mine, lax.ppermute(theirs, "mem", swap))
    else:
        states = (
            lax.all_to_all(
                ensemble.reshape(local_members, fields, tile_cells),
                "mem", split_axis=2, concat_axis=0, tiled=True,
            ),
        )
    spare = -per_dev % LANES
    pad = lambda a: jnp.pad(a, [(0, 0)] * (a.ndim - 1) + [(0, spare)]) if spare else a
    states = tuple(pad(state) for state in states)
    cell = me * per_dev + jnp.arange(per_dev, dtype=jnp.int32)
    dev, mix, keep = solve_cells(
        pool,
        pad(jnp.transpose(patch_index[0])),
        pad(patch_count),
        pad((cell // columns).astype(jnp.float32)[None]),
        pad((cell % columns).astype(jnp.float32)[None]),
        members,
    )

    loss = jnp.exp(-dep_velocity[:, None, None] * surface_factor[None])
    if paired:
        lowest = (jnp.arange(levels, dtype=jnp.int32) == 0)[None, None, :, None]
        factor = jnp.where(lowest, jnp.moveaxis(loss, 1, 0)[:, :, None], 1.0).reshape(tile_rows, fields, columns)
        out = finish(*states, late, dev, mix, keep, edge, factor, slots, tile_rows)
        return out.reshape(ensemble.shape)

    width = next(w for w in (32, 16, fields) if fields % w == 0)
    wide_x = wide_rows(jnp.moveaxis(courant_x, 1, 0), SUBSTEPS)
    wide_y = wide_rows(jnp.moveaxis(courant_y, 1, 0), SUBSTEPS)
    out = analyse(states, dev, mix, keep, slots, 0, fields, width)
    back = lax.all_to_all(out[0][..., :per_dev], "mem", split_axis=0, concat_axis=2, tiled=True)
    rows = jnp.moveaxis(back.reshape(local_members, fields, tile_rows, columns), 2, 0)
    south, north = halo(rows, SUBSTEPS)
    shape = (local_members, species, levels, columns)
    now = [
        part[r].reshape(shape).astype(jnp.float32)
        for part in (south, rows, north)
        for r in range(part.shape[0])
    ]
    for repeat in range(SUBSTEPS):
        first = repeat + 1
        now = [
            col_step(
                row_step(now[r - 1], now[r], now[r + 1], wide_y[first + r - 1]),
                wide_x[first + r - 1],
            )
            for r in range(1, len(now) - 1)
        ]
    lowest = (jnp.arange(levels, dtype=jnp.int32) == 0)[:, None]
    now = [row * jnp.where(lowest, loss[:, r][:, None], 1.0) for r, row in enumerate(now)]
    joined = jnp.stack([row.astype(jnp.bfloat16) for row in now], axis=3)
    return joined.reshape(local_members, fields, tile_rows, columns)


def solution(mesh):
    in_specs = (
        P("mem", None, "space", None),
        P("space", None),
        P("space", None),
        P("space", None),
        P("space", None),
        P("space", "mem", None),
        P("space", "mem"),
        P(None, "space", None),
        P(None, "space", None),
        P(),
        P("space", None),
    )
    out_specs = P("mem", None, "space", None)
    return jax.shard_map(shards, mesh=mesh, in_specs=in_specs, out_specs=out_specs, check_vma=False)
```

```python
import functools
import math

import jax
import jax.numpy as jnp
from jax import lax
from jax.experimental import pallas as pl
from jax.experimental.pallas import tpu as pltpu
from jax.sharding import PartitionSpec as P

NEWTON = 8
SUBSTEPS = 2
LOC = 1
LANES = 128
GROUP = 8
PITCH = 40
WIDTH = 16
LAG = 8
RELAY = 3
LATE = 2
QUAD = 4
UNROLL = 8
INTERPRET = False


def lane_product(left, right, depth, rows, width, finish, unroll=4, group=GROUP):
    def several(block, carry):
        first = pl.multiple_of(block * group, group)

        def step(k, sums):
            row = right(k)
            return tuple(sums[r] + left(k, first, r) * row for r in range(group))

        zero = jnp.zeros((width, LANES), jnp.float32)
        sums = lax.fori_loop(0, depth, step, (zero,) * group, unroll=unroll)
        finish(first, sums)
        return carry

    lax.fori_loop(0, rows // group, several, 0)


def weights_kernel(
    members, repeats, radius,
    pool_ref, idx_ref, cnt_ref, row_ref, col_ref,
    dev_ref, mix_ref, keep_ref,
    first_v, one_v, two_v, step_g, keys, innov, scal,
):
    slots = idx_ref.shape[0]
    pooled = pool_ref.shape[1]
    blocks = slots // GROUP
    info = pool_ref[members:, :]
    high = info.astype(jnp.bfloat16).astype(jnp.float32)
    rest = info - high
    middle = rest.astype(jnp.bfloat16).astype(jnp.float32)
    low = rest - middle
    table = jnp.concatenate([pool_ref[:members, :], high, middle, low, jnp.zeros_like(low)], axis=0)
    table = table.astype(jnp.bfloat16)
    place = lax.broadcasted_iota(jnp.int32, (pooled, LANES), 0)
    extra = info.shape[0]

    def pick(k, total):
        hot = jnp.where(place == idx_ref[pl.ds(k, 1), :], 1.0, 0.0).astype(jnp.bfloat16)
        got = jnp.dot(table, hot, preferred_element_type=jnp.float32)
        equiv = got[:members]
        facts = (
            got[members : members + extra]
            + got[members + extra : members + 2 * extra]
            + got[members + 2 * extra : members + 3 * extra]
        )
        mean = jnp.sum(equiv, axis=0, keepdims=True) * (1.0 / members)
        dist = (facts[2:3] - row_ref[...]) ** 2 + (facts[3:4] - col_ref[...]) ** 2
        rho = jnp.exp(-dist / (2.0 * radius * radius)) / facts[1:2]
        scale = jnp.sqrt(jnp.where(k < cnt_ref[...], rho, 0.0))
        scaled = (equiv - mean) * scale
        dev_ref[pl.ds(k, members, stride=PITCH), :] = scaled
        innov[pl.ds(k, 1), :] = (facts[0:1] - mean) * scale
        return total + jnp.sum(scaled * scaled, axis=0, keepdims=True)

    spread = lax.fori_loop(0, slots, pick, jnp.zeros((1, LANES), jnp.float32), unroll=8)
    shift = members - 1.0
    inverse = 1.0 / (spread + shift * members)
    level = lax.broadcasted_iota(jnp.int32, (GROUP, LANES), 0)

    def eye(r, value):
        return jnp.where(level == r, value, 0.0)

    def at(ref, i, j, base=0):
        start = i * PITCH + j * GROUP
        start = start if isinstance(start, int) else pl.multiple_of(start, GROUP)
        return ref[pl.ds(base + start, GROUP), :]

    def put(ref, i, parts, base=0):
        for j, part in enumerate(parts):
            ref[pl.ds(base + i * PITCH + j * GROUP, GROUP), :] = part
            if j < i // GROUP:
                ref[pl.ds(base + j * GROUP * PITCH + i, GROUP, stride=PITCH), :] = part

    def product(left, right, depth, finish, unroll=16):
        for pair in range((blocks + 1) // 2):
            groups = sorted({pair, blocks - 1 - pair})

            def step(k, sums):
                wide = [right(k, j) for j in range(groups[-1] + 1)]
                out, spot = [], 0
                for g in groups:
                    for r in range(GROUP):
                        one = left(k, g * GROUP + r)
                        for j in range(g + 1):
                            out.append(sums[spot] + one * wide[j])
                            spot += 1
                return tuple(out)

            zero = jnp.zeros((GROUP, LANES), jnp.float32)
            count = sum((g + 1) * GROUP for g in groups)
            sums = lax.fori_loop(0, depth, step, (zero,) * count, unroll=unroll)
            spot = 0
            for g in groups:
                for r in range(GROUP):
                    finish(g * GROUP + r, sums[spot : spot + g + 1])
                    spot += g + 1

    def square(left, right, finish, base=0):
        product(
            lambda k, i: left[pl.ds(base + k * PITCH + i, 1), :],
            lambda k, j: at(right, k, j),
            slots, finish,
        )

    def gram_done(i, sums):
        put(first_v, i, [part * inverse for part in sums])

    product(
        lambda k, i: dev_ref[pl.ds(k * PITCH + i, 1), :],
        lambda k, j: at(dev_ref, k, j),
        members, gram_done,
    )

    xi = shift * inverse
    mus = []
    for k in range(repeats):
        mu = 1.5 - 0.5 * xi
        scal[pl.ds(k, 1), :] = xi
        scal[pl.ds(repeats + k, 1), :] = mu
        mus.append(mu)
        xi = xi * mu * mu
    after = mus[-1]
    for k in reversed(range(repeats - 1)):
        scal[pl.ds(2 * repeats + k, 1), :] = after
        after = after * mus[k]
    last_z = after
    area = slots * PITCH

    def forward(n, old, new):
        xi = scal[pl.ds(n, 1), :]
        mu = scal[pl.ds(repeats + n, 1), :]
        flat, slope = mu * mu - xi * mu, 0.25 * xi - mu
        base = pl.multiple_of(n * area, GROUP)

        def to_g(i, sums):
            parts = [0.25 * part + slope * at(old, i, j) for j, part in enumerate(sums)]
            parts[-1] = parts[-1] + eye(i % GROUP, flat)
            put(step_g, i, parts)

        square(old, old, to_g)

        def to_v(i, sums):
            put(new, i, sums)
            put(keys, i, [mu * at(step_g, i, j) - 0.5 * part for j, part in enumerate(sums)], base)

        square(step_g, old, to_v)

    def forward_pair(n, carry):
        forward(2 * n + 1, one_v, two_v)
        forward(2 * n + 2, two_v, one_v)
        return carry

    forward(0, first_v, one_v)
    lax.fori_loop(0, repeats // 2 - 1, forward_pair, 0)

    after = scal[pl.ds(3 * repeats - 2, 1), :]
    for i in range(slots):
        parts = [-0.5 * at(keys, i, j, (repeats - 2) * area) for j in range(blocks)]
        parts[i // GROUP] = parts[i // GROUP] - eye(i % GROUP, 0.5 * after)
        for j, part in enumerate(parts):
            one_v[pl.ds(i * PITCH + j * GROUP, GROUP), :] = part

    def backward(n, old, new):
        base = pl.multiple_of(n * area, GROUP)
        half = 0.5 * scal[pl.ds(2 * repeats + n, 1), :]

        def to_h(i, sums):
            parts = list(sums)
            parts[-1] = parts[-1] - eye(i % GROUP, half)
            put(new, i, parts)

        square(keys, old, to_h, base)

    def backward_pair(m, carry):
        backward(repeats - 3 - 2 * m, one_v, two_v)
        backward(repeats - 4 - 2 * m, two_v, one_v)
        return carry

    lax.fori_loop(0, repeats // 2 - 1, backward_pair, 0)

    def whole(ref, k):
        return ref[pl.ds(pl.multiple_of(k * PITCH, GROUP), slots), :]

    none = jnp.zeros((slots, LANES), jnp.float32)

    def apply(ref):
        def step(k, total):
            return total + innov[pl.ds(k, 1), :] * whole(ref, k)

        return lax.fori_loop(0, slots, step, none)

    for _ in range(2):
        start = innov[...]
        innov[...] = apply(one_v)
        innov[...] = last_z * start + apply(first_v)
    gain = innov[...] * inverse
    factor = math.sqrt(shift) * jnp.sqrt(inverse)
    keep_ref[...] = factor * last_z
    both = factor * inverse

    def to_mix(first, sums):
        for r in range(GROUP):
            mix_ref[pl.ds(pl.multiple_of((first + r) * slots, slots), slots), :] = both * sums[r] + gain

    lane_product(
        lambda k, first, r: dev_ref[pl.ds((first + r) * PITCH + k, 1), :],
        lambda k: whole(one_v, k), slots, members, slots, to_mix, unroll=16,
    )


def solve_cells(pool, idx, counts, rows, cols, members):
    slots, cells = idx.shape
    lane = lambda height: pl.BlockSpec((height, LANES), lambda c: (0, c))
    square = pltpu.VMEM((slots * PITCH, LANES), jnp.float32)
    return pl.pallas_call(
        functools.partial(weights_kernel, members, NEWTON, LOC),
        grid=(cells // LANES,),
        in_specs=[pl.BlockSpec(pool.shape, lambda c: (0, 0)), lane(slots), lane(1), lane(1), lane(1)],
        out_specs=[lane(members * PITCH), lane(members * slots), lane(1)],
        out_shape=[
            jax.ShapeDtypeStruct((members * PITCH, cells), jnp.float32),
            jax.ShapeDtypeStruct((members * slots, cells), jnp.float32),
            jax.ShapeDtypeStruct((1, cells), jnp.float32),
        ],
        scratch_shapes=[
            square,
            square,
            square,
            square,
            pltpu.VMEM(((NEWTON - 1) * slots * PITCH, LANES), jnp.float32),
            pltpu.VMEM((slots, LANES), jnp.float32),
            pltpu.VMEM((3 * NEWTON, LANES), jnp.float32),
        ],
        compiler_params=pltpu.CompilerParams(vmem_limit_bytes=40 * 1024 * 1024),
        cost_estimate=pl.CostEstimate(flops=2 * 10**9, bytes_accessed=200 * 10**6, transcendentals=0),
        interpret=INTERPRET,
    )(pool, idx, counts, rows, cols)


def split_kernel(rows, levels, flat_ref, mine_ref, early_ref, late_ref, lowest_ref, spread):
    me = lax.axis_index("mem")
    batch, fields, _ = mine_ref.shape
    species = fields // levels
    span = fields * rows
    for slot in range(batch):
        spread[slot] = flat_ref[pl.ds(slot * span, span), :].astype(jnp.float32)
        mine_ref[slot] = spread[slot, pl.ds(me, fields, stride=rows), :].astype(jnp.bfloat16)
        theirs = spread[slot, pl.ds(1 - me, fields, stride=rows), :].astype(jnp.bfloat16)
        early_ref[slot] = theirs[: early_ref.shape[1]]
        late_ref[slot] = theirs[early_ref.shape[1] :]
        lowest_ref[slot] = jnp.concatenate(
            [spread[slot, pl.ds(r, species, stride=rows * levels), :] for r in range(rows)], axis=0
        ).astype(jnp.bfloat16)


def separate(flat, share, fields, rows, levels):
    span = fields * rows
    block = lambda height: pl.BlockSpec((UNROLL, height, LANES), lambda n: (n, 0, 0))
    out = lambda height: jax.ShapeDtypeStruct((share, height, LANES), jnp.bfloat16)
    late = LATE * WIDTH
    heights = (fields, fields - late, late, rows * fields // levels)
    return pl.pallas_call(
        functools.partial(split_kernel, rows, levels),
        grid=(share // UNROLL,),
        in_specs=[pl.BlockSpec((UNROLL * span, LANES), lambda n: (n, 0))],
        out_specs=[block(height) for height in heights],
        out_shape=[out(height) for height in heights],
        scratch_shapes=[pltpu.VMEM((UNROLL, span, LANES), jnp.float32)],
        compiler_params=pltpu.CompilerParams(vmem_limit_bytes=16 * 1024 * 1024),
        cost_estimate=pl.CostEstimate(flops=10**7, bytes_accessed=6 * 10**6, transcendentals=0),
        interpret=INTERPRET,
    )(flat)


def prep_kernel(
    rows, species,
    lowest_ref, value_ref, error_ref, cell_ref, species_ref, courant_x_ref, courant_y_ref,
    pool_ref, edge_ref, found, block, facts_ref, wind, land, land_facts, send_sems, recv_sems, facts_sent, facts_come,
):
    share = lowest_ref.shape[0]
    observed = value_ref.shape[1]
    levels = courant_x_ref.shape[0] // rows
    me, place, count = lax.axis_index("mem"), lax.axis_index("space"), lax.axis_size("space")

    def exists(step):
        return (place + step >= 0) & (place + step < count)

    def guard(step, act):
        if step == 0:
            act()
        else:
            pl.when(exists(step))(act)

    ways = [(1, 0), (0, -1), (0, 1), (1, -1), (1, 1)]
    barrier = pltpu.get_barrier_semaphore()

    def target(flip, step):
        return (1 - me if flip else me, place + step)

    for flip, step in ways:
        def greet(flip=flip, step=step):
            pl.semaphore_signal(barrier, inc=1, device_id=target(flip, step), device_id_type=pl.DeviceIdType.MESH)

        guard(step, greet)

    cell = cell_ref[...]
    row, column = lax.shift_right_logical(cell, LANES.bit_length() - 1), cell & (LANES - 1)
    facts_ref[pl.ds(0, GROUP), :] = jnp.zeros((GROUP, observed), jnp.float32)
    facts = (value_ref[...], error_ref[...], row.astype(jnp.float32), column.astype(jnp.float32))
    for n, fact in enumerate(facts):
        facts_ref[pl.ds(n, 1), :] = fact
    for n, courant in enumerate((courant_x_ref, courant_y_ref)):
        wind[n, pl.ds(0, rows * levels), :] = courant[...]
        for copy in range(GROUP // levels):
            for r in range(rows):
                start = (n + 1) * GROUP + copy * levels
                facts_ref[pl.ds(start, levels), pl.ds(r * LANES, LANES)] = wind[n, pl.ds(r, levels, stride=rows), :]
    hot = jnp.where(lax.broadcasted_iota(jnp.int32, (LANES, observed), 0) == column, 1.0, 0.0).astype(jnp.bfloat16)
    wanted = lax.broadcasted_iota(jnp.int32, (rows * species, observed), 0) == row * species + species_ref[...]

    def look(n, carry):
        for slot in range(UNROLL):
            i = UNROLL * n + slot
            got = jnp.dot(lowest_ref[i], hot, preferred_element_type=jnp.float32)
            found[pl.ds(i, 1), :] = jnp.sum(jnp.where(wanted, got, 0.0), axis=0, keepdims=True)
        return carry

    lax.fori_loop(0, share // UNROLL, look, 0)
    block[...] = found[pl.ds(0, share), :].astype(jnp.bfloat16)

    greeted = 1 + 2 * exists(-1).astype(jnp.int32) + 2 * exists(1).astype(jnp.int32)
    pl.semaphore_wait(barrier, greeted)

    def copy(n):
        flip, step = ways[n]
        return pltpu.make_async_remote_copy(
            src_ref=block, dst_ref=land.at[1 - step, flip],
            send_sem=send_sems.at[n], recv_sem=recv_sems.at[1 - step, flip],
            device_id=target(flip, step), device_id_type=pl.DeviceIdType.MESH,
        )

    def copy_facts(step):
        return pltpu.make_async_remote_copy(
            src_ref=facts_ref.at[pl.ds(0, 3 * GROUP)], dst_ref=land_facts.at[1 - step],
            send_sem=facts_sent.at[1 - step], recv_sem=facts_come.at[1 - step],
            device_id=(me, place + step), device_id_type=pl.DeviceIdType.MESH,
        )

    for n, (flip, step) in enumerate(ways):
        guard(step, lambda n=n: copy(n).start())
    for step in (-1, 1):
        guard(step, lambda step=step: copy_facts(step).start())
    for step in (-1, 1):
        def blank(step=step):
            land[1 + step] = jnp.zeros_like(land[1 + step])
            land_facts[1 + step] = jnp.zeros_like(land_facts[1 + step])

        pl.when(jnp.logical_not(exists(step)))(blank)
    for n, (flip, step) in enumerate(ways):
        def landed(n=n):
            copy(n).wait_recv()

        guard(-step, landed)
    for step in (-1, 1):
        guard(-step, lambda step=step: copy_facts(step).wait_recv())
    line = lax.broadcasted_iota(jnp.int32, (GROUP, observed), 0)
    for part in range(3):
        lanes = pl.ds(part * observed, observed)
        own = found[pl.ds(0, share), :] if part == 1 else land[part, 0].astype(jnp.float32)
        facts = facts_ref[pl.ds(0, 3 * GROUP), :] if part == 1 else land_facts[part]
        pool_ref[pl.ds(0, share), lanes] = own
        pool_ref[pl.ds(share, share), lanes] = land[part, 1].astype(jnp.float32)
        pool_ref[pl.ds(2 * share, GROUP), lanes] = facts[:GROUP] + jnp.where(
            line == 2, float(rows * (part - 1)), 0.0
        )
        edge_ref[part] = facts[GROUP:]
    for n, (flip, step) in enumerate(ways):
        def sent(n=n):
            copy(n).wait_send()

        guard(step, sent)
    for step in (-1, 1):
        guard(step, lambda step=step: copy_facts(step).wait_send())


def prepare(lowest, facts, courants, rows, species):
    share = lowest.shape[0]
    observed = facts[0].shape[1]
    vmem = pl.BlockSpec(memory_space=pltpu.VMEM)
    return pl.pallas_call(
        functools.partial(prep_kernel, rows, species),
        in_specs=[vmem] * 7,
        out_specs=[vmem] * 2,
        out_shape=[
            jax.ShapeDtypeStruct((2 * share + GROUP, 3 * observed), jnp.float32),
            jax.ShapeDtypeStruct((3, 2 * GROUP, observed), jnp.float32),
        ],
        scratch_shapes=[
            pltpu.VMEM((share + GROUP, observed), jnp.float32),
            pltpu.VMEM((share, observed), jnp.bfloat16),
            pltpu.VMEM((4 * GROUP, observed), jnp.float32),
            pltpu.VMEM((2, 4 * GROUP, LANES), jnp.float32),
            pltpu.VMEM((3, 2, share, observed), jnp.bfloat16),
            pltpu.VMEM((3, 3 * GROUP, observed), jnp.float32),
            pltpu.SemaphoreType.DMA((5,)),
            pltpu.SemaphoreType.DMA((3, 2)),
            pltpu.SemaphoreType.DMA((3,)),
            pltpu.SemaphoreType.DMA((3,)),
        ],
        compiler_params=pltpu.CompilerParams(
            vmem_limit_bytes=16 * 1024 * 1024, collective_id=0, has_side_effects=True
        ),
        cost_estimate=pl.CostEstimate(flops=10**8, bytes_accessed=10**6, transcendentals=0),
        interpret=INTERPRET,
    )(lowest, *facts, *courants)


def analysis_kernel(parts, slots, *refs):
    states = refs[:parts]
    dev_ref, mix_ref, keep_ref = refs[parts : parts + 3]
    outs = refs[parts + 3 : 2 * parts + 3]
    anomaly, mapped, mean_ref = refs[2 * parts + 3 :]
    share, width, _ = states[0].shape
    members = share * parts
    total = jnp.zeros((width, LANES), jnp.float32)
    for state in states:
        total = lax.fori_loop(
            0, share, lambda i, t, s=state: t + s[i].astype(jnp.float32), total, unroll=4
        )
    mean = total * (1.0 / members)
    mean_ref[...] = mean
    for part, state in enumerate(states):

        def subtract(i, carry, s=state, base=part * share):
            anomaly[base + i] = s[i].astype(jnp.float32) - mean_ref[...]
            return carry

        lax.fori_loop(0, share, subtract, 0, unroll=4)

    def to_mapped(first, sums):
        for r in range(GROUP):
            mapped[first + r] = sums[r]

    lane_product(
        lambda i, first, r: dev_ref[pl.ds(i * PITCH + first + r, 1), :],
        lambda i: anomaly[i], members, slots, width, to_mapped,
    )
    for part, out in enumerate(outs):
        base = part * share

        def to_out(first, sums, out=out, base=base):
            for r in range(GROUP):
                held = mean_ref[...] + keep_ref[...] * anomaly[base + first + r]
                out[first + r] = (held + sums[r]).astype(jnp.bfloat16)

        lane_product(
            lambda k, first, r, base=base: mix_ref[pl.ds((base + first + r) * slots + k, 1), :],
            lambda k: mapped[k], slots, share, width, to_out,
        )


def finish_kernel(
    slots, width,
    mine_ref, other_ref, theirs_ref, dev_ref, mix_ref, keep_ref, edge_ref, loss_ref, out_ref,
    rows, away, south, north, held_ref, late_ref, values, mapped, mean_ref, coef, weave,
    away_sent, away_come, edge_sent, edge_come, held_sent, held_come, late_sent, late_come,
):
    share, fields, _ = mine_ref.shape
    members = 2 * share
    chunks = fields // width
    early = other_ref.shape[1] // width
    group = 2 * LANES // width
    me, place, count = lax.axis_index("mem"), lax.axis_index("space"), lax.axis_size("space")
    mesh_id = pl.DeviceIdType.MESH
    exists = (place > 0, place + 1 < count)
    sides = ((1 - me, place), (me, place - 1), (me, place + 1))
    relays = count % QUAD == 0 and count > QUAD
    floors, floor, corner = count // QUAD, place // QUAD, place % QUAD
    near, far = corner == 0, corner == QUAD - 1
    across = (me, jnp.where(far, place - (QUAD - 1), place + (QUAD - 1)))
    ahead = (me, jnp.where(far, place - QUAD, place + QUAD))
    behind = (me, jnp.where(far, place + QUAD, place - QUAD))
    goes = jnp.where(far, floor > 0, floor < floors - 1)
    comes = jnp.where(far, floor < floors - 1, floor > 0)
    barrier = pltpu.get_barrier_semaphore()
    pl.semaphore_signal(barrier, inc=1, device_id=sides[0], device_id_type=mesh_id)
    for side in range(2):
        @pl.when(exists[side])
        def _():
            pl.semaphore_signal(barrier, inc=1, device_id=sides[1 + side], device_id_type=mesh_id)

    if relays:
        for there, device in ((True, across), (goes, ahead), (comes, behind)):
            @pl.when((near | far) & there)
            def _():
                pl.semaphore_signal(barrier, inc=1, device_id=device, device_id_type=mesh_id)

    for side, buffer in enumerate((south, north)):
        @pl.when(jnp.logical_not(exists[side]))
        def _():
            def clear(n, carry):
                for r in range(2):
                    buffer[r, n // share, n % share] = jnp.zeros((width, LANES), jnp.bfloat16)
                return carry

            lax.fori_loop(0, chunks * share, clear, 0)

    lane = lax.broadcasted_iota(jnp.int32, (GROUP, LANES), 1)
    for at, (part, r) in enumerate(((0, 1), (1, 0), (1, 1), (2, 0))):
        cut = pl.ds(r * LANES, LANES)
        cx = edge_ref[part, pl.ds(0, GROUP), cut]
        cy = edge_ref[part, pl.ds(GROUP, GROUP), cut]
        six = (
            1.0 - cy * cy,
            0.5 * cy * cy - 0.5 * cy,
            0.5 * cy * cy + 0.5 * cy,
            1.0 - cx * cx,
            jnp.where(lane == LANES - 1, 0.0, 0.5 * cx * cx - 0.5 * cx),
            jnp.where(lane == 0, 0.0, 0.5 * cx * cx + 0.5 * cx),
        )
        for n, value in enumerate(six):
            for piece in range(width // GROUP):
                coef[6 * at + n, pl.ds(piece * GROUP, GROUP), :] = value

    greeted = 1 + exists[0].astype(jnp.int32) + exists[1].astype(jnp.int32)
    if relays:
        more = 1 + goes.astype(jnp.int32) + comes.astype(jnp.int32)
        greeted = greeted + jnp.where(near | far, more, 0)
    pl.semaphore_wait(barrier, greeted)

    def share_of(r, q, part):
        return (2 * r + q % 2) * floors < 4 * part

    def detours(side, r, q):
        if side:
            return far & share_of(r, q, floors - 1 - floor)
        return near & share_of(r, q, floor)

    def hand_over(side, r, q):
        return pltpu.make_async_remote_copy(
            src_ref=rows.at[r, q], dst_ref=held_ref.at[r, q],
            send_sem=edge_sent.at[side, r, q], recv_sem=held_come.at[r, q],
            device_id=across, device_id_type=mesh_id,
        )

    def hand_on(side, r, q):
        return pltpu.make_async_remote_copy(
            src_ref=held_ref.at[r, q], dst_ref=(north, south)[side].at[r, q],
            send_sem=held_sent.at[r, q], recv_sem=edge_come.at[side, r, q],
            device_id=ahead, device_id_type=mesh_id,
        )

    def relayed(side, r, q):
        if side:
            return near & share_of(r, q, floors - 1 - floor)
        return far & share_of(r, q, floor)

    def relay(r, q):
        for side in range(2):
            @pl.when(relayed(side, r, q))
            def _():
                hand_over(side, r, q).wait_recv()
                hand_on(side, r, q).start()

    def swap(q):
        return pltpu.make_async_remote_copy(
            src_ref=away.at[q], dst_ref=rows.at[me, q],
            send_sem=away_sent.at[q], recv_sem=away_come.at[q],
            device_id=sides[0], device_id_type=mesh_id,
        )

    def pass_on(side, r, q):
        return pltpu.make_async_remote_copy(
            src_ref=rows.at[r, q], dst_ref=(north, south)[side].at[r, q],
            send_sem=edge_sent.at[side, r, q], recv_sem=edge_come.at[side, r, q],
            device_id=sides[1 + side], device_id_type=mesh_id,
        )

    def pass_both(r, q):
        for side in range(2):
            if not relays:
                pl.when(exists[side])(pass_on(side, r, q).start)
                continue
            turn = detours(side, r, q)

            @pl.when(turn)
            def _():
                hand_over(side, r, q).start()

            @pl.when(exists[side] & jnp.logical_not(turn))
            def _():
                pass_on(side, r, q).start()

    def follow(n):
        return pltpu.make_async_remote_copy(
            src_ref=theirs_ref.at[:, pl.ds(pl.multiple_of(n * width, width), width), :], dst_ref=late_ref.at[n],
            send_sem=late_sent.at[n], recv_sem=late_come.at[n],
            device_id=sides[0], device_id_type=mesh_id,
        )

    def analyse_chunk(q):
        cut = pl.ds(pl.multiple_of(q * width, width), width)
        zero = jnp.zeros((width, LANES), jnp.float32)

        def fill(load, base):
            def one(i, total):
                value = load(i).astype(jnp.float32)
                values[base + i] = value
                return total + value

            return lax.fori_loop(0, share, one, zero, unroll=8)

        mean_ref[...] = fill(lambda i: mine_ref[i, cut, :], 0)

        @pl.when(q < early)
        def _():
            mean_ref[...] += fill(lambda i: other_ref[i, cut, :], share)

        @pl.when(q >= early)
        def _():
            follow(q - early).wait_recv()
            mean_ref[...] += fill(lambda i: late_ref[q - early, i], share)

        mean_ref[...] = (1.0 - keep_ref[...]) * (mean_ref[...] * (1.0 / members))

        def to_mapped(first, sums):
            for r in range(group):
                mapped[first + r] = sums[r]

        lane_product(
            lambda i, first, r: dev_ref[pl.ds(i * PITCH + first + r, 1), :],
            lambda i: values[i], members, slots, width, to_mapped, group=group,
        )
        for part in (0, 1):
            base = part * share

            def to_out(first, sums, base=base, part=part):
                for r in range(group):
                    held = mean_ref[...] + keep_ref[...] * values[base + first + r]
                    value = (held + sums[r]).astype(jnp.bfloat16)
                    if part:
                        away[q, first + r] = value
                    else:
                        rows[me, q, first + r] = value

            lane_product(
                lambda k, first, r, base=base: mix_ref[pl.ds((base + first + r) * slots + k, 1), :],
                lambda k: mapped[k], slots, share, width, to_out, group=group,
            )
            if part:
                swap(q).start()

                @pl.when(q < chunks - early)
                def _():
                    follow(q).start()
            else:
                pass_both(me, q)

    def advect_chunk(q):
        cut = pl.ds(pl.multiple_of(q * width, width), width)

        def along(at, low, middle, high):
            now = coef[6 * at] * middle + coef[6 * at + 1] * high + coef[6 * at + 2] * low
            thin = now.astype(jnp.bfloat16)
            east = pltpu.roll(thin, LANES - 1, 1).astype(jnp.float32)
            west = pltpu.roll(thin, 1, 1).astype(jnp.float32)
            return coef[6 * at + 3] * now + coef[6 * at + 4] * east + coef[6 * at + 5] * west

        def several(n, carry):
            for slot in range(UNROLL):
                i = UNROLL * n + slot
                now = [
                    part[r, q, i].astype(jnp.float32) for part in (south, rows, north) for r in range(2)
                ]
                now = [along(at, *now[at : at + 3]) for at in range(4)]
                now = [along(1 + at, *now[at : at + 3]) for at in range(2)]
                for r in range(2):
                    weave[slot, pl.ds(r, width, stride=2), :] = now[r] * loss_ref[r, cut, :]
                start = pl.multiple_of((i * fields + q * width) * 2, 2 * width)
                out_ref[pl.ds(start, 2 * width), :] = weave[slot].astype(jnp.bfloat16)
            return carry

        lax.fori_loop(0, share // UNROLL, several, 0)

    def step(q, carry):
        @pl.when(q < chunks)
        def _():
            analyse_chunk(q)

        @pl.when((q >= 1) & (q - 1 < chunks))
        def _():
            swap(q - 1).wait_recv()
            pass_both(1 - me, q - 1)

        if relays:
            @pl.when((q >= RELAY) & (q - RELAY < chunks))
            def _():
                relay(me, q - RELAY)
                relay(1 - me, q - RELAY)

        @pl.when((q >= LAG) & (q - LAG < chunks))
        def _():
            for side in range(2):
                @pl.when(exists[1 - side])
                def _():
                    for r in range(2):
                        pass_on(side, r, q - LAG).wait_recv()

            advect_chunk(q - LAG)

        return carry

    lax.fori_loop(0, chunks + LAG, step, 0)

    def drain(q, carry):
        swap(q).wait_send()

        @pl.when(q < chunks - early)
        def _():
            follow(q).wait_send()

        for side in range(2):
            @pl.when(exists[side])
            def _():
                for r in range(2):
                    pass_on(side, r, q).wait_send()

            if relays:
                for r in range(2):
                    @pl.when(relayed(side, r, q))
                    def _():
                        hand_on(side, r, q).wait_send()

        return carry

    lax.fori_loop(0, chunks, drain, 0)


def finish(mine, other, theirs, dev, mix, keep, edge, loss, slots, rows):
    share, fields, _ = mine.shape
    width = WIDTH
    chunks = fields // width
    late = theirs.shape[1] // width
    vmem = pl.BlockSpec(memory_space=pltpu.VMEM)
    piece = (chunks, share, width, LANES)
    return pl.pallas_call(
        functools.partial(finish_kernel, slots, width),
        in_specs=[vmem] * 8,
        out_specs=vmem,
        out_shape=jax.ShapeDtypeStruct((share * fields * rows, LANES), jnp.bfloat16),
        scratch_shapes=[
            pltpu.VMEM((2,) + piece, jnp.bfloat16),
            pltpu.VMEM(piece, jnp.bfloat16),
            pltpu.VMEM((2,) + piece, jnp.bfloat16),
            pltpu.VMEM((2,) + piece, jnp.bfloat16),
            pltpu.VMEM((2,) + piece, jnp.bfloat16),
            pltpu.VMEM((late,) + piece[1:], jnp.bfloat16),
            pltpu.VMEM((2 * share, width, LANES), jnp.float32),
            pltpu.VMEM((slots, width, LANES), jnp.float32),
            pltpu.VMEM((width, LANES), jnp.float32),
            pltpu.VMEM((24, width, LANES), jnp.float32),
            pltpu.VMEM((UNROLL, 2 * width, LANES), jnp.float32),
            pltpu.SemaphoreType.DMA((chunks,)),
            pltpu.SemaphoreType.DMA((chunks,)),
            pltpu.SemaphoreType.DMA((2, 2, chunks)),
            pltpu.SemaphoreType.DMA((2, 2, chunks)),
            pltpu.SemaphoreType.DMA((2, chunks)),
            pltpu.SemaphoreType.DMA((2, chunks)),
            pltpu.SemaphoreType.DMA((late,)),
            pltpu.SemaphoreType.DMA((late,)),
        ],
        compiler_params=pltpu.CompilerParams(
            vmem_limit_bytes=40 * 1024 * 1024, collective_id=1, has_side_effects=True
        ),
        cost_estimate=pl.CostEstimate(flops=10**9, bytes_accessed=10**7, transcendentals=0),
        interpret=INTERPRET,
    )(mine, other, theirs, dev, mix, keep, edge, loss)


def analyse(states, dev, mix, keep, slots, first, count, width):
    share, _, cells = states[0].shape
    parts = len(states)
    members = share * parts
    wide = lambda height: pl.BlockSpec((height, LANES), lambda c, f: (0, c))
    return pl.pallas_call(
        functools.partial(analysis_kernel, parts, slots),
        grid=(cells // LANES, count // width),
        in_specs=[
            pl.BlockSpec((share, width, LANES), lambda c, f: (0, f + first // width, c))
        ] * parts + [wide(members * PITCH), wide(members * slots), wide(1)],
        out_specs=[pl.BlockSpec((share, width, LANES), lambda c, f: (0, f, c))] * parts,
        out_shape=[jax.ShapeDtypeStruct((share, count, cells), jnp.bfloat16)] * parts,
        scratch_shapes=[
            pltpu.VMEM((members, width, LANES), jnp.float32),
            pltpu.VMEM((slots, width, LANES), jnp.float32),
            pltpu.VMEM((width, LANES), jnp.float32),
        ],
        compiler_params=pltpu.CompilerParams(vmem_limit_bytes=32 * 1024 * 1024),
        cost_estimate=pl.CostEstimate(flops=10**9, bytes_accessed=50 * 10**6, transcendentals=0),
        interpret=INTERPRET,
    )(*states, dev, mix, keep)


def halo(cells, width):
    count = lax.axis_size("space")
    before = lax.ppermute(cells[-width:], "space", [(i, i + 1) for i in range(count - 1)])
    after = lax.ppermute(cells[:width], "space", [(i + 1, i) for i in range(count - 1)])
    return before, after


def wide_rows(cells, width):
    before, after = halo(cells, width)
    return jnp.concatenate([before, cells, after], axis=0)


def row_step(south, middle, north, courant):
    return (
        middle
        - 0.5 * courant * (north - south)
        + 0.5 * courant * courant * (north - 2.0 * middle + south)
    )


def col_step(middle, courant):
    padded = jnp.pad(middle, [(0, 0)] * (middle.ndim - 1) + [(1, 1)])
    east, west = padded[..., 2:], padded[..., :-2]
    return (
        middle
        - 0.5 * courant * (east - west)
        + 0.5 * courant * courant * (east - 2.0 * middle + west)
    )


def shards(
    ensemble, obs_value, obs_error, obs_cell, obs_species, patch_index, patch_count,
    courant_x, courant_y, dep_velocity, surface_factor,
):
    local_members, fields, tile_rows, columns = ensemble.shape
    species = dep_velocity.shape[0]
    levels = fields // species
    tile_cells = tile_rows * columns
    groups = lax.axis_size("mem")
    members = local_members * groups
    me = lax.axis_index("mem")
    slots = patch_index.shape[2]
    per_dev = tile_cells // groups
    paired = groups == 2 and tile_rows == 2 and columns == LANES
    paired = paired and GROUP % levels == 0 and fields % WIDTH == 0 and fields > 2 * LATE * WIDTH and species % GROUP == 0
    paired = paired and tile_rows * levels <= GROUP
    paired = paired and local_members % UNROLL == 0
    swap = [(0, 1), (1, 0)]

    if paired:
        mine, theirs, late, lowest = separate(
            ensemble.reshape(-1, columns), local_members, fields, tile_rows, levels
        )
        pool, edge = prepare(
            lowest,
            (obs_value, obs_error, obs_cell, obs_species),
            (courant_x.reshape(-1, columns), courant_y.reshape(-1, columns)),
            tile_rows, species,
        )
        theirs, pool = lax.optimization_barrier((theirs, pool))
    else:
        surface = ensemble.reshape(local_members, species, levels, tile_cells)[:, :, 0]
        position = obs_species[0] * tile_cells + obs_cell[0]
        equiv = jnp.take(surface.reshape(local_members, -1), position, axis=1).astype(jnp.float32)
        equiv = lax.all_gather(equiv, "mem", axis=0, tiled=True)
        zeros = jnp.zeros_like(obs_value[0])
        info = jnp.stack(
            [
                obs_value[0],
                obs_error[0],
                (obs_cell[0] // columns).astype(jnp.float32),
                (obs_cell[0] % columns).astype(jnp.float32),
            ]
            + [zeros] * 4
        )
        packed = jnp.concatenate([equiv, info], axis=0)
        before, after = halo(packed[None], 1)
        offset = jnp.zeros((packed.shape[0], 1), jnp.float32).at[members + 2, 0].set(float(tile_rows))
        pool = jnp.concatenate([before[0] - offset, packed, after[0] + offset], axis=1)

    if paired:
        states = (mine, lax.ppermute(theirs, "mem", swap))
    else:
        states = (
            lax.all_to_all(
                ensemble.reshape(local_members, fields, tile_cells),
                "mem", split_axis=2, concat_axis=0, tiled=True,
            ),
        )
    spare = -per_dev % LANES
    pad = lambda a: jnp.pad(a, [(0, 0)] * (a.ndim - 1) + [(0, spare)]) if spare else a
    states = tuple(pad(state) for state in states)
    cell = me * per_dev + jnp.arange(per_dev, dtype=jnp.int32)
    dev, mix, keep = solve_cells(
        pool,
        pad(jnp.transpose(patch_index[0])),
        pad(patch_count),
        pad((cell // columns).astype(jnp.float32)[None]),
        pad((cell % columns).astype(jnp.float32)[None]),
        members,
    )

    loss = jnp.exp(-dep_velocity[:, None, None] * surface_factor[None])
    if paired:
        lowest = (jnp.arange(levels, dtype=jnp.int32) == 0)[None, None, :, None]
        factor = jnp.where(lowest, jnp.moveaxis(loss, 1, 0)[:, :, None], 1.0).reshape(tile_rows, fields, columns)
        out = finish(*states, late, dev, mix, keep, edge, factor, slots, tile_rows)
        return out.reshape(ensemble.shape)

    width = next(w for w in (32, 16, fields) if fields % w == 0)
    wide_x = wide_rows(jnp.moveaxis(courant_x, 1, 0), SUBSTEPS)
    wide_y = wide_rows(jnp.moveaxis(courant_y, 1, 0), SUBSTEPS)
    out = analyse(states, dev, mix, keep, slots, 0, fields, width)
    back = lax.all_to_all(out[0][..., :per_dev], "mem", split_axis=0, concat_axis=2, tiled=True)
    rows = jnp.moveaxis(back.reshape(local_members, fields, tile_rows, columns), 2, 0)
    south, north = halo(rows, SUBSTEPS)
    shape = (local_members, species, levels, columns)
    now = [
        part[r].reshape(shape).astype(jnp.float32)
        for part in (south, rows, north)
        for r in range(part.shape[0])
    ]
    for repeat in range(SUBSTEPS):
        first = repeat + 1
        now = [
            col_step(
                row_step(now[r - 1], now[r], now[r + 1], wide_y[first + r - 1]),
                wide_x[first + r - 1],
            )
            for r in range(1, len(now) - 1)
        ]
    lowest = (jnp.arange(levels, dtype=jnp.int32) == 0)[:, None]
    now = [row * jnp.where(lowest, loss[:, r][:, None], 1.0) for r, row in enumerate(now)]
    joined = jnp.stack([row.astype(jnp.bfloat16) for row in now], axis=3)
    return joined.reshape(local_members, fields, tile_rows, columns)


def solution(mesh):
    in_specs = (
        P("mem", None, "space", None),
        P("space", None),
        P("space", None),
        P("space", None),
        P("space", None),
        P("space", "mem", None),
        P("space", "mem"),
        P(None, "space", None),
        P(None, "space", None),
        P(),
        P("space", None),
    )
    out_specs = P("mem", None, "space", None)
    return jax.shard_map(shards, mesh=mesh, in_specs=in_specs, out_specs=out_specs, check_vma=False)
```
